32 devices in a mesh: row: 4 (over y, x), col: 8 (over z, core).
Axes of the slice: x: 2, y: 2, z: 4, core: 2. Of those that a mesh axis runs over, the one named last changes fastest.
Arguments:
- trail_u: float32 [2, 4, 8, 64, 2048], P(None, 'row', 'col'), may hold values from -6 to 6
- trail_v: float32 [2, 4, 8, 64, 2048], P(None, 'row', 'col'), may hold values from -0.75 to 0.75
- ranks: int32 [2, 4, 8], P(None, 'row', 'col'), may hold values from 16 to 64
- panel_u: float32 [2, 4, 64, 2048], P(None, 'row', None, 'col'), may hold values from -6 to 6
- panel_v: float32 [2, 4, 64, 2048], P(None, 'row', None, 'col'), may hold values from -0.125 to 0.125
- locations: float32 [2, 4, 2, 2048], P(None, 'row', None, 'col'), may hold values from 0 to 1
- pend_locs: float32 [2, 2048], P(None, 'col'), may hold values from 0 to 1
- sketch: float32 [64, 2048], replicated, may hold values from -0.125 to 0.125
Outputs:
- trail_y: float32 [2, 4, 8, 64, 2048], P(None, 'row', 'col')
- trail_z: float32 [2, 4, 8, 64, 2048], P(None, 'row', 'col')
- pend_y: float32 [2, 4, 64, 2048], P(None, 'row', None, 'col')
- pend_z: float32 [2, 4, 64, 2048], P(None, 'row', None, 'col')
The draws below stay inside these ranges and needn't reach their ends.
Inputs may be any that keep to these rules, and one draw needn't show every extreme that they name: `ranks`: ranks_ij leading columns of tile (i, j)'s left factor are in use.
All inputs are finite; a program needn't handle non-finite values.
Results may differ from the reference program's by a relative error of at most 0.0003.
Values sent between devices are 32-bit elements; how exact they have to be, the bound alone decides.
A program may use at most 64 MiB of HBM per device.

```python
import math
import jax
import jax.numpy as jnp
from jax import lax

NB = 2048
K = 64
M = 8
TPR = 2
N_ROW = 4
N_COL = 8


def plant(result, own_key, least, top_value):
    spot = [jax.random.randint(jax.random.fold_in(own_key, axis), (), 0, length) for axis, length in enumerate(result.shape)]
    widest = result.shape.index(max(result.shape))
    beside = spot[:widest] + [(spot[widest] + 1) % result.shape[widest]] + spot[widest + 1:]
    return result.at[tuple(spot)].set(least).at[tuple(beside)].set(top_value)


def level_of(key, extent, pieces, least, top_value):
    factor_of = 1.0
    for dim, shards_of in pieces:
        heights = jax.random.uniform(jax.random.fold_in(jax.random.fold_in(key, 6), dim), (shards_of,), jnp.float32, least / len(pieces), top_value / len(pieces))
        factor_of = factor_of * jnp.repeat(jnp.exp(heights), extent[dim] // shards_of).reshape((-1,) + (1,) * (len(extent) - 1 - dim))
    return factor_of


def scatter_about(own_key, shape, width, most, split=(), kind=jnp.bfloat16):
    loudness = level_of(own_key, shape, split, -0.22, 0.18) if split else 1.0
    values = jax.random.normal(own_key, shape, jnp.float32) * width * loudness
    return jnp.minimum(jnp.maximum(values, -most), most).astype(kind)


def setup_inputs(seed: int = 0) -> dict:
    key_of = jax.random.split(jax.random.key(seed), 9)
    trail_u = scatter_about(key_of[0], (TPR, N_ROW, N_COL, K, NB), 1.0, 6.0, ((1, 4), (2, 8)), jnp.float32)
    trail_v = scatter_about(key_of[1], (TPR, N_ROW, N_COL, K, NB), K ** -0.5, 0.75, ((1, 4), (2, 8)), jnp.float32)
    ranks = plant(jax.random.randint(key_of[2], (TPR, N_ROW, N_COL), K // 4, K + 1), jax.random.fold_in(key_of[2], 1), K // 4, K).astype(jnp.int32)
    panel_u = scatter_about(key_of[3], (TPR, N_ROW, K, NB), 1.0, 6.0, ((1, 4), (3, 8)), jnp.float32)
    panel_v = scatter_about(key_of[4], (TPR, N_ROW, K, NB), NB ** -0.5, 0.125, ((1, 4), (3, 8)), jnp.float32)
    locations = jnp.clip(1.0 * jax.random.uniform(key_of[5], (TPR, N_ROW, 2, NB), jnp.float32) ** level_of(key_of[5], (TPR, N_ROW, 2, NB), ((1, 4), (3, 8)), -0.2, 0.2), 0.0, 1.0)
    pend_locs = jnp.clip(1.0 * jax.random.uniform(key_of[6], (2, NB), jnp.float32) ** level_of(key_of[6], (2, NB), ((1, 8),), -0.2, 0.2), 0.0, 1.0)
    sketch = scatter_about(key_of[7], (K, NB), NB ** -0.5, 0.125, (), jnp.float32)
    return {"trail_u": trail_u, "trail_v": trail_v, "ranks": ranks, "panel_u": panel_u, "panel_v": panel_v, "locations": locations, "pend_locs": pend_locs, "sketch": sketch}


matern_scale = 4.0
length_scale = 0.15
root_three = math.sqrt(3.0)

def matmul(left, right):
    return jnp.dot(left, right, precision=lax.Precision.HIGHEST, preferred_element_type=jnp.float32)

def matern(row_points, col_points):
    delta_x = row_points[0][:, None] - col_points[0][None, :]
    delta_y = row_points[1][:, None] - col_points[1][None, :]
    distance = jnp.sqrt(delta_x * delta_x + delta_y * delta_y)
    scaled = root_three * distance / length_scale
    return matern_scale * (1.0 + scaled) * jnp.exp(-scaled)

def reference(trail_u, trail_v, ranks, panel_u, panel_v, locations, pend_locs, sketch):
    whole_u = panel_u.reshape(M, K, NB)
    whole_v = panel_v.reshape(M, K, NB)
    flat_u = trail_u.reshape(M * N_COL, K, NB)
    flat_v = trail_v.reshape(M * N_COL, K, NB)
    flat_rank = ranks.reshape(M * N_COL)

    def one_tile(flat_index):
        row_tile = flat_index // N_COL
        col_tile = flat_index % N_COL
        in_use = (jnp.arange(K, dtype=jnp.int32) < flat_rank[flat_index]).astype(jnp.float32)
        u_tile = flat_u[flat_index] * in_use[:, None]
        v_tile = flat_v[flat_index]
        row_pu = whole_u[row_tile]
        row_pv = whole_v[row_tile]
        col_pu = whole_u[col_tile]
        col_pv = whole_v[col_tile]
        v_sketch = matmul(v_tile, sketch.T)
        u_sketch = matmul(u_tile, sketch.T)
        cross_gram = matmul(row_pv, col_pv.T)
        col_sketch = matmul(col_pu, sketch.T)
        row_sketch = matmul(row_pu, sketch.T)
        y_tile = matmul(v_sketch.T, u_tile) - matmul(matmul(cross_gram, col_sketch).T, row_pu)
        z_tile = matmul(u_sketch.T, v_tile) - matmul(matmul(row_sketch.T, cross_gram), col_pu)
        keep_tile = row_tile > col_tile
        return (jnp.where(keep_tile, y_tile, 0.0), jnp.where(keep_tile, z_tile, 0.0))
    trail_y, trail_z = lax.map(one_tile, jnp.arange(M * N_COL, dtype=jnp.int32))

    def one_pending(row_points):
        kernel = matern(row_points, pend_locs)
        return (matmul(sketch, kernel.T), matmul(sketch, kernel))
    pend_y, pend_z = lax.map(one_pending, locations.reshape(M, 2, NB))
    return (trail_y.reshape(TPR, N_ROW, N_COL, K, NB), trail_z.reshape(TPR, N_ROW, N_COL, K, NB), pend_y.reshape(TPR, N_ROW, K, NB), pend_z.reshape(TPR, N_ROW, K, NB))
```

```python
import functools
import math

import jax
import jax.numpy as jnp
from jax import lax
from jax.experimental import pallas as pl
from jax.experimental.pallas import tpu as pltpu
from jax.sharding import PartitionSpec as P

matern_scale = 4.0
length_scale = 0.15
root_three = math.sqrt(3.0)
point_scale = root_three / length_scale
log2_e = math.log2(math.e)
smallest = 1e-30

MESH = pl.DeviceIdType.MESH
NN = (((1,), (0,)), ((), ()))
NT = (((1,), (1,)), ((), ()))
SLAB = 16
UNROLL = 8
VMEM_LIMIT = 32 << 20


def halves(value):
    high = value.astype(jnp.bfloat16)
    low = (value - high.astype(jnp.float32)).astype(jnp.bfloat16)
    return high, low


def product(left, right, dims):
    return lax.dot_general(left, right, dims, preferred_element_type=jnp.float32)


def dot3_split(left_both, right, dims):
    rows = left_both.shape[0] // 2
    right_high, right_low = halves(right)
    both = product(left_both, right_high, dims)
    return both[:rows] + both[rows:] + product(left_both[:rows], right_low, dims)


def dot3(left, right, dims):
    left_high, left_low = halves(left)
    return dot3_split(jnp.concatenate([left_high, left_low], axis=0), right, dims)


def kernel(
    n_row, n_col,
    ranks, trail_u, trail_v, panel_u, panel_v, locs, pend, sketch,
    ru, rv, rp, rj, y_left, z_left, pend_acc,
    u_buf, v_buf, sk_buf, loc_all, pu_all, pj_all, pv_all, g_part, g_peer, g_sum, g_all,
    points, own_points, sk_both, mat_high, mat_low, acc, own_sketches, row_sketch, col_sketch,
    far_sem, load_sem, trail_sem, loc_send, loc_recv, pu_send, pf_send, pr_send, pu_recv,
    pv_send, pv_recv, pj_send, pj_recv, gx_send, gx_recv, g_send, g_recv,
):
    row, col = lax.axis_index("row"), lax.axis_index("col")
    n_z = n_col // 2
    z, core = col // 2, col % 2
    other = 1 - core
    partner = 2 * z + other
    slots, rank_dim, width = u_buf.shape
    w = pu_all.shape[3]
    half_z = n_row // 2
    last = (slots - 1) * n_row
    owner_row, owner_slot = col % n_row, col // n_row
    is_owner = row == owner_row
    x_row = row + 1 - 2 * (row % 2)
    y_row = (row + half_z) % n_row
    any_active = last + row > col

    def active(slot):
        return slot * n_row + row > col

    def needs(slot, chip):
        return 2 * chip <= slot * n_row + row

    def carries(slot, chip, source):
        return jnp.logical_or(
            needs(slot, chip), jnp.logical_and(chip == 1, source >= 2))

    def direct(slot, chip, source):
        return jnp.logical_and(
            carries(slot, chip, source),
            jnp.logical_or(chip > 0, source < 2))

    def chip_at(step):
        over = (z + step) // n_z
        return z + step + over * (n_z - 1 - 2 * step - z)

    def wants_column(at_row):
        return last + at_row > col

    def remote(src, dst, send, recv, to_row, to_col):
        return pltpu.make_async_remote_copy(
            src_ref=src, dst_ref=dst, send_sem=send, recv_sem=recv,
            device_id=(to_row, to_col), device_id_type=MESH)

    def loc_copy(source, target):
        return remote(loc_all.at[source], loc_all.at[source], loc_send.at[target],
                      loc_recv.at[source], row, target)

    def pv_copy(slot, source, target):
        return remote(pv_all.at[source, slot], pv_all.at[source, slot],
                      pv_send.at[slot, target], pv_recv.at[slot, source], target, col)

    def pu_copy(slot, block, send, target):
        return remote(pu_all.at[block, slot], pu_all.at[block, slot], send,
                      pu_recv.at[slot, block], row, target)

    def pu_direct(slot, chip):
        return pu_copy(slot, col, pu_send.at[slot, chip], 2 * chip + core)

    def pu_partner(slot, block):
        return pu_copy(slot, block, pf_send.at[slot, block], partner)

    def pu_relay(slot, block):
        return pu_copy(slot, block, pr_send.at[slot, block], core)

    def pj_copy(block, way):
        src = pj_all.at[block] if way == 2 else pu_all.at[block, owner_slot]
        return remote(src, pj_all.at[block], pj_send.at[way, block], pj_recv.at[block],
                      y_row if way == 1 else x_row, col)

    def gx_copy(batch):
        chips = pl.ds(batch * half_z, half_z)
        return remote(g_part.at[other, chips], g_peer.at[chips], gx_send.at[batch],
                      gx_recv.at[batch], row, partner)

    def g_copy(source, chip):
        return remote(g_sum.at[chip], g_all.at[source], g_send.at[chip], g_recv.at[source],
                      row, 2 * chip + core)

    def when(*terms):
        return pl.when(functools.reduce(jnp.logical_and, terms))

    to_y = jnp.logical_or(wants_column(y_row), wants_column(n_row - 1 - row))
    y_of_owner = row == (owner_row + half_z) % n_row
    is_relay = jnp.logical_and(y_of_owner, wants_column(x_row))
    takes_column = jnp.logical_and(
        jnp.logical_not(is_owner),
        jnp.logical_or(wants_column(row), is_relay))

    barrier = pltpu.get_barrier_semaphore()

    def hello(semaphore, to_row, to_col):
        pl.semaphore_signal(semaphore, inc=1, device_id=(to_row, to_col), device_id_type=MESH)

    for step in range(1, n_row):
        hello(barrier, (row + step) % n_row, col)
    hello(barrier, row, partner)
    for chip in range(1, n_z):
        @pl.when(z < chip)
        def _(chip=chip):
            hello(barrier, row, 2 * chip)
            hello(barrier, row, 2 * chip + 1)

    loads = [
        pltpu.make_async_copy(locs, loc_all.at[col, pl.ds(0, slots)], load_sem.at[0]),
        pltpu.make_async_copy(pend, loc_all.at[col, slots], load_sem.at[1]),
        pltpu.make_async_copy(panel_v, pv_all.at[row], load_sem.at[2]),
        pltpu.make_async_copy(panel_u, pu_all.at[col], load_sem.at[3]),
        pltpu.make_async_copy(sketch, sk_buf, load_sem.at[4]),
    ]
    for load in loads:
        load.start()

    def trail_load(slot, which):
        src, dst = ((trail_u, u_buf), (trail_v, v_buf))[which]
        return pltpu.make_async_copy(src.at[slot], dst.at[slot], trail_sem.at[slot, which])

    for slot in range(slots):
        @pl.when(active(slot))
        def _(slot=slot):
            trail_load(slot, 0).start()
            trail_load(slot, 1).start()

    for load in loads[:4]:
        load.wait()
    pl.semaphore_wait(barrier, n_row + 2 * z)

    for chip in range(n_z - 1):
        @pl.when(z > chip)
        def _(chip=chip):
            hello(far_sem, row, 2 * chip)
            hello(far_sem, row, 2 * chip + 1)

    def each_loc(act, higher):
        for chip in range(n_z):
            @pl.when(z < chip if higher else z > chip)
            def _(chip=chip):
                act(loc_copy(col, 2 * chip))
                act(loc_copy(col, 2 * chip + 1))

    def each_direct(act, higher, slot):
        for chip in (range(1, n_z) if higher else reversed(range(n_z - 1))):
            @when(z < chip if higher else z > chip, direct(slot, chip, z))
            def _(chip=chip):
                act(pu_direct(slot, chip))

    def each_pv(act, slot):
        for step in range(1, n_row):
            target = (row + step) % n_row

            @pl.when(last + target > slot * n_row + row)
            def _(target=target):
                act(pv_copy(slot, row, target))

    def each_column(act, block, slot=None):
        ours = is_owner if slot is None else jnp.logical_and(is_owner, owner_slot == slot)

        @when(ours, wants_column(x_row))
        def _():
            act(pj_copy(block, 0))

        @when(ours, to_y)
        def _():
            act(pj_copy(block, 1))

    def start(copy):
        copy.start()

    def wait_send(copy):
        copy.wait_send()

    start(loc_copy(col, partner))
    each_loc(start, False)
    each_pv(start, 0)
    for slot in range(slots):
        each_direct(start, False, slot)

        @pl.when(needs(slot, z))
        def _(slot=slot):
            start(pu_partner(slot, col))
    each_column(start, col)
    for slot in range(1, slots):
        each_pv(start, slot)

    loads[4].wait()
    sk_high, sk_low = halves(sk_buf[...])
    for block in range(n_col):
        sk_both[block, 0:rank_dim] = sk_high[:, block * w:(block + 1) * w]
        sk_both[block, rank_dim:2 * rank_dim] = sk_low[:, block * w:(block + 1) * w]

    acc[...] = jnp.zeros_like(acc)
    row_sketch[...] = jnp.zeros_like(row_sketch)
    col_sketch[...] = jnp.zeros_like(col_sketch)
    own_points[0:1, :] = jnp.concatenate(
        [loc_all[col, slot, 0:1] for slot in range(slots)] + [loc_all[col, slots, 0:1]] * slots,
        axis=1) * point_scale
    own_points[1:2, :] = jnp.concatenate(
        [loc_all[col, slot, 1:2] for slot in range(slots)] + [loc_all[col, slots, 1:2]] * slots,
        axis=1) * point_scale
    pad_rows = points.shape[2] - 2 * slots - 2

    def chunk(step):
        block = 2 * chip_at(step // 2) + (core + step) % 2

        @pl.when(step > 0)
        def _():
            loc_copy(block, partner).wait_recv()

        stack = [loc_all[block, slot] for slot in range(slots + 1)]
        if pad_rows:
            stack.append(jnp.zeros((pad_rows, w), jnp.float32))
        points[0] = jnp.concatenate(stack, axis=0).T * point_scale

        @pl.loop(0, w // SLAB, unroll=UNROLL)
        def _(slab):
            rows = pl.ds(pl.multiple_of(slab * SLAB, SLAB), SLAB)
            at = points[0, rows, :]
            for part in range(2 * slots):
                base = 2 * slots if part < slots else 2 * (part - slots)
                lanes = slice(part * w, (part + 1) * w)
                delta_x = at[:, base:base + 1] - own_points[0:1, lanes]
                delta_y = at[:, base + 1:base + 2] - own_points[1:2, lanes]
                square = delta_x * delta_x + delta_y * delta_y
                scaled = square * lax.rsqrt(jnp.maximum(square, smallest))
                value = (1.0 + scaled) * jnp.exp2(scaled * -log2_e)
                high, low = halves(value)
                mat_high[rows, lanes] = high
                mat_low[rows, lanes] = low

        sk = sk_both[block]
        both = product(sk, mat_high[...], NN)
        acc[...] += (both[:rank_dim] + both[rank_dim:]
                     + product(sk[:rank_dim], mat_low[...], NN))

    def chunks(first, final):
        pl.loop(first * n_col // 8, final * n_col // 8)(chunk)

    def sketch_of(block, high, low):
        sk = sk_both[block]
        both = product(sk, high, NT)
        return both[:rank_dim] + both[rank_dim:] + product(sk[:rank_dim], low, NT)

    def own_sketch(slot):
        trail_load(slot, 0).wait()
        trail_load(slot, 1).wait()
        in_use = lax.broadcasted_iota(jnp.int32, (rank_dim, 1), 0) < ranks[slot]
        v_sketch = jnp.zeros((rank_dim, rank_dim), jnp.float32)
        u_sketch = jnp.zeros((rank_dim, rank_dim), jnp.float32)
        for block in range(n_col):
            lanes = slice(block * w, (block + 1) * w)
            high, low = halves(v_buf[slot, :, lanes])
            rv[slot, 0, :, lanes] = high
            rv[slot, 1, :, lanes] = low
            v_sketch += sketch_of(block, high, low)
            high, low = halves(jnp.where(in_use, u_buf[slot, :, lanes], 0.0))
            ru[slot, 0, :, lanes] = high
            ru[slot, 1, :, lanes] = low
            u_sketch += sketch_of(block, high, low)
        own_sketches[slot, 0] = v_sketch
        own_sketches[slot, 1] = u_sketch

    def own_all():
        for slot in range(slots):
            @pl.when(active(slot))
            def _(slot=slot):
                own_sketch(slot)

    def arrive(slot, step):
        chip = chip_at(step)
        block = 2 * chip + core

        @pl.when(carries(slot, z, chip))
        def _():
            pu_partner(slot, block).wait_recv()

            @when(z == 1, chip >= 2)
            def _():
                pu_relay(slot, block).start()

            @pl.when(needs(slot, z))
            def _():
                pu_partner(slot, block).start()
            each_column(start, block, slot)

    def from_partner(slot, step):
        block = 2 * chip_at(step) + other

        @pl.when(needs(slot, z))
        def _():
            pu_partner(slot, block).wait_recv()
            each_column(start, block, slot)

    def column(step):
        for flip in range(2):
            block = 2 * chip_at(step) + (core + flip) % 2

            @pl.when(takes_column)
            def _():
                pj_copy(block, 0).wait_recv()

                @pl.when(is_relay)
                def _():
                    pj_copy(block, 2).start()

    def gram_part(slot):
        own_v = pv_all[row].reshape(slots * rank_dim, w)
        own_high, own_low = halves(own_v)
        for source in range(n_row):
            tile = slot * n_row + source

            @pl.when(last + row > tile)
            def _(source=source, tile=tile):
                @pl.when(row != source)
                def _():
                    pv_copy(slot, source, row).wait_recv()
                high, low = halves(pv_all[source, slot])
                both = product(jnp.concatenate([high, low], axis=0), own_high, NT)
                g_part[tile % 2, tile // 2] = (
                    both[:rank_dim] + both[rank_dim:] + product(high, own_low, NT))

    def has_batch(batch):
        return last + row > batch * n_row

    def gram_swap(batch):
        @pl.when(has_batch(batch))
        def _():
            gx_copy(batch).start()

    def gram_sum(batch):
        @pl.when(has_batch(batch))
        def _():
            gx_copy(batch).wait_recv()
            for chip in range(batch * half_z, (batch + 1) * half_z):
                g_sum[chip] = g_part[core, chip] + g_peer[chip]

    def each_gram(act, batch):
        for chip in range(batch * half_z, (batch + 1) * half_z):
            @when(last + row > 2 * chip + core, z != chip)
            def _(chip=chip):
                act(g_copy(z, chip))

    def blocks_of(first, final):
        return [2 * chip_at(step) + flip for step in range(first, final) for flip in range(2)]

    def absorb_rows(slot, first, final):
        @pl.when(active(slot))
        def _():
            total = row_sketch[slot]
            for block in blocks_of(first, final):
                lanes = pl.ds(pl.multiple_of(block * w, w), w)
                high, low = halves(pu_all[block, slot])
                rp[slot, 0, :, lanes] = high
                rp[slot, 1, :, lanes] = low
                total += sketch_of(block, high, low)
            row_sketch[slot] = total

    def absorb_column(first, final):
        @pl.when(any_active)
        def _():
            @pl.when(is_owner)
            def _():
                for block in blocks_of(first, final):
                    pj_all[block] = pu_all[block, owner_slot]
            total = col_sketch[...]
            for block in blocks_of(first, final):
                lanes = pl.ds(pl.multiple_of(block * w, w), w)
                high, low = halves(pj_all[block])
                rj[0, :, lanes] = high
                rj[1, :, lanes] = low
                total += sketch_of(block, high, low)
            col_sketch[...] = total

    def upward():
        @pl.when(z < n_z - 1)
        def _():
            pl.semaphore_wait(far_sem, 2 * (n_z - 1 - z))
        each_loc(start, True)
        for slot in range(slots):
            each_direct(start, True, slot)

    chunks(0, 2)
    own_all()
    upward()
    for slot in range(slots):
        from_partner(slot, 0)
    gram_part(0)
    for slot in range(slots):
        arrive(slot, 1)
    column(0)
    gram_swap(0)
    chunks(2, 3)
    gram_sum(0)
    for slot in range(slots):
        from_partner(slot, 1)
    arrive(0, 2)
    each_gram(start, 0)
    chunks(3, 4)
    for slot in range(1, slots):
        arrive(slot, 2)
    column(1)
    for slot in range(1, slots):
        gram_part(slot)
    from_partner(0, 2)
    chunks(4, 5)
    for slot in range(1, slots):
        gram_swap(slot)
    for slot in range(1, slots):
        from_partner(slot, 2)
    arrive(0, 3)
    column(2)
    chunks(5, 6)
    for slot in range(1, slots):
        gram_sum(slot)
    for slot in range(1, slots):
        arrive(slot, 3)
    from_partner(0, 3)
    for slot in range(slots):
        absorb_rows(slot, 0, n_z - 1)
    for slot in range(1, slots):
        each_gram(start, slot)
    absorb_column(0, n_z - 1)
    chunks(6, 8)
    pend_acc[...] = acc[...] * matern_scale
    column(3)
    for slot in range(1, slots):
        from_partner(slot, 3)
    for slot in range(slots):
        absorb_rows(slot, n_z - 1, n_z)
    absorb_column(n_z - 1, n_z)

    @pl.when(any_active)
    def _():
        gram = g_sum[z]
        for step in range(1, n_z):
            chip = chip_at(step)
            g_copy(chip, z).wait_recv()
            gram = gram + g_all[chip]
        left_core = dot3(col_sketch[...], gram, NN)
        nothing = jnp.zeros((rank_dim, 2 * rank_dim), jnp.bfloat16)

        def stacked(value):
            high, low = halves(value)
            return jnp.concatenate([
                jnp.concatenate([high, high], axis=1), jnp.concatenate([low, nothing], axis=1)
            ], axis=0)

        for slot in range(slots):
            lanes = slice(slot * rank_dim, (slot + 1) * rank_dim)

            @pl.when(active(slot))
            def _(slot=slot, lanes=lanes):
                right_core = dot3(row_sketch[slot], gram[:, lanes], NT)
                y_left[slot] = stacked(
                    jnp.concatenate([own_sketches[slot, 0], -left_core[:, lanes]], axis=1))
                z_left[slot] = stacked(
                    jnp.concatenate([own_sketches[slot, 1], -right_core], axis=1))

    wait_send(loc_copy(col, partner))
    for higher in (False, True):
        each_loc(wait_send, higher)
        for slot in range(slots):
            each_direct(wait_send, higher, slot)
    for slot in range(slots):
        each_pv(wait_send, slot)
        each_gram(wait_send, slot)

        @pl.when(has_batch(slot))
        def _(slot=slot):
            gx_copy(slot).wait_send()
        for step in range(n_z):
            chip = chip_at(step)
            block = 2 * chip + core

            @pl.when(needs(slot, z))
            def _(slot=slot, block=block):
                pu_partner(slot, block).wait_send()

            @when(z == 1, chip >= 2)
            def _(slot=slot, block=block):
                pu_relay(slot, block).wait_send()

    @pl.loop(0, n_col)
    def _(block):
        each_column(wait_send, block)

        @pl.when(is_relay)
        def _():
            pj_copy(block, 2).wait_send()


def finish(
    n_row, ru, rv, rp, rj, y_left, z_left, pend_acc,
    trail_y, trail_z, pend_y, pend_z,
    y_buf, z_buf, out_sem, pend_sem,
):
    row, col = lax.axis_index("row"), lax.axis_index("col")
    slots, _, rank_dim, width = ru.shape
    w = pend_y.shape[3]
    pieces = out_sem.shape[2]
    span = width // pieces

    def pend_copy(slot, which):
        lanes = pl.ds((which * slots + slot) * w, w)
        return pltpu.make_async_copy(
            pend_acc.at[:, lanes], (pend_y, pend_z)[which].at[slot, 0], pend_sem.at[slot, which])

    def out_copy(slot, which, piece):
        lanes = pl.ds(piece * span, span)
        src, dst = ((y_buf, trail_y), (z_buf, trail_z))[which]
        return pltpu.make_async_copy(
            src.at[slot, :, lanes], dst.at[slot, 0, 0, :, lanes], out_sem.at[slot, which, piece])

    for slot in range(slots):
        pend_copy(slot, 0).start()
        pend_copy(slot, 1).start()

    for slot in range(slots):
        active = slot * n_row + row > col

        @pl.when(jnp.logical_not(active))
        def _(slot=slot):
            y_buf[slot] = jnp.zeros((rank_dim, width), jnp.float32)
            z_buf[slot] = jnp.zeros((rank_dim, width), jnp.float32)
            for which in range(2):
                for piece in range(pieces):
                    out_copy(slot, which, piece).start()

        @pl.when(active)
        def _(slot=slot):
            for which in range(2):
                left = (y_left, z_left)[which][slot]
                first = (ru, rv)[which]
                buf = (y_buf, z_buf)[which]
                for piece in range(pieces):
                    lanes = slice(piece * span, (piece + 1) * span)
                    second = [rj[part, :, lanes] if which else rp[slot, part, :, lanes]
                              for part in range(2)]
                    right = jnp.concatenate(
                        [first[slot, 0, :, lanes], second[0], first[slot, 1, :, lanes], second[1]],
                        axis=0)
                    both = product(left, right, NN)
                    buf[slot, :, lanes] = both[:rank_dim] + both[rank_dim:]
                    out_copy(slot, which, piece).start()

    for slot in range(slots):
        for which in range(2):
            pend_copy(slot, which).wait()
            for piece in range(pieces):
                out_copy(slot, which, piece).wait()


def broadcast(block, axis, owner):
    block = jnp.where(lax.axis_index(axis) == owner, block, jnp.zeros_like(block))
    return lax.psum(block, axis)


def matmul(left, right):
    return jnp.dot(left, right, precision=lax.Precision.HIGHEST, preferred_element_type=jnp.float32)


def batched(form, left, right):
    return jnp.einsum(
        form, left, right, precision=lax.Precision.HIGHEST, preferred_element_type=jnp.float32
    )


def matern(row_points, col_points):
    delta_x = row_points[0][:, None] - col_points[0][None, :]
    delta_y = row_points[1][:, None] - col_points[1][None, :]
    distance = jnp.sqrt(delta_x * delta_x + delta_y * delta_y)
    scaled = root_three * distance / length_scale
    return matern_scale * (1.0 + scaled) * jnp.exp(-scaled)


def plain_on_device(trail_u, trail_v, ranks, panel_u, panel_v, locations, pend_locs, sketch):
    row_count = lax.axis_size("row")
    row_index = lax.axis_index("row")
    col_index = lax.axis_index("col")
    row_slots = trail_u.shape[0]
    rank_dim = trail_u.shape[3]
    width = trail_u.shape[4]
    local_width = pend_locs.shape[1]
    gathered_u, gathered_v = (
        lax.all_gather(panel_u, "col", axis=3, tiled=True),
        lax.all_gather(panel_v, "col", axis=3, tiled=True),
    )
    slot_index = col_index // row_count
    own_u = lax.dynamic_index_in_dim(gathered_u[:, 0], slot_index, 0, keepdims=False)
    own_v = lax.dynamic_index_in_dim(gathered_v[:, 0], slot_index, 0, keepdims=False)
    col_pu, col_pv = (
        broadcast(own_u, "row", col_index % row_count),
        broadcast(own_v, "row", col_index % row_count),
    )
    rank_iota = lax.broadcasted_iota(jnp.int32, (row_slots, rank_dim), 1)
    in_use = (rank_iota < ranks[:, 0, 0][:, None]).astype(jnp.float32)
    u_tiles = trail_u[:, 0, 0] * in_use[:, :, None]
    v_tiles = trail_v[:, 0, 0]
    row_pu = gathered_u[:, 0]
    row_pv = gathered_v[:, 0]
    v_sketch = batched("tkn,ln->tkl", v_tiles, sketch)
    u_sketch = batched("tkn,ln->tkl", u_tiles, sketch)
    cross_gram = batched("tkn,ln->tkl", row_pv, col_pv)
    col_sketch = matmul(col_pu, sketch.T)
    row_sketch = batched("tkn,ln->tkl", row_pu, sketch)
    left_core = batched("tkm,ml->tkl", cross_gram, col_sketch)
    y_tiles = batched("tkl,tkn->tln", v_sketch, u_tiles) - batched(
        "tkl,tkn->tln", left_core, row_pu
    )
    right_core = batched("tkl,tkm->tlm", row_sketch, cross_gram)
    z_tiles = batched("tkl,tkn->tln", u_sketch, v_tiles) - batched(
        "tlm,mn->tln", right_core, col_pu
    )
    tile_rows = jnp.arange(row_slots, dtype=jnp.int32) * row_count + row_index
    keep_mask = (tile_rows > col_index)[:, None, None]
    trail_y = jnp.where(keep_mask, y_tiles, 0.0).reshape(row_slots, 1, 1, rank_dim, width)
    trail_z = jnp.where(keep_mask, z_tiles, 0.0).reshape(row_slots, 1, 1, rank_dim, width)
    y_list = []
    z_list = []
    rows_all, pend_all = (
        lax.all_gather(locations, "col", axis=3, tiled=True),
        lax.all_gather(pend_locs.reshape(1, 1, 2, local_width), "col", axis=3, tiled=True),
    )
    col_points = pend_all[0, 0]
    for slot_num in range(row_slots):
        own_kernel = matern(locations[slot_num, 0], col_points)
        y_list.append(matmul(sketch, own_kernel.T))
        col_kernel = matern(rows_all[slot_num, 0], pend_locs)
        z_list.append(matmul(sketch, col_kernel))
    pend_y = jnp.stack(y_list)
    pend_z = jnp.stack(z_list)
    pend_y = pend_y.reshape(row_slots, 1, rank_dim, local_width)
    pend_z = pend_z.reshape(row_slots, 1, rank_dim, local_width)
    return (trail_y, trail_z, pend_y, pend_z)


def on_device(n_row, n_col, trail_u, trail_v, ranks, panel_u, panel_v, locations, pend_locs, sketch):
    slots, _, _, rank_dim, width = trail_u.shape
    w = pend_locs.shape[1]
    n_z = n_col // 2
    fits = n_col == slots * n_row and n_row == 4 and slots == 2
    if w % 128 or rank_dim % 16 or not fits:
        return plain_on_device(
            trail_u, trail_v, ranks, panel_u, panel_v, locations, pend_locs, sketch
        )
    flat = slots * rank_dim
    f32, bf16 = jnp.float32, jnp.bfloat16
    dma = pltpu.SemaphoreType.DMA
    vmem = pl.BlockSpec(memory_space=pltpu.VMEM)
    hbm = pl.BlockSpec(memory_space=pltpu.HBM)
    smem = pl.BlockSpec(memory_space=pltpu.SMEM)
    point_rows = -(-(2 * slots + 2) // 8) * 8
    shape = jax.ShapeDtypeStruct
    kept = pl.pallas_call(
        functools.partial(kernel, n_row, n_col),
        out_shape=(
            pltpu.VMEM((slots, 2, rank_dim, width), bf16),
            pltpu.VMEM((slots, 2, rank_dim, width), bf16),
            pltpu.VMEM((slots, 2, rank_dim, width), bf16),
            pltpu.VMEM((2, rank_dim, width), bf16),
            pltpu.VMEM((slots, 2 * rank_dim, 4 * rank_dim), bf16),
            pltpu.VMEM((slots, 2 * rank_dim, 4 * rank_dim), bf16),
            pltpu.VMEM((rank_dim, 2 * slots * w), f32),
        ),
        in_specs=[smem] + [hbm] * 7,
        out_specs=(vmem,) * 7,
        scratch_shapes=[
            pltpu.VMEM((slots, rank_dim, width), f32),
            pltpu.VMEM((slots, rank_dim, width), f32),
            pltpu.VMEM((rank_dim, width), f32),
            pltpu.VMEM((n_col, slots + 1, 2, w), f32),
            pltpu.VMEM((n_col, slots, rank_dim, w), f32),
            pltpu.VMEM((n_col, rank_dim, w), f32),
            pltpu.VMEM((n_row, slots, rank_dim, w), f32),
            pltpu.VMEM((2, n_z, rank_dim, flat), f32),
            pltpu.VMEM((n_z, rank_dim, flat), f32),
            pltpu.VMEM((n_z, rank_dim, flat), f32),
            pltpu.VMEM((n_z, rank_dim, flat), f32),
            pltpu.VMEM((1, w, point_rows), f32),
            pltpu.VMEM((2, 2 * slots * w), f32),
            pltpu.VMEM((n_col, 2 * rank_dim, w), bf16),
            pltpu.VMEM((w, 2 * slots * w), bf16),
            pltpu.VMEM((w, 2 * slots * w), bf16),
            pltpu.VMEM((rank_dim, 2 * slots * w), f32),
            pltpu.VMEM((slots, 2, rank_dim, rank_dim), f32),
            pltpu.VMEM((slots, rank_dim, rank_dim), f32),
            pltpu.VMEM((rank_dim, rank_dim), f32),
            pltpu.SemaphoreType.REGULAR,
            dma((5,)), dma((slots, 2)), dma((n_col,)), dma((n_col,)),
            dma((slots, n_z)), dma((slots, n_col)), dma((slots, n_col)), dma((slots, n_col)),
            dma((slots, n_row)), dma((slots, n_row)),
            dma((3, n_col)), dma((n_col,)),
            dma((slots,)), dma((slots,)), dma((n_z,)), dma((n_z,)),
        ],
        compiler_params=pltpu.CompilerParams(
            collective_id=0, has_side_effects=True, vmem_limit_bytes=VMEM_LIMIT),
    )(*[
        pltpu.with_memory_space_constraint(value, pltpu.HBM) for value in (
            ranks.reshape(slots),
            trail_u.reshape(slots, rank_dim, width),
            trail_v.reshape(slots, rank_dim, width),
            panel_u.reshape(slots, rank_dim, w),
            panel_v.reshape(slots, rank_dim, w),
            locations.reshape(slots, 2, w),
            pend_locs,
            sketch,
        )
    ])
    kept = [pltpu.with_memory_space_constraint(value, pltpu.VMEM) for value in kept]
    pieces = 2
    return pl.pallas_call(
        functools.partial(finish, n_row),
        out_shape=(
            shape((slots, 1, 1, rank_dim, width), f32),
            shape((slots, 1, 1, rank_dim, width), f32),
            shape((slots, 1, rank_dim, w), f32),
            shape((slots, 1, rank_dim, w), f32),
        ),
        in_specs=[vmem] * 7,
        out_specs=(hbm,) * 4,
        scratch_shapes=[
            pltpu.VMEM((slots, rank_dim, width), f32),
            pltpu.VMEM((slots, rank_dim, width), f32),
            dma((slots, 2, pieces)), dma((slots, 2)),
        ],
        compiler_params=pltpu.CompilerParams(vmem_limit_bytes=VMEM_LIMIT),
    )(*kept)


def solution(mesh):
    in_specs = (
        P(None, "row", "col", None, None),
        P(None, "row", "col", None, None),
        P(None, "row", "col"),
        P(None, "row", None, "col"),
        P(None, "row", None, "col"),
        P(None, "row", None, "col"),
        P(None, "col"),
        P(),
    )
    out_specs = (
        P(None, "row", "col", None, None),
        P(None, "row", "col", None, None),
        P(None, "row", None, "col"),
        P(None, "row", None, "col"),
    )
    body = functools.partial(on_device, mesh.shape["row"], mesh.shape["col"])
    return jax.shard_map(
        body, mesh=mesh, in_specs=in_specs, out_specs=out_specs, check_vma=False
    )
```

```python
import functools
import math

import jax
import jax.numpy as jnp
from jax import lax
from jax.experimental import pallas as pl
from jax.experimental.pallas import tpu as pltpu
from jax.sharding import PartitionSpec as P

matern_scale = 4.0
length_scale = 0.15
root_three = math.sqrt(3.0)
point_scale = root_three / length_scale
log2_e = math.log2(math.e)
smallest = 1e-30

MESH = pl.DeviceIdType.MESH
NN = (((1,), (0,)), ((), ()))
NT = (((1,), (1,)), ((), ()))
SLAB = 16
UNROLL = 8
VMEM_LIMIT = 32 << 20


def halves(value):
    high = value.astype(jnp.bfloat16)
    low = (value - high.astype(jnp.float32)).astype(jnp.bfloat16)
    return high, low


def product(left, right, dims):
    return lax.dot_general(left, right, dims, preferred_element_type=jnp.float32)


def dot3_split(left_both, right, dims):
    rows = left_both.shape[0] // 2
    right_high, right_low = halves(right)
    both = product(left_both, right_high, dims)
    return both[:rows] + both[rows:] + product(left_both[:rows], right_low, dims)


def dot3(left, right, dims):
    left_high, left_low = halves(left)
    return dot3_split(jnp.concatenate([left_high, left_low], axis=0), right, dims)


def kernel(
    n_row, n_col,
    ranks_hbm, trail_u, trail_v, panel_u, panel_v, locs, pend, sketch,
    ru, rv, rp, rj, y_left, z_left, pend_acc,
    ranks, u_buf, v_buf, sk_buf, loc_all, pu_all, pj_all, pv_all, g_part, g_peer, g_sum, g_all,
    points, own_points, sk_both, mat_high, mat_low, acc, own_sketches, row_sketch, col_sketch,
    far_sem, load_sem, trail_sem, loc_send, loc_recv, pu_send, pf_send, pr_send, pu_recv,
    pv_send, pv_recv, pj_send, pj_recv, gx_send, gx_recv, g_send, g_recv,
):
    row, col = lax.axis_index("row"), lax.axis_index("col")
    n_z = n_col // 2
    z, core = col // 2, col % 2
    other = 1 - core
    partner = 2 * z + other
    slots, rank_dim, width = u_buf.shape
    w = pu_all.shape[3]
    half_z = n_row // 2
    last = (slots - 1) * n_row
    owner_row, owner_slot = col % n_row, col // n_row
    is_owner = row == owner_row
    x_row = row + 1 - 2 * (row % 2)
    y_row = (row + half_z) % n_row
    diagonal = n_row - 1 - row
    any_active = last + row > col

    def active(slot):
        return slot * n_row + row > col

    def needs(slot, chip):
        return 2 * chip <= slot * n_row + row

    def carries(slot, chip, source):
        return jnp.logical_or(
            needs(slot, chip), jnp.logical_and(chip == 1, source >= 2))

    def direct(slot, chip, source):
        return jnp.logical_and(
            carries(slot, chip, source),
            jnp.logical_or(chip > 0, source < 2))

    def chip_at(step):
        over = (z + step) // n_z
        return z + step + over * (n_z - 1 - 2 * step - z)

    def wants_column(at_row):
        return last + at_row > col

    def remote(src, dst, send, recv, to_row, to_col):
        return pltpu.make_async_remote_copy(
            src_ref=src, dst_ref=dst, send_sem=send, recv_sem=recv,
            device_id=(to_row, to_col), device_id_type=MESH)

    def loc_copy(source, target):
        return remote(loc_all.at[source], loc_all.at[source], loc_send.at[target],
                      loc_recv.at[source], row, target)

    def pv_copy(slot, source, target):
        return remote(pv_all.at[source, slot], pv_all.at[source, slot],
                      pv_send.at[slot, target], pv_recv.at[slot, source], target, col)

    def pu_copy(slot, block, send, target):
        return remote(pu_all.at[block, slot], pu_all.at[block, slot], send,
                      pu_recv.at[slot, block], row, target)

    def pu_direct(slot, chip):
        return pu_copy(slot, col, pu_send.at[slot, chip], 2 * chip + core)

    def pu_partner(slot, block):
        return pu_copy(slot, block, pf_send.at[slot, block], partner)

    def pu_relay(slot, block):
        return pu_copy(slot, block, pr_send.at[slot, block], core)

    def pj_copy(block, way):
        src = pj_all.at[block] if way == 2 else pu_all.at[block, owner_slot]
        return remote(src, pj_all.at[block], pj_send.at[way, block], pj_recv.at[block],
                      (x_row, y_row, x_row, diagonal)[way], col)

    def gx_copy(batch):
        chips = pl.ds(batch * half_z, half_z)
        return remote(g_part.at[other, chips], g_peer.at[chips], gx_send.at[batch],
                      gx_recv.at[batch], row, partner)

    def g_copy(source, chip):
        return remote(g_sum.at[chip], g_all.at[source], g_send.at[chip], g_recv.at[source],
                      row, 2 * chip + core)

    def when(*terms):
        return pl.when(functools.reduce(jnp.logical_and, terms))

    to_y = jnp.logical_or(wants_column(y_row), wants_column(diagonal))
    y_of_owner = row == (owner_row + half_z) % n_row
    is_relay = jnp.logical_and(y_of_owner, wants_column(x_row))

    barrier = pltpu.get_barrier_semaphore()

    def hello(semaphore, to_row, to_col):
        pl.semaphore_signal(semaphore, inc=1, device_id=(to_row, to_col), device_id_type=MESH)

    for step in range(1, n_row):
        hello(barrier, (row + step) % n_row, col)
    hello(barrier, row, partner)
    for chip in range(1, n_z):
        @pl.when(z < chip)
        def _(chip=chip):
            hello(barrier, row, 2 * chip)
            hello(barrier, row, 2 * chip + 1)

    loads = [
        pltpu.make_async_copy(locs, loc_all.at[col, pl.ds(0, slots)], load_sem.at[0]),
        pltpu.make_async_copy(pend, loc_all.at[col, slots], load_sem.at[1]),
        pltpu.make_async_copy(panel_v, pv_all.at[row], load_sem.at[2]),
        pltpu.make_async_copy(panel_u, pu_all.at[col], load_sem.at[3]),
        pltpu.make_async_copy(sketch, sk_buf, load_sem.at[4]),
        pltpu.make_async_copy(ranks_hbm, ranks, load_sem.at[5]),
    ]
    for load in loads:
        load.start()

    def trail_load(slot, which):
        src, dst = ((trail_u, u_buf), (trail_v, v_buf))[which]
        return pltpu.make_async_copy(src.at[slot], dst.at[slot], trail_sem.at[slot, which])

    for slot in range(slots):
        @pl.when(active(slot))
        def _(slot=slot):
            trail_load(slot, 0).start()
            trail_load(slot, 1).start()

    for load in loads:
        load.wait()
    sk_high, sk_low = halves(sk_buf[...])
    for block in range(n_col):
        sk_both[block, 0:rank_dim] = sk_high[:, block * w:(block + 1) * w]
        sk_both[block, rank_dim:2 * rank_dim] = sk_low[:, block * w:(block + 1) * w]

    acc[...] = jnp.zeros_like(acc)
    row_sketch[...] = jnp.zeros_like(row_sketch)
    col_sketch[...] = jnp.zeros_like(col_sketch)
    own_points[0:1, :] = jnp.concatenate(
        [loc_all[col, slot, 0:1] for slot in range(slots)] + [loc_all[col, slots, 0:1]] * slots,
        axis=1) * point_scale
    own_points[1:2, :] = jnp.concatenate(
        [loc_all[col, slot, 1:2] for slot in range(slots)] + [loc_all[col, slots, 1:2]] * slots,
        axis=1) * point_scale
    pad_rows = points.shape[2] - 2 * slots - 2

    def chunk(step):
        block = 2 * chip_at(step // 2) + (core + step) % 2

        @pl.when(step > 0)
        def _():
            loc_copy(block, partner).wait_recv()

        stack = [loc_all[block, slot] for slot in range(slots + 1)]
        if pad_rows:
            stack.append(jnp.zeros((pad_rows, w), jnp.float32))
        points[0] = jnp.concatenate(stack, axis=0).T * point_scale

        @pl.loop(0, w // SLAB, unroll=UNROLL)
        def _(slab):
            rows = pl.ds(pl.multiple_of(slab * SLAB, SLAB), SLAB)
            at = points[0, rows, :]
            for part in range(2 * slots):
                base = 2 * slots if part < slots else 2 * (part - slots)
                lanes = slice(part * w, (part + 1) * w)
                delta_x = at[:, base:base + 1] - own_points[0:1, lanes]
                delta_y = at[:, base + 1:base + 2] - own_points[1:2, lanes]
                square = delta_x * delta_x + delta_y * delta_y
                scaled = square * lax.rsqrt(jnp.maximum(square, smallest))
                value = (1.0 + scaled) * jnp.exp2(scaled * -log2_e)
                high, low = halves(value)
                mat_high[rows, lanes] = high
                mat_low[rows, lanes] = low

        sk = sk_both[block]
        both = product(sk, mat_high[...], NN)
        acc[...] += (both[:rank_dim] + both[rank_dim:]
                     + product(sk[:rank_dim], mat_low[...], NN))

    def chunks(first, final):
        pl.loop(first * n_col // 8, final * n_col // 8)(chunk)

    def sketch_of(block, high, low):
        sk = sk_both[block]
        both = product(sk, high, NT)
        return both[:rank_dim] + both[rank_dim:] + product(sk[:rank_dim], low, NT)

    def own_sketch(slot):
        trail_load(slot, 0).wait()
        trail_load(slot, 1).wait()
        in_use = lax.broadcasted_iota(jnp.int32, (rank_dim, 1), 0) < ranks[slot]
        v_sketch = jnp.zeros((rank_dim, rank_dim), jnp.float32)
        u_sketch = jnp.zeros((rank_dim, rank_dim), jnp.float32)
        for block in range(n_col):
            lanes = slice(block * w, (block + 1) * w)
            high, low = halves(v_buf[slot, :, lanes])
            rv[slot, 0, :, lanes] = high
            rv[slot, 1, :, lanes] = low
            v_sketch += sketch_of(block, high, low)
            high, low = halves(jnp.where(in_use, u_buf[slot, :, lanes], 0.0))
            ru[slot, 0, :, lanes] = high
            ru[slot, 1, :, lanes] = low
            u_sketch += sketch_of(block, high, low)
        own_sketches[slot, 0] = v_sketch
        own_sketches[slot, 1] = u_sketch

    def own_all():
        for slot in range(slots):
            @pl.when(active(slot))
            def _(slot=slot):
                own_sketch(slot)

    corner = (n_row - row) // n_row
    pl.loop(0, corner)(chunk)

    @pl.when(corner == 1)
    def _():
        own_all()
    pl.semaphore_wait(barrier, n_row + 2 * z)

    for chip in range(n_z - 1):
        @pl.when(z > chip)
        def _(chip=chip):
            hello(far_sem, row, 2 * chip)
            hello(far_sem, row, 2 * chip + 1)

    def each_loc(act, higher):
        for chip in range(n_z):
            @pl.when(z < chip if higher else z > chip)
            def _(chip=chip):
                act(loc_copy(col, 2 * chip))
                act(loc_copy(col, 2 * chip + 1))

    def each_direct(act, higher, slot):
        for chip in (range(1, n_z) if higher else reversed(range(n_z - 1))):
            @when(z < chip if higher else z > chip, direct(slot, chip, z))
            def _(chip=chip):
                act(pu_direct(slot, chip))

    def each_pv(act, slot):
        for step in range(1, n_row):
            target = (row + step) % n_row

            @pl.when(last + target > slot * n_row + row)
            def _(target=target):
                act(pv_copy(slot, row, target))

    def each_column(act, block, step, slot=None):
        ours = is_owner if slot is None else jnp.logical_and(is_owner, owner_slot == slot)
        final = step == n_z - 1

        @when(ours, wants_column(x_row))
        def _():
            act(pj_copy(block, 0))

        @when(ours, wants_column(y_row) if final else to_y)
        def _():
            act(pj_copy(block, 1))

        if final:
            @when(ours, wants_column(diagonal))
            def _():
                act(pj_copy(block, 3))

    def start(copy):
        copy.start()

    def wait_send(copy):
        copy.wait_send()

    def send_lower(slot):
        each_direct(start, False, slot)

        @pl.when(needs(slot, z))
        def _():
            start(pu_partner(slot, col))

    start(loc_copy(col, partner))
    each_loc(start, False)
    each_pv(start, 0)
    send_lower(0)
    def arrive(slot, step):
        chip = chip_at(step)
        block = 2 * chip + core

        @pl.when(carries(slot, z, chip))
        def _():
            pu_partner(slot, block).wait_recv()

            @when(z == 1, chip >= 2)
            def _():
                pu_relay(slot, block).start()

            @pl.when(needs(slot, z))
            def _():
                pu_partner(slot, block).start()
            each_column(start, block, step, slot)

    def spreads(slot):
        return jnp.logical_and(is_owner, owner_slot == slot)

    def from_partner(slot, step):
        block = 2 * chip_at(step) + other

        @when(needs(slot, z), spreads(slot))
        def _():
            pu_partner(slot, block).wait_recv()
            each_column(start, block, step, slot)

    def settle_rows(slot, first, final):
        @when(needs(slot, z), jnp.logical_not(spreads(slot)))
        def _():
            for step in range(first, final):
                pu_partner(slot, 2 * chip_at(step) + other).wait_recv()
        absorb_rows(slot, first, final)

    def pair(step):
        return [2 * chip_at(step) + (core + flip) % 2 for flip in range(2)]

    def column(step):
        @pl.when(is_relay)
        def _():
            for block in pair(step):
                pj_copy(block, 0).wait_recv()
                pj_copy(block, 2).start()

    def settle_column(first, final):
        for step in range(first, final):
            late = step == n_z - 1

            @when(jnp.logical_not(is_owner), wants_column(row),
                  True if late else jnp.logical_not(is_relay))
            def _(step=step):
                for block in pair(step):
                    pj_copy(block, 0).wait_recv()
        absorb_column(first, final)

    def gram_part(slot):
        own_v = pv_all[row].reshape(slots * rank_dim, w)
        own_high, own_low = halves(own_v)
        for source in range(n_row):
            tile = slot * n_row + source

            @pl.when(last + row > tile)
            def _(source=source, tile=tile):
                @pl.when(row != source)
                def _():
                    pv_copy(slot, source, row).wait_recv()
                high, low = halves(pv_all[source, slot])
                both = product(jnp.concatenate([high, low], axis=0), own_high, NT)
                g_part[tile % 2, tile // 2] = (
                    both[:rank_dim] + both[rank_dim:] + product(high, own_low, NT))

    def has_batch(batch):
        return last + row > batch * n_row

    def gram_swap(batch):
        @pl.when(has_batch(batch))
        def _():
            gx_copy(batch).start()

    def gram_sum(batch):
        @pl.when(has_batch(batch))
        def _():
            gx_copy(batch).wait_recv()
            for chip in range(batch * half_z, (batch + 1) * half_z):
                g_sum[chip] = g_part[core, chip] + g_peer[chip]

    def each_gram(act, batch):
        for chip in range(batch * half_z, (batch + 1) * half_z):
            @when(last + row > 2 * chip + core, z != chip)
            def _(chip=chip):
                act(g_copy(z, chip))

    def blocks_of(first, final):
        return [2 * chip_at(step) + flip for step in range(first, final) for flip in range(2)]

    def absorb_rows(slot, first, final):
        @pl.when(active(slot))
        def _():
            total = row_sketch[slot]
            for block in blocks_of(first, final):
                lanes = pl.ds(pl.multiple_of(block * w, w), w)
                high, low = halves(pu_all[block, slot])
                rp[slot, 0, :, lanes] = high
                rp[slot, 1, :, lanes] = low
                total += sketch_of(block, high, low)
            row_sketch[slot] = total

    def absorb_column(first, final):
        @pl.when(any_active)
        def _():
            @pl.when(is_owner)
            def _():
                for block in blocks_of(first, final):
                    pj_all[block] = pu_all[block, owner_slot]
            total = col_sketch[...]
            for block in blocks_of(first, final):
                lanes = pl.ds(pl.multiple_of(block * w, w), w)
                high, low = halves(pj_all[block])
                rj[0, :, lanes] = high
                rj[1, :, lanes] = low
                total += sketch_of(block, high, low)
            col_sketch[...] = total

    def upward():
        @pl.when(z < n_z - 1)
        def _():
            pl.semaphore_wait(far_sem, 2 * (n_z - 1 - z))
        each_loc(start, True)
        for slot in range(slots):
            each_direct(start, True, slot)

    pl.loop(corner, 2)(chunk)
    for slot in range(1, slots):
        send_lower(slot)

    @pl.when(corner == 0)
    def _():
        own_all()
    upward()
    arrive(0, 1)
    each_column(start, col, 0)
    from_partner(0, 0)
    chunks(2, 3)
    gram_part(0)
    for slot in range(1, slots):
        each_pv(start, slot)
    arrive(0, 2)
    gram_swap(0)
    from_partner(0, 1)
    chunks(3, 4)
    gram_sum(0)
    for slot in range(1, slots):
        arrive(slot, 1)
        from_partner(slot, 0)
    each_gram(start, 0)
    column(0)
    chunks(4, 5)
    for slot in range(1, slots):
        arrive(slot, 2)
    arrive(0, 3)
    from_partner(0, 2)
    for slot in range(1, slots):
        from_partner(slot, 1)
    column(1)
    chunks(5, 6)
    from_partner(0, 3)
    for slot in range(1, slots):
        from_partner(slot, 2)
    column(2)
    for slot in range(1, slots):
        gram_part(slot)
    settle_rows(0, 0, n_z - 1)
    for slot in range(1, slots):
        gram_swap(slot)
    chunks(6, 7)
    for slot in range(1, slots):
        arrive(slot, 3)
        gram_sum(slot)
    chunks(7, 8)
    for slot in range(1, slots):
        each_gram(start, slot)
        from_partner(slot, 3)
        settle_rows(slot, 0, n_z - 1)
    settle_rows(0, n_z - 1, n_z)
    settle_column(0, n_z - 1)
    pend_acc[...] = acc[...] * matern_scale

    wait_send(loc_copy(col, partner))
    for higher in (False, True):
        each_loc(wait_send, higher)
        for slot in range(slots):
            each_direct(wait_send, higher, slot)
    for slot in range(slots):
        each_pv(wait_send, slot)
    settle_column(n_z - 1, n_z)
    for slot in range(1, slots):
        settle_rows(slot, n_z - 1, n_z)

    @pl.when(any_active)
    def _():
        gram = g_sum[z]
        for step in range(1, n_z):
            chip = chip_at(step)
            g_copy(chip, z).wait_recv()
            gram = gram + g_all[chip]
        left_core = dot3(col_sketch[...], gram, NN)
        nothing = jnp.zeros((rank_dim, 2 * rank_dim), jnp.bfloat16)

        def stacked(value):
            high, low = halves(value)
            return jnp.concatenate([
                jnp.concatenate([high, high], axis=1), jnp.concatenate([low, nothing], axis=1)
            ], axis=0)

        for slot in range(slots):
            lanes = slice(slot * rank_dim, (slot + 1) * rank_dim)

            @pl.when(active(slot))
            def _(slot=slot, lanes=lanes):
                right_core = dot3(row_sketch[slot], gram[:, lanes], NT)
                y_left[slot] = stacked(
                    jnp.concatenate([own_sketches[slot, 0], -left_core[:, lanes]], axis=1))
                z_left[slot] = stacked(
                    jnp.concatenate([own_sketches[slot, 1], -right_core], axis=1))

    for slot in range(slots):
        each_gram(wait_send, slot)

        @pl.when(has_batch(slot))
        def _(slot=slot):
            gx_copy(slot).wait_send()
        for step in range(n_z):
            block = 2 * chip_at(step) + core

            @pl.when(needs(slot, z))
            def _(slot=slot, block=block):
                pu_partner(slot, block).wait_send()

            @when(z == 1, chip_at(step) >= 2)
            def _(slot=slot, block=block):
                pu_relay(slot, block).wait_send()
    for step in range(n_z):
        for block in pair(step):
            each_column(wait_send, block, step)
        if step < n_z - 1:
            @pl.when(is_relay)
            def _(step=step):
                for block in pair(step):
                    pj_copy(block, 2).wait_send()


def finish(
    n_row, ru, rv, rp, rj, y_left, z_left, pend_acc,
    trail_y, trail_z, pend_y, pend_z,
    y_buf, z_buf, out_sem, pend_sem,
):
    row, col = lax.axis_index("row"), lax.axis_index("col")
    slots, _, rank_dim, width = ru.shape
    w = pend_y.shape[3]
    pieces = out_sem.shape[2]
    span = width // pieces

    def pend_copy(slot, which):
        lanes = pl.ds((which * slots + slot) * w, w)
        return pltpu.make_async_copy(
            pend_acc.at[:, lanes], (pend_y, pend_z)[which].at[slot, 0], pend_sem.at[slot, which])

    def out_copy(slot, which, piece):
        lanes = pl.ds(piece * span, span)
        src, dst = ((y_buf, trail_y), (z_buf, trail_z))[which]
        return pltpu.make_async_copy(
            src.at[slot, :, lanes], dst.at[slot, 0, 0, :, lanes], out_sem.at[slot, which, piece])

    for slot in range(slots):
        pend_copy(slot, 0).start()
        pend_copy(slot, 1).start()

    for slot in range(slots):
        active = slot * n_row + row > col

        @pl.when(jnp.logical_not(active))
        def _(slot=slot):
            y_buf[slot] = jnp.zeros((rank_dim, width), jnp.float32)
            z_buf[slot] = jnp.zeros((rank_dim, width), jnp.float32)
            for which in range(2):
                for piece in range(pieces):
                    out_copy(slot, which, piece).start()

        @pl.when(active)
        def _(slot=slot):
            for which in range(2):
                left = (y_left, z_left)[which][slot]
                first = (ru, rv)[which]
                buf = (y_buf, z_buf)[which]
                for piece in range(pieces):
                    lanes = slice(piece * span, (piece + 1) * span)
                    second = [rj[part, :, lanes] if which else rp[slot, part, :, lanes]
                              for part in range(2)]
                    right = jnp.concatenate(
                        [first[slot, 0, :, lanes], second[0], first[slot, 1, :, lanes], second[1]],
                        axis=0)
                    both = product(left, right, NN)
                    buf[slot, :, lanes] = both[:rank_dim] + both[rank_dim:]
                    out_copy(slot, which, piece).start()

    for slot in range(slots):
        for which in range(2):
            pend_copy(slot, which).wait()
            for piece in range(pieces):
                out_copy(slot, which, piece).wait()


def broadcast(block, axis, owner):
    block = jnp.where(lax.axis_index(axis) == owner, block, jnp.zeros_like(block))
    return lax.psum(block, axis)


def matmul(left, right):
    return jnp.dot(left, right, precision=lax.Precision.HIGHEST, preferred_element_type=jnp.float32)


def batched(form, left, right):
    return jnp.einsum(
        form, left, right, precision=lax.Precision.HIGHEST, preferred_element_type=jnp.float32
    )


def matern(row_points, col_points):
    delta_x = row_points[0][:, None] - col_points[0][None, :]
    delta_y = row_points[1][:, None] - col_points[1][None, :]
    distance = jnp.sqrt(delta_x * delta_x + delta_y * delta_y)
    scaled = root_three * distance / length_scale
    return matern_scale * (1.0 + scaled) * jnp.exp(-scaled)


def plain_on_device(trail_u, trail_v, ranks, panel_u, panel_v, locations, pend_locs, sketch):
    row_count = lax.axis_size("row")
    row_index = lax.axis_index("row")
    col_index = lax.axis_index("col")
    row_slots = trail_u.shape[0]
    rank_dim = trail_u.shape[3]
    width = trail_u.shape[4]
    local_width = pend_locs.shape[1]
    gathered_u, gathered_v = (
        lax.all_gather(panel_u, "col", axis=3, tiled=True),
        lax.all_gather(panel_v, "col", axis=3, tiled=True),
    )
    slot_index = col_index // row_count
    own_u = lax.dynamic_index_in_dim(gathered_u[:, 0], slot_index, 0, keepdims=False)
    own_v = lax.dynamic_index_in_dim(gathered_v[:, 0], slot_index, 0, keepdims=False)
    col_pu, col_pv = (
        broadcast(own_u, "row", col_index % row_count),
        broadcast(own_v, "row", col_index % row_count),
    )
    rank_iota = lax.broadcasted_iota(jnp.int32, (row_slots, rank_dim), 1)
    in_use = (rank_iota < ranks[:, 0, 0][:, None]).astype(jnp.float32)
    u_tiles = trail_u[:, 0, 0] * in_use[:, :, None]
    v_tiles = trail_v[:, 0, 0]
    row_pu = gathered_u[:, 0]
    row_pv = gathered_v[:, 0]
    v_sketch = batched("tkn,ln->tkl", v_tiles, sketch)
    u_sketch = batched("tkn,ln->tkl", u_tiles, sketch)
    cross_gram = batched("tkn,ln->tkl", row_pv, col_pv)
    col_sketch = matmul(col_pu, sketch.T)
    row_sketch = batched("tkn,ln->tkl", row_pu, sketch)
    left_core = batched("tkm,ml->tkl", cross_gram, col_sketch)
    y_tiles = batched("tkl,tkn->tln", v_sketch, u_tiles) - batched(
        "tkl,tkn->tln", left_core, row_pu
    )
    right_core = batched("tkl,tkm->tlm", row_sketch, cross_gram)
    z_tiles = batched("tkl,tkn->tln", u_sketch, v_tiles) - batched(
        "tlm,mn->tln", right_core, col_pu
    )
    tile_rows = jnp.arange(row_slots, dtype=jnp.int32) * row_count + row_index
    keep_mask = (tile_rows > col_index)[:, None, None]
    trail_y = jnp.where(keep_mask, y_tiles, 0.0).reshape(row_slots, 1, 1, rank_dim, width)
    trail_z = jnp.where(keep_mask, z_tiles, 0.0).reshape(row_slots, 1, 1, rank_dim, width)
    y_list = []
    z_list = []
    rows_all, pend_all = (
        lax.all_gather(locations, "col", axis=3, tiled=True),
        lax.all_gather(pend_locs.reshape(1, 1, 2, local_width), "col", axis=3, tiled=True),
    )
    col_points = pend_all[0, 0]
    for slot_num in range(row_slots):
        own_kernel = matern(locations[slot_num, 0], col_points)
        y_list.append(matmul(sketch, own_kernel.T))
        col_kernel = matern(rows_all[slot_num, 0], pend_locs)
        z_list.append(matmul(sketch, col_kernel))
    pend_y = jnp.stack(y_list)
    pend_z = jnp.stack(z_list)
    pend_y = pend_y.reshape(row_slots, 1, rank_dim, local_width)
    pend_z = pend_z.reshape(row_slots, 1, rank_dim, local_width)
    return (trail_y, trail_z, pend_y, pend_z)


def on_device(n_row, n_col, trail_u, trail_v, ranks, panel_u, panel_v, locations, pend_locs, sketch):
    slots, _, _, rank_dim, width = trail_u.shape
    w = pend_locs.shape[1]
    n_z = n_col // 2
    fits = n_col == slots * n_row and n_row == 4 and slots == 2
    if w % 128 or rank_dim % 16 or not fits:
        return plain_on_device(
            trail_u, trail_v, ranks, panel_u, panel_v, locations, pend_locs, sketch
        )
    flat = slots * rank_dim
    f32, bf16 = jnp.float32, jnp.bfloat16
    dma = pltpu.SemaphoreType.DMA
    vmem = pl.BlockSpec(memory_space=pltpu.VMEM)
    hbm = pl.BlockSpec(memory_space=pltpu.HBM)
    point_rows = -(-(2 * slots + 2) // 8) * 8
    shape = jax.ShapeDtypeStruct
    kept = pl.pallas_call(
        functools.partial(kernel, n_row, n_col),
        out_shape=(
            pltpu.VMEM((slots, 2, rank_dim, width), bf16),
            pltpu.VMEM((slots, 2, rank_dim, width), bf16),
            pltpu.VMEM((slots, 2, rank_dim, width), bf16),
            pltpu.VMEM((2, rank_dim, width), bf16),
            pltpu.VMEM((slots, 2 * rank_dim, 4 * rank_dim), bf16),
            pltpu.VMEM((slots, 2 * rank_dim, 4 * rank_dim), bf16),
            pltpu.VMEM((rank_dim, 2 * slots * w), f32),
        ),
        in_specs=[hbm] * 8,
        out_specs=(vmem,) * 7,
        scratch_shapes=[
            pltpu.SMEM((slots,), jnp.int32),
            pltpu.VMEM((slots, rank_dim, width), f32),
            pltpu.VMEM((slots, rank_dim, width), f32),
            pltpu.VMEM((rank_dim, width), f32),
            pltpu.VMEM((n_col, slots + 1, 2, w), f32),
            pltpu.VMEM((n_col, slots, rank_dim, w), f32),
            pltpu.VMEM((n_col, rank_dim, w), f32),
            pltpu.VMEM((n_row, slots, rank_dim, w), f32),
            pltpu.VMEM((2, n_z, rank_dim, flat), f32),
            pltpu.VMEM((n_z, rank_dim, flat), f32),
            pltpu.VMEM((n_z, rank_dim, flat), f32),
            pltpu.VMEM((n_z, rank_dim, flat), f32),
            pltpu.VMEM((1, w, point_rows), f32),
            pltpu.VMEM((2, 2 * slots * w), f32),
            pltpu.VMEM((n_col, 2 * rank_dim, w), bf16),
            pltpu.VMEM((w, 2 * slots * w), bf16),
            pltpu.VMEM((w, 2 * slots * w), bf16),
            pltpu.VMEM((rank_dim, 2 * slots * w), f32),
            pltpu.VMEM((slots, 2, rank_dim, rank_dim), f32),
            pltpu.VMEM((slots, rank_dim, rank_dim), f32),
            pltpu.VMEM((rank_dim, rank_dim), f32),
            pltpu.SemaphoreType.REGULAR,
            dma((6,)), dma((slots, 2)), dma((n_col,)), dma((n_col,)),
            dma((slots, n_z)), dma((slots, n_col)), dma((slots, n_col)), dma((slots, n_col)),
            dma((slots, n_row)), dma((slots, n_row)),
            dma((4, n_col)), dma((n_col,)),
            dma((slots,)), dma((slots,)), dma((n_z,)), dma((n_z,)),
        ],
        compiler_params=pltpu.CompilerParams(
            collective_id=0, has_side_effects=True, vmem_limit_bytes=VMEM_LIMIT),
    )(*[
        pltpu.with_memory_space_constraint(value, pltpu.HBM) for value in (
            ranks.reshape(slots),
            trail_u.reshape(slots, rank_dim, width),
            trail_v.reshape(slots, rank_dim, width),
            panel_u.reshape(slots, rank_dim, w),
            panel_v.reshape(slots, rank_dim, w),
            locations.reshape(slots, 2, w),
            pend_locs,
            sketch,
        )
    ])
    kept = [pltpu.with_memory_space_constraint(value, pltpu.VMEM) for value in kept]
    pieces = 2
    return pl.pallas_call(
        functools.partial(finish, n_row),
        out_shape=(
            shape((slots, 1, 1, rank_dim, width), f32),
            shape((slots, 1, 1, rank_dim, width), f32),
            shape((slots, 1, rank_dim, w), f32),
            shape((slots, 1, rank_dim, w), f32),
        ),
        in_specs=[vmem] * 7,
        out_specs=(hbm,) * 4,
        scratch_shapes=[
            pltpu.VMEM((slots, rank_dim, width), f32),
            pltpu.VMEM((slots, rank_dim, width), f32),
            dma((slots, 2, pieces)), dma((slots, 2)),
        ],
        compiler_params=pltpu.CompilerParams(vmem_limit_bytes=VMEM_LIMIT),
    )(*kept)


def solution(mesh):
    in_specs = (
        P(None, "row", "col", None, None),
        P(None, "row", "col", None, None),
        P(None, "row", "col"),
        P(None, "row", None, "col"),
        P(None, "row", None, "col"),
        P(None, "row", None, "col"),
        P(None, "col"),
        P(),
    )
    out_specs = (
        P(None, "row", "col", None, None),
        P(None, "row", "col", None, None),
        P(None, "row", None, "col"),
        P(None, "row", None, "col"),
    )
    body = functools.partial(on_device, mesh.shape["row"], mesh.shape["col"])
    return jax.shard_map(
        body, mesh=mesh, in_specs=in_specs, out_specs=out_specs, check_vma=False
    )
```

```python
import functools
import math

import jax
import jax.numpy as jnp
from jax import lax
from jax.experimental import pallas as pl
from jax.experimental.pallas import tpu as pltpu
from jax.sharding import PartitionSpec as P

matern_scale = 4.0
length_scale = 0.15
root_three = math.sqrt(3.0)
point_scale = root_three / length_scale
log2_e = math.log2(math.e)
smallest = 1e-30

MESH = pl.DeviceIdType.MESH
NN = (((1,), (0,)), ((), ()))
NT = (((1,), (1,)), ((), ()))
SLAB = 16
UNROLL = 8
VMEM_LIMIT = 32 << 20


def halves(value):
    high = value.astype(jnp.bfloat16)
    low = (value - high.astype(jnp.float32)).astype(jnp.bfloat16)
    return high, low


def product(left, right, dims):
    return lax.dot_general(left, right, dims, preferred_element_type=jnp.float32)


def dot3_split(left_both, right, dims):
    rows = left_both.shape[0] // 2
    right_high, right_low = halves(right)
    both = product(left_both, right_high, dims)
    return both[:rows] + both[rows:] + product(left_both[:rows], right_low, dims)


def dot3(left, right, dims):
    left_high, left_low = halves(left)
    return dot3_split(jnp.concatenate([left_high, left_low], axis=0), right, dims)


def kernel(
    n_row, n_col,
    ranks_hbm, trail_u, trail_v, panel_u, panel_v, locs, pend, sketch,
    ru, rv, rp, rj, y_left, z_left, pend_acc,
    ranks, u_buf, v_buf, sk_buf, loc_all, pu_all, pj_all, pv_all, g_part, g_peer, g_sum, g_all,
    points, own_points, sk_both, mat_high, mat_low, acc, own_sketches, row_sketch, col_sketch,
    far_sem, load_sem, trail_sem, loc_send, loc_recv, pu_send, pf_send, pr_send, pu_recv,
    pv_send, pv_recv, pj_send, pj_recv, gx_send, gx_recv, g_send, g_recv,
):
    row, col = lax.axis_index("row"), lax.axis_index("col")
    n_z = n_col // 2
    z, core = col // 2, col % 2
    other = 1 - core
    partner = 2 * z + other
    slots, rank_dim, width = u_buf.shape
    w = pu_all.shape[3]
    half_z = n_row // 2
    last = (slots - 1) * n_row
    owner_row, owner_slot = col % n_row, col // n_row
    is_owner = row == owner_row
    x_row = row + 1 - 2 * (row % 2)
    y_row = (row + half_z) % n_row
    diagonal = n_row - 1 - row
    any_active = last + row > col

    def active(slot):
        return slot * n_row + row > col

    def needs(slot, chip):
        return 2 * chip <= slot * n_row + row

    def carries(slot, chip, source):
        return jnp.logical_or(
            needs(slot, chip), jnp.logical_and(chip == 1, source >= 2))

    def direct(slot, chip, source):
        return jnp.logical_and(
            carries(slot, chip, source),
            jnp.logical_or(chip > 0, source < 2))

    def chip_at(step):
        over = (z + step) // n_z
        return z + step + over * (n_z - 1 - 2 * step - z)

    def wants_column(at_row):
        return last + at_row > col

    def remote(src, dst, send, recv, to_row, to_col):
        return pltpu.make_async_remote_copy(
            src_ref=src, dst_ref=dst, send_sem=send, recv_sem=recv,
            device_id=(to_row, to_col), device_id_type=MESH)

    def loc_copy(source, target):
        return remote(loc_all.at[source], loc_all.at[source], loc_send.at[target],
                      loc_recv.at[source], row, target)

    def pv_copy(slot, source, target):
        return remote(pv_all.at[source, slot], pv_all.at[source, slot],
                      pv_send.at[slot, target], pv_recv.at[slot, source], target, col)

    def pu_copy(slot, block, send, target):
        return remote(pu_all.at[block, slot], pu_all.at[block, slot], send,
                      pu_recv.at[slot, block], row, target)

    def pu_direct(slot, chip):
        return pu_copy(slot, col, pu_send.at[slot, chip], 2 * chip + core)

    def pu_partner(slot, block):
        return pu_copy(slot, block, pf_send.at[slot, block], partner)

    def pu_relay(slot, block):
        return pu_copy(slot, block, pr_send.at[slot, block], core)

    def pj_copy(block, way):
        src = pj_all.at[block] if way == 2 else pu_all.at[block, owner_slot]
        return remote(src, pj_all.at[block], pj_send.at[way, block], pj_recv.at[block],
                      (x_row, y_row, x_row, diagonal)[way], col)

    def gx_copy(batch):
        chips = pl.ds(batch * half_z, half_z)
        return remote(g_part.at[other, chips], g_peer.at[chips], gx_send.at[batch],
                      gx_recv.at[batch], row, partner)

    def g_copy(source, chip):
        return remote(g_sum.at[chip], g_all.at[source], g_send.at[chip], g_recv.at[source],
                      row, 2 * chip + core)

    def when(*terms):
        return pl.when(functools.reduce(jnp.logical_and, terms))

    to_y = jnp.logical_or(wants_column(y_row), wants_column(diagonal))
    y_of_owner = row == (owner_row + half_z) % n_row
    is_relay = jnp.logical_and(y_of_owner, wants_column(x_row))

    barrier = pltpu.get_barrier_semaphore()

    def hello(semaphore, to_row, to_col):
        pl.semaphore_signal(semaphore, inc=1, device_id=(to_row, to_col), device_id_type=MESH)

    for step in range(1, n_row):
        hello(barrier, (row + step) % n_row, col)
    hello(barrier, row, partner)
    for chip in range(1, n_z):
        @pl.when(z < chip)
        def _(chip=chip):
            hello(barrier, row, 2 * chip)
            hello(barrier, row, 2 * chip + 1)

    loads = [
        pltpu.make_async_copy(locs, loc_all.at[col, pl.ds(0, slots)], load_sem.at[0]),
        pltpu.make_async_copy(pend, loc_all.at[col, slots], load_sem.at[1]),
        pltpu.make_async_copy(panel_v, pv_all.at[row], load_sem.at[2]),
        pltpu.make_async_copy(panel_u, pu_all.at[col], load_sem.at[3]),
        pltpu.make_async_copy(sketch, sk_buf, load_sem.at[4]),
        pltpu.make_async_copy(ranks_hbm, ranks, load_sem.at[5]),
    ]
    for load in loads:
        load.start()

    def trail_load(slot, which):
        src, dst = ((trail_u, u_buf), (trail_v, v_buf))[which]
        return pltpu.make_async_copy(src.at[slot], dst.at[slot], trail_sem.at[slot, which])

    for slot in range(slots):
        @pl.when(active(slot))
        def _(slot=slot):
            trail_load(slot, 0).start()
            trail_load(slot, 1).start()

    for load in loads:
        load.wait()
    sk_high, sk_low = halves(sk_buf[...])
    for block in range(n_col):
        sk_both[block, 0:rank_dim] = sk_high[:, block * w:(block + 1) * w]
        sk_both[block, rank_dim:2 * rank_dim] = sk_low[:, block * w:(block + 1) * w]

    acc[...] = jnp.zeros_like(acc)
    row_sketch[...] = jnp.zeros_like(row_sketch)
    col_sketch[...] = jnp.zeros_like(col_sketch)
    own_points[0:1, :] = jnp.concatenate(
        [loc_all[col, slot, 0:1] for slot in range(slots)] + [loc_all[col, slots, 0:1]] * slots,
        axis=1) * point_scale
    own_points[1:2, :] = jnp.concatenate(
        [loc_all[col, slot, 1:2] for slot in range(slots)] + [loc_all[col, slots, 1:2]] * slots,
        axis=1) * point_scale
    pad_rows = points.shape[2] - 2 * slots - 2

    def chunk(step):
        block = 2 * chip_at(step // 2) + (core + step) % 2

        @pl.when(step > 0)
        def _():
            loc_copy(block, partner).wait_recv()

        stack = [loc_all[block, slot] for slot in range(slots + 1)]
        if pad_rows:
            stack.append(jnp.zeros((pad_rows, w), jnp.float32))
        points[0] = jnp.concatenate(stack, axis=0).T * point_scale

        @pl.loop(0, w // SLAB, unroll=UNROLL)
        def _(slab):
            rows = pl.ds(pl.multiple_of(slab * SLAB, SLAB), SLAB)
            at = points[0, rows, :]
            for part in range(2 * slots):
                base = 2 * slots if part < slots else 2 * (part - slots)
                lanes = slice(part * w, (part + 1) * w)
                delta_x = at[:, base:base + 1] - own_points[0:1, lanes]
                delta_y = at[:, base + 1:base + 2] - own_points[1:2, lanes]
                square = delta_x * delta_x + delta_y * delta_y
                scaled = square * lax.rsqrt(jnp.maximum(square, smallest))
                value = (1.0 + scaled) * jnp.exp2(scaled * -log2_e)
                high, low = halves(value)
                mat_high[rows, lanes] = high
                mat_low[rows, lanes] = low

        sk = sk_both[block]
        both = product(sk, mat_high[...], NN)
        acc[...] += (both[:rank_dim] + both[rank_dim:]
                     + product(sk[:rank_dim], mat_low[...], NN))

    def chunks(first, final):
        pl.loop(first * n_col // 8, final * n_col // 8)(chunk)

    def sketch_of(block, high, low):
        sk = sk_both[block]
        both = product(sk, high, NT)
        return both[:rank_dim] + both[rank_dim:] + product(sk[:rank_dim], low, NT)

    def own_sketch(slot):
        trail_load(slot, 0).wait()
        trail_load(slot, 1).wait()
        in_use = lax.broadcasted_iota(jnp.int32, (rank_dim, 1), 0) < ranks[slot]
        v_sketch = jnp.zeros((rank_dim, rank_dim), jnp.float32)
        u_sketch = jnp.zeros((rank_dim, rank_dim), jnp.float32)
        for block in range(n_col):
            lanes = slice(block * w, (block + 1) * w)
            high, low = halves(v_buf[slot, :, lanes])
            rv[slot, 0, :, lanes] = high
            rv[slot, 1, :, lanes] = low
            v_sketch += sketch_of(block, high, low)
            high, low = halves(jnp.where(in_use, u_buf[slot, :, lanes], 0.0))
            ru[slot, 0, :, lanes] = high
            ru[slot, 1, :, lanes] = low
            u_sketch += sketch_of(block, high, low)
        own_sketches[slot, 0] = v_sketch
        own_sketches[slot, 1] = u_sketch

    def own_all():
        for slot in range(slots):
            @pl.when(active(slot))
            def _(slot=slot):
                own_sketch(slot)

    corner = (n_row - row) // n_row
    pl.loop(0, corner)(chunk)

    @pl.when(corner == 1)
    def _():
        own_all()
    pl.semaphore_wait(barrier, n_row + 2 * z)

    for chip in range(n_z - 1):
        @pl.when(z > chip)
        def _(chip=chip):
            hello(far_sem, row, 2 * chip)
            hello(far_sem, row, 2 * chip + 1)

    def each_loc(act, higher):
        for chip in range(n_z):
            @pl.when(z < chip if higher else z > chip)
            def _(chip=chip):
                act(loc_copy(col, 2 * chip))
                act(loc_copy(col, 2 * chip + 1))

    def each_direct(act, higher, slot):
        for chip in (range(1, n_z) if higher else reversed(range(n_z - 1))):
            @when(z < chip if higher else z > chip, direct(slot, chip, z))
            def _(chip=chip):
                act(pu_direct(slot, chip))

    def each_pv(act, slot):
        for step in range(1, n_row):
            target = (row + step) % n_row

            @pl.when(last + target > slot * n_row + row)
            def _(target=target):
                act(pv_copy(slot, row, target))

    def each_column(act, block, step, slot=None):
        ours = is_owner if slot is None else jnp.logical_and(is_owner, owner_slot == slot)
        final = step == n_z - 1

        @when(ours, wants_column(x_row))
        def _():
            act(pj_copy(block, 0))

        @when(ours, wants_column(y_row) if final else to_y)
        def _():
            act(pj_copy(block, 1))

        if final:
            @when(ours, wants_column(diagonal))
            def _():
                act(pj_copy(block, 3))

    def start(copy):
        copy.start()

    def wait_send(copy):
        copy.wait_send()

    def send_lower(slot):
        each_direct(start, False, slot)

        @pl.when(needs(slot, z))
        def _():
            start(pu_partner(slot, col))

    start(loc_copy(col, partner))
    each_loc(start, False)
    each_pv(start, 0)

    @pl.when(z < n_z - 1)
    def _():
        send_lower(0)

    @pl.when(z == 1)
    def _():
        for slot in range(1, slots):
            send_lower(slot)
    def arrive(slot, step):
        chip = chip_at(step)
        block = 2 * chip + core

        @pl.when(carries(slot, z, chip))
        def _():
            pu_partner(slot, block).wait_recv()

            @when(z == 1, chip >= 2)
            def _():
                pu_relay(slot, block).start()

            @pl.when(needs(slot, z))
            def _():
                pu_partner(slot, block).start()
            each_column(start, block, step, slot)

    def spreads(slot):
        return jnp.logical_and(is_owner, owner_slot == slot)

    def from_partner(slot, step):
        block = 2 * chip_at(step) + other

        @when(needs(slot, z), spreads(slot))
        def _():
            pu_partner(slot, block).wait_recv()
            each_column(start, block, step, slot)

    def settle_rows(slot, first, final):
        @when(needs(slot, z), jnp.logical_not(spreads(slot)))
        def _():
            for step in range(first, final):
                pu_partner(slot, 2 * chip_at(step) + other).wait_recv()
        absorb_rows(slot, first, final)

    def pair(step):
        return [2 * chip_at(step) + (core + flip) % 2 for flip in range(2)]

    def column(step):
        @pl.when(is_relay)
        def _():
            for block in pair(step):
                pj_copy(block, 0).wait_recv()
                pj_copy(block, 2).start()

    def settle_column(first, final):
        for step in range(first, final):
            late = step == n_z - 1

            @when(jnp.logical_not(is_owner), wants_column(row),
                  True if late else jnp.logical_not(is_relay))
            def _(step=step):
                for block in pair(step):
                    pj_copy(block, 0).wait_recv()
        absorb_column(first, final)

    def gram_part(slot):
        own_v = pv_all[row].reshape(slots * rank_dim, w)
        own_high, own_low = halves(own_v)
        for source in range(n_row):
            tile = slot * n_row + source

            @pl.when(last + row > tile)
            def _(source=source, tile=tile):
                @pl.when(row != source)
                def _():
                    pv_copy(slot, source, row).wait_recv()
                high, low = halves(pv_all[source, slot])
                both = product(jnp.concatenate([high, low], axis=0), own_high, NT)
                g_part[tile % 2, tile // 2] = (
                    both[:rank_dim] + both[rank_dim:] + product(high, own_low, NT))

    def has_batch(batch):
        return last + row > batch * n_row

    def gram_swap(batch):
        @pl.when(has_batch(batch))
        def _():
            gx_copy(batch).start()

    def gram_sum(batch):
        @pl.when(has_batch(batch))
        def _():
            gx_copy(batch).wait_recv()
            for chip in range(batch * half_z, (batch + 1) * half_z):
                g_sum[chip] = g_part[core, chip] + g_peer[chip]

    def each_gram(act, batch):
        for chip in range(batch * half_z, (batch + 1) * half_z):
            @when(last + row > 2 * chip + core, z != chip)
            def _(chip=chip):
                act(g_copy(z, chip))

    def blocks_of(first, final):
        return [2 * chip_at(step) + flip for step in range(first, final) for flip in range(2)]

    def absorb_rows(slot, first, final):
        @pl.when(active(slot))
        def _():
            total = row_sketch[slot]
            for block in blocks_of(first, final):
                lanes = pl.ds(pl.multiple_of(block * w, w), w)
                high, low = halves(pu_all[block, slot])
                rp[slot, 0, :, lanes] = high
                rp[slot, 1, :, lanes] = low
                total += sketch_of(block, high, low)
            row_sketch[slot] = total

    def absorb_column(first, final):
        @pl.when(any_active)
        def _():
            @pl.when(is_owner)
            def _():
                for block in blocks_of(first, final):
                    pj_all[block] = pu_all[block, owner_slot]
            total = col_sketch[...]
            for block in blocks_of(first, final):
                lanes = pl.ds(pl.multiple_of(block * w, w), w)
                high, low = halves(pj_all[block])
                rj[0, :, lanes] = high
                rj[1, :, lanes] = low
                total += sketch_of(block, high, low)
            col_sketch[...] = total

    def upward():
        @pl.when(z < n_z - 1)
        def _():
            pl.semaphore_wait(far_sem, 2 * (n_z - 1 - z))
        each_loc(start, True)
        for slot in range(slots):
            each_direct(start, True, slot)

    def early(slot, step):
        @pl.when(z > 0)
        def _():
            arrive(slot, step)

    def late(slot, step):
        @pl.when(z == 0)
        def _():
            arrive(slot, step)

    top = n_z - 1
    pl.loop(corner, 1)(chunk)

    @pl.when(z == top)
    def _():
        send_lower(0)
    chunks(1, 2)

    @when(z != 1, z < top)
    def _():
        for slot in range(1, slots):
            send_lower(slot)
    for slot in range(1, slots):
        each_pv(start, slot)
    each_column(start, col, 0)

    @pl.when(corner == 0)
    def _():
        own_all()
    upward()

    @pl.when(z == top)
    def _():
        for slot in range(1, slots):
            send_lower(slot)
    from_partner(0, 0)
    chunks(2, 3)
    for slot in range(1, slots):
        from_partner(slot, 0)
    arrive(0, 1)
    gram_part(0)
    from_partner(0, 1)
    early(0, 2)
    gram_swap(0)
    chunks(3, 4)
    gram_sum(0)
    for slot in range(1, slots):
        early(slot, 1)
    column(0)
    each_gram(start, 0)
    chunks(4, 5)
    for slot in range(1, slots):
        gram_part(slot)
        early(slot, 2)
        from_partner(slot, 1)
    late(0, 2)
    for slot in range(1, slots):
        gram_swap(slot)
    column(1)
    chunks(5, 6)
    for slot in range(1, slots):
        gram_sum(slot)
        late(slot, 1)
        from_partner(slot, 2)
    from_partner(0, 2)
    for slot in range(1, slots):
        each_gram(start, slot)
    arrive(0, 3)
    chunks(6, 7)
    column(2)
    for slot in range(1, slots):
        late(slot, 2)
        early(slot, 3)
    from_partner(0, 3)
    settle_rows(0, 0, n_z - 1)
    chunks(7, 8)
    for slot in range(1, slots):
        late(slot, 3)
        from_partner(slot, 3)
        settle_rows(slot, 0, n_z - 1)
    settle_rows(0, n_z - 1, n_z)
    settle_column(0, n_z - 1)
    pend_acc[...] = acc[...] * matern_scale

    wait_send(loc_copy(col, partner))
    for higher in (False, True):
        each_loc(wait_send, higher)
        for slot in range(slots):
            each_direct(wait_send, higher, slot)

    def forwards_done(slot, first, final):
        for step in range(first, final):
            block = 2 * chip_at(step) + core

            @pl.when(needs(slot, z))
            def _(block=block):
                pu_partner(slot, block).wait_send()

            @when(z == 1, chip_at(step) >= 2)
            def _(block=block):
                pu_relay(slot, block).wait_send()

    def columns_done(step):
        for block in pair(step):
            each_column(wait_send, block, step)
        if step < n_z - 1:
            @pl.when(is_relay)
            def _():
                for block in pair(step):
                    pj_copy(block, 2).wait_send()

    for slot in range(slots):
        each_pv(wait_send, slot)

        @pl.when(has_batch(slot))
        def _(slot=slot):
            gx_copy(slot).wait_send()
        each_gram(wait_send, slot)
        forwards_done(slot, 0, n_z - 1)
    forwards_done(0, n_z - 1, n_z)
    for step in range(n_z - 1):
        columns_done(step)
    settle_column(n_z - 1, n_z)
    for slot in range(1, slots):
        settle_rows(slot, n_z - 1, n_z)

    @pl.when(any_active)
    def _():
        gram = g_sum[z]
        for step in range(1, n_z):
            chip = chip_at(step)
            g_copy(chip, z).wait_recv()
            gram = gram + g_all[chip]
        left_core = dot3(col_sketch[...], gram, NN)
        nothing = jnp.zeros((rank_dim, 2 * rank_dim), jnp.bfloat16)

        def stacked(value):
            high, low = halves(value)
            return jnp.concatenate([
                jnp.concatenate([high, high], axis=1), jnp.concatenate([low, nothing], axis=1)
            ], axis=0)

        for slot in range(slots):
            lanes = slice(slot * rank_dim, (slot + 1) * rank_dim)

            @pl.when(active(slot))
            def _(slot=slot, lanes=lanes):
                right_core = dot3(row_sketch[slot], gram[:, lanes], NT)
                y_left[slot] = stacked(
                    jnp.concatenate([own_sketches[slot, 0], -left_core[:, lanes]], axis=1))
                z_left[slot] = stacked(
                    jnp.concatenate([own_sketches[slot, 1], -right_core], axis=1))

    for slot in range(1, slots):
        forwards_done(slot, n_z - 1, n_z)
    columns_done(n_z - 1)


def finish(
    n_row, ru, rv, rp, rj, y_left, z_left, pend_acc,
    trail_y, trail_z, pend_y, pend_z,
    y_buf, z_buf, out_sem, pend_sem,
):
    row, col = lax.axis_index("row"), lax.axis_index("col")
    slots, _, rank_dim, width = ru.shape
    w = pend_y.shape[3]
    pieces = out_sem.shape[2]
    span = width // pieces

    def pend_copy(slot, which):
        lanes = pl.ds((which * slots + slot) * w, w)
        return pltpu.make_async_copy(
            pend_acc.at[:, lanes], (pend_y, pend_z)[which].at[slot, 0], pend_sem.at[slot, which])

    def out_copy(slot, which, piece):
        lanes = pl.ds(piece * span, span)
        src, dst = ((y_buf, trail_y), (z_buf, trail_z))[which]
        return pltpu.make_async_copy(
            src.at[slot, :, lanes], dst.at[slot, 0, 0, :, lanes], out_sem.at[slot, which, piece])

    for slot in range(slots):
        pend_copy(slot, 0).start()
        pend_copy(slot, 1).start()

    for slot in range(slots):
        active = slot * n_row + row > col

        @pl.when(jnp.logical_not(active))
        def _(slot=slot):
            y_buf[slot] = jnp.zeros((rank_dim, width), jnp.float32)
            z_buf[slot] = jnp.zeros((rank_dim, width), jnp.float32)
            for which in range(2):
                for piece in range(pieces):
                    out_copy(slot, which, piece).start()

        @pl.when(active)
        def _(slot=slot):
            for which in range(2):
                left = (y_left, z_left)[which][slot]
                first = (ru, rv)[which]
                buf = (y_buf, z_buf)[which]
                for piece in range(pieces):
                    lanes = slice(piece * span, (piece + 1) * span)
                    second = [rj[part, :, lanes] if which else rp[slot, part, :, lanes]
                              for part in range(2)]
                    right = jnp.concatenate(
                        [first[slot, 0, :, lanes], second[0], first[slot, 1, :, lanes], second[1]],
                        axis=0)
                    both = product(left, right, NN)
                    buf[slot, :, lanes] = both[:rank_dim] + both[rank_dim:]
                    out_copy(slot, which, piece).start()

    for slot in range(slots):
        for which in range(2):
            pend_copy(slot, which).wait()
            for piece in range(pieces):
                out_copy(slot, which, piece).wait()


def broadcast(block, axis, owner):
    block = jnp.where(lax.axis_index(axis) == owner, block, jnp.zeros_like(block))
    return lax.psum(block, axis)


def matmul(left, right):
    return jnp.dot(left, right, precision=lax.Precision.HIGHEST, preferred_element_type=jnp.float32)


def batched(form, left, right):
    return jnp.einsum(
        form, left, right, precision=lax.Precision.HIGHEST, preferred_element_type=jnp.float32
    )


def matern(row_points, col_points):
    delta_x = row_points[0][:, None] - col_points[0][None, :]
    delta_y = row_points[1][:, None] - col_points[1][None, :]
    distance = jnp.sqrt(delta_x * delta_x + delta_y * delta_y)
    scaled = root_three * distance / length_scale
    return matern_scale * (1.0 + scaled) * jnp.exp(-scaled)


def plain_on_device(trail_u, trail_v, ranks, panel_u, panel_v, locations, pend_locs, sketch):
    row_count = lax.axis_size("row")
    row_index = lax.axis_index("row")
    col_index = lax.axis_index("col")
    row_slots = trail_u.shape[0]
    rank_dim = trail_u.shape[3]
    width = trail_u.shape[4]
    local_width = pend_locs.shape[1]
    gathered_u, gathered_v = (
        lax.all_gather(panel_u, "col", axis=3, tiled=True),
        lax.all_gather(panel_v, "col", axis=3, tiled=True),
    )
    slot_index = col_index // row_count
    own_u = lax.dynamic_index_in_dim(gathered_u[:, 0], slot_index, 0, keepdims=False)
    own_v = lax.dynamic_index_in_dim(gathered_v[:, 0], slot_index, 0, keepdims=False)
    col_pu, col_pv = (
        broadcast(own_u, "row", col_index % row_count),
        broadcast(own_v, "row", col_index % row_count),
    )
    rank_iota = lax.broadcasted_iota(jnp.int32, (row_slots, rank_dim), 1)
    in_use = (rank_iota < ranks[:, 0, 0][:, None]).astype(jnp.float32)
    u_tiles = trail_u[:, 0, 0] * in_use[:, :, None]
    v_tiles = trail_v[:, 0, 0]
    row_pu = gathered_u[:, 0]
    row_pv = gathered_v[:, 0]
    v_sketch = batched("tkn,ln->tkl", v_tiles, sketch)
    u_sketch = batched("tkn,ln->tkl", u_tiles, sketch)
    cross_gram = batched("tkn,ln->tkl", row_pv, col_pv)
    col_sketch = matmul(col_pu, sketch.T)
    row_sketch = batched("tkn,ln->tkl", row_pu, sketch)
    left_core = batched("tkm,ml->tkl", cross_gram, col_sketch)
    y_tiles = batched("tkl,tkn->tln", v_sketch, u_tiles) - batched(
        "tkl,tkn->tln", left_core, row_pu
    )
    right_core = batched("tkl,tkm->tlm", row_sketch, cross_gram)
    z_tiles = batched("tkl,tkn->tln", u_sketch, v_tiles) - batched(
        "tlm,mn->tln", right_core, col_pu
    )
    tile_rows = jnp.arange(row_slots, dtype=jnp.int32) * row_count + row_index
    keep_mask = (tile_rows > col_index)[:, None, None]
    trail_y = jnp.where(keep_mask, y_tiles, 0.0).reshape(row_slots, 1, 1, rank_dim, width)
    trail_z = jnp.where(keep_mask, z_tiles, 0.0).reshape(row_slots, 1, 1, rank_dim, width)
    y_list = []
    z_list = []
    rows_all, pend_all = (
        lax.all_gather(locations, "col", axis=3, tiled=True),
        lax.all_gather(pend_locs.reshape(1, 1, 2, local_width), "col", axis=3, tiled=True),
    )
    col_points = pend_all[0, 0]
    for slot_num in range(row_slots):
        own_kernel = matern(locations[slot_num, 0], col_points)
        y_list.append(matmul(sketch, own_kernel.T))
        col_kernel = matern(rows_all[slot_num, 0], pend_locs)
        z_list.append(matmul(sketch, col_kernel))
    pend_y = jnp.stack(y_list)
    pend_z = jnp.stack(z_list)
    pend_y = pend_y.reshape(row_slots, 1, rank_dim, local_width)
    pend_z = pend_z.reshape(row_slots, 1, rank_dim, local_width)
    return (trail_y, trail_z, pend_y, pend_z)


def on_device(n_row, n_col, trail_u, trail_v, ranks, panel_u, panel_v, locations, pend_locs, sketch):
    slots, _, _, rank_dim, width = trail_u.shape
    w = pend_locs.shape[1]
    n_z = n_col // 2
    fits = n_col == slots * n_row and n_row == 4 and slots == 2
    if w % 128 or rank_dim % 16 or not fits:
        return plain_on_device(
            trail_u, trail_v, ranks, panel_u, panel_v, locations, pend_locs, sketch
        )
    flat = slots * rank_dim
    f32, bf16 = jnp.float32, jnp.bfloat16
    dma = pltpu.SemaphoreType.DMA
    vmem = pl.BlockSpec(memory_space=pltpu.VMEM)
    hbm = pl.BlockSpec(memory_space=pltpu.HBM)
    point_rows = -(-(2 * slots + 2) // 8) * 8
    shape = jax.ShapeDtypeStruct
    kept = pl.pallas_call(
        functools.partial(kernel, n_row, n_col),
        out_shape=(
            pltpu.VMEM((slots, 2, rank_dim, width), bf16),
            pltpu.VMEM((slots, 2, rank_dim, width), bf16),
            pltpu.VMEM((slots, 2, rank_dim, width), bf16),
            pltpu.VMEM((2, rank_dim, width), bf16),
            pltpu.VMEM((slots, 2 * rank_dim, 4 * rank_dim), bf16),
            pltpu.VMEM((slots, 2 * rank_dim, 4 * rank_dim), bf16),
            pltpu.VMEM((rank_dim, 2 * slots * w), f32),
        ),
        in_specs=[hbm] * 8,
        out_specs=(vmem,) * 7,
        scratch_shapes=[
            pltpu.SMEM((slots,), jnp.int32),
            pltpu.VMEM((slots, rank_dim, width), f32),
            pltpu.VMEM((slots, rank_dim, width), f32),
            pltpu.VMEM((rank_dim, width), f32),
            pltpu.VMEM((n_col, slots + 1, 2, w), f32),
            pltpu.VMEM((n_col, slots, rank_dim, w), f32),
            pltpu.VMEM((n_col, rank_dim, w), f32),
            pltpu.VMEM((n_row, slots, rank_dim, w), f32),
            pltpu.VMEM((2, n_z, rank_dim, flat), f32),
            pltpu.VMEM((n_z, rank_dim, flat), f32),
            pltpu.VMEM((n_z, rank_dim, flat), f32),
            pltpu.VMEM((n_z, rank_dim, flat), f32),
            pltpu.VMEM((1, w, point_rows), f32),
            pltpu.VMEM((2, 2 * slots * w), f32),
            pltpu.VMEM((n_col, 2 * rank_dim, w), bf16),
            pltpu.VMEM((w, 2 * slots * w), bf16),
            pltpu.VMEM((w, 2 * slots * w), bf16),
            pltpu.VMEM((rank_dim, 2 * slots * w), f32),
            pltpu.VMEM((slots, 2, rank_dim, rank_dim), f32),
            pltpu.VMEM((slots, rank_dim, rank_dim), f32),
            pltpu.VMEM((rank_dim, rank_dim), f32),
            pltpu.SemaphoreType.REGULAR,
            dma((6,)), dma((slots, 2)), dma((n_col,)), dma((n_col,)),
            dma((slots, n_z)), dma((slots, n_col)), dma((slots, n_col)), dma((slots, n_col)),
            dma((slots, n_row)), dma((slots, n_row)),
            dma((4, n_col)), dma((n_col,)),
            dma((slots,)), dma((slots,)), dma((n_z,)), dma((n_z,)),
        ],
        compiler_params=pltpu.CompilerParams(
            collective_id=0, has_side_effects=True, vmem_limit_bytes=VMEM_LIMIT),
    )(*[
        pltpu.with_memory_space_constraint(value, pltpu.HBM) for value in (
            ranks.reshape(slots),
            trail_u.reshape(slots, rank_dim, width),
            trail_v.reshape(slots, rank_dim, width),
            panel_u.reshape(slots, rank_dim, w),
            panel_v.reshape(slots, rank_dim, w),
            locations.reshape(slots, 2, w),
            pend_locs,
            sketch,
        )
    ])
    kept = [pltpu.with_memory_space_constraint(value, pltpu.VMEM) for value in kept]
    pieces = 2
    return pl.pallas_call(
        functools.partial(finish, n_row),
        out_shape=(
            shape((slots, 1, 1, rank_dim, width), f32),
            shape((slots, 1, 1, rank_dim, width), f32),
            shape((slots, 1, rank_dim, w), f32),
            shape((slots, 1, rank_dim, w), f32),
        ),
        in_specs=[vmem] * 7,
        out_specs=(hbm,) * 4,
        scratch_shapes=[
            pltpu.VMEM((slots, rank_dim, width), f32),
            pltpu.VMEM((slots, rank_dim, width), f32),
            dma((slots, 2, pieces)), dma((slots, 2)),
        ],
        compiler_params=pltpu.CompilerParams(vmem_limit_bytes=VMEM_LIMIT),
    )(*kept)


def solution(mesh):
    in_specs = (
        P(None, "row", "col", None, None),
        P(None, "row", "col", None, None),
        P(None, "row", "col"),
        P(None, "row", None, "col"),
        P(None, "row", None, "col"),
        P(None, "row", None, "col"),
        P(None, "col"),
        P(),
    )
    out_specs = (
        P(None, "row", "col", None, None),
        P(None, "row", "col", None, None),
        P(None, "row", None, "col"),
        P(None, "row", None, "col"),
    )
    body = functools.partial(on_device, mesh.shape["row"], mesh.shape["col"])
    return jax.shard_map(
        body, mesh=mesh, in_specs=in_specs, out_specs=out_specs, check_vma=False
    )
```

```python
import functools
import math

import jax
import jax.numpy as jnp
from jax import lax
from jax.experimental import pallas as pl
from jax.experimental.pallas import tpu as pltpu
from jax.sharding import PartitionSpec as P

matern_scale = 4.0
length_scale = 0.15
root_three = math.sqrt(3.0)
point_scale = root_three / length_scale
log2_e = math.log2(math.e)
smallest = 1e-30

MESH = pl.DeviceIdType.MESH
NN = (((1,), (0,)), ((), ()))
NT = (((1,), (1,)), ((), ()))
SLAB = 16
VMEM_LIMIT = 32 << 20


def halves(value):
    high = value.astype(jnp.bfloat16)
    low = (value - high.astype(jnp.float32)).astype(jnp.bfloat16)
    return high, low


def product(left, right, dims):
    return lax.dot_general(left, right, dims, preferred_element_type=jnp.float32)


def dot3_split(left_both, right, dims):
    rows = left_both.shape[0] // 2
    right_high, right_low = halves(right)
    both = product(left_both, right_high, dims)
    return both[:rows] + both[rows:] + product(left_both[:rows], right_low, dims)


def dot3(left, right, dims):
    left_high, left_low = halves(left)
    return dot3_split(jnp.concatenate([left_high, left_low], axis=0), right, dims)


def kernel(
    n_row, n_col,
    ranks_hbm, trail_u, trail_v, panel_u, panel_v, locs, pend, sketch,
    ru, rv, rp, rj, y_left, z_left, pend_acc,
    ranks, u_buf, v_buf, sk_buf, loc_all, pu_all, pj_all, pv_all, g_part, g_peer, g_sum, g_all,
    points, own_points, sk_both, mat_high, mat_low, acc, own_sketches, row_sketch, col_sketch,
    far_sem, load_sem, trail_sem, loc_send, loc_recv, pu_send, pf_send, pr_send, pu_recv,
    pv_send, pv_recv, pj_send, pj_recv, gx_send, gx_recv, g_send, g_recv,
):
    row, col = lax.axis_index("row"), lax.axis_index("col")
    n_z = n_col // 2
    z, core = col // 2, col % 2
    other = 1 - core
    partner = 2 * z + other
    slots, rank_dim, width = u_buf.shape
    w = pu_all.shape[3]
    half_z = n_row // 2
    last = (slots - 1) * n_row
    owner_row, owner_slot = col % n_row, col // n_row
    is_owner = row == owner_row
    x_row = row + 1 - 2 * (row % 2)
    y_row = (row + half_z) % n_row
    diagonal = n_row - 1 - row
    any_active = last + row > col

    def active(slot):
        return slot * n_row + row > col

    def needs(slot, chip):
        return 2 * chip <= slot * n_row + row

    def direct(slot, chip, source):
        near = jnp.logical_or(chip > 0, source < 2)
        return jnp.logical_and(
            needs(slot, chip), jnp.logical_or(near, jnp.logical_not(needs(slot, 1))))

    def hosts(slot):
        return (slot * n_row + row) // 2 == z

    def chip_at(step):
        over = (z + step) // n_z
        return z + step + over * (n_z - 1 - 2 * step - z)

    def wants_column(at_row):
        return last + at_row > col

    def remote(src, dst, send, recv, to_row, to_col):
        return pltpu.make_async_remote_copy(
            src_ref=src, dst_ref=dst, send_sem=send, recv_sem=recv,
            device_id=(to_row, to_col), device_id_type=MESH)

    def loc_copy(source, target):
        return remote(loc_all.at[source], loc_all.at[source], loc_send.at[target],
                      loc_recv.at[source], row, target)

    def pv_copy(slot, source, target):
        return remote(pv_all.at[source, slot], pv_all.at[source, slot],
                      pv_send.at[slot, target], pv_recv.at[slot, source], target, col)

    def pu_copy(slot, block, send, target):
        return remote(pu_all.at[block, slot], pu_all.at[block, slot], send,
                      pu_recv.at[slot, block], row, target)

    def pu_direct(slot, chip):
        return pu_copy(slot, col, pu_send.at[slot, chip], 2 * chip + core)

    def pu_partner(slot, block):
        return pu_copy(slot, block, pf_send.at[slot, block], partner)

    def pu_relay(slot, block):
        return pu_copy(slot, block, pr_send.at[slot, block], core)

    def pj_copy(block, way):
        src = pj_all.at[block] if way == 2 else pu_all.at[block, owner_slot]
        return remote(src, pj_all.at[block], pj_send.at[way, block], pj_recv.at[block],
                      (x_row, y_row, x_row, diagonal)[way], col)

    def gx_copy(batch):
        chips = pl.ds(batch * half_z, half_z)
        return remote(g_part.at[other, chips], g_peer.at[chips], gx_send.at[batch],
                      gx_recv.at[batch], row, partner)

    def g_copy(source, chip):
        return remote(g_sum.at[chip], g_all.at[source], g_send.at[chip], g_recv.at[source],
                      row, 2 * chip + core)

    def when(*terms):
        return pl.when(functools.reduce(jnp.logical_and, terms))

    to_y = jnp.logical_or(wants_column(y_row), wants_column(diagonal))
    y_of_owner = row == (owner_row + half_z) % n_row
    is_relay = jnp.logical_and(y_of_owner, wants_column(x_row))

    barrier = pltpu.get_barrier_semaphore()

    def hello(semaphore, to_row, to_col):
        pl.semaphore_signal(semaphore, inc=1, device_id=(to_row, to_col), device_id_type=MESH)

    for step in range(1, n_row):
        hello(barrier, (row + step) % n_row, col)
    hello(barrier, row, partner)
    for chip in range(1, n_z):
        @pl.when(z < chip)
        def _(chip=chip):
            hello(barrier, row, 2 * chip)
            hello(barrier, row, 2 * chip + 1)

    loads = [
        pltpu.make_async_copy(locs, loc_all.at[col, pl.ds(0, slots)], load_sem.at[0]),
        pltpu.make_async_copy(pend, loc_all.at[col, slots], load_sem.at[1]),
        pltpu.make_async_copy(panel_v, pv_all.at[row], load_sem.at[2]),
        pltpu.make_async_copy(panel_u, pu_all.at[col], load_sem.at[3]),
        pltpu.make_async_copy(sketch, sk_buf, load_sem.at[4]),
        pltpu.make_async_copy(ranks_hbm, ranks, load_sem.at[5]),
    ]
    for load in loads:
        load.start()

    def trail_load(slot, which):
        src, dst = ((trail_u, u_buf), (trail_v, v_buf))[which]
        return pltpu.make_async_copy(src.at[slot], dst.at[slot], trail_sem.at[slot, which])

    for slot in range(slots):
        @pl.when(active(slot))
        def _(slot=slot):
            trail_load(slot, 0).start()
            trail_load(slot, 1).start()

    for load in loads:
        load.wait()
    sk_high, sk_low = halves(sk_buf[...])
    for block in range(n_col):
        sk_both[block, 0:rank_dim] = sk_high[:, block * w:(block + 1) * w]
        sk_both[block, rank_dim:2 * rank_dim] = sk_low[:, block * w:(block + 1) * w]

    acc[...] = jnp.zeros_like(acc)
    row_sketch[...] = jnp.zeros_like(row_sketch)
    col_sketch[...] = jnp.zeros_like(col_sketch)
    own_points[0:1, :] = jnp.concatenate(
        [loc_all[col, slot, 0:1] for slot in range(slots)] + [loc_all[col, slots, 0:1]] * slots,
        axis=1) * point_scale
    own_points[1:2, :] = jnp.concatenate(
        [loc_all[col, slot, 1:2] for slot in range(slots)] + [loc_all[col, slots, 1:2]] * slots,
        axis=1) * point_scale
    pad_rows = points.shape[2] - 2 * slots - 2

    def chunk(step):
        block = 2 * chip_at(step // 2) + (core + step) % 2

        @pl.when(step > 0)
        def _():
            loc_copy(block, partner).wait_recv()

        stack = [loc_all[block, slot] for slot in range(slots + 1)]
        if pad_rows:
            stack.append(jnp.zeros((pad_rows, w), jnp.float32))
        points[0] = jnp.concatenate(stack, axis=0).T * point_scale

        sk = sk_both[block]
        for part in range(2 * slots):
            base = 2 * slots if part < slots else 2 * (part - slots)
            lanes = slice(part * w, (part + 1) * w)
            for slab in range(w // SLAB):
                rows = slice(slab * SLAB, (slab + 1) * SLAB)
                at = points[0, rows, :]
                delta_x = at[:, base:base + 1] - own_points[0:1, lanes]
                delta_y = at[:, base + 1:base + 2] - own_points[1:2, lanes]
                square = delta_x * delta_x + delta_y * delta_y
                scaled = square * lax.rsqrt(jnp.maximum(square, smallest))
                value = (1.0 + scaled) * jnp.exp2(scaled * -log2_e)
                high, low = halves(value)
                mat_high[rows, lanes] = high
                mat_low[rows, lanes] = low
            both = product(sk, mat_high[:, lanes], NN)
            acc[:, lanes] += (both[:rank_dim] + both[rank_dim:]
                              + product(sk[:rank_dim], mat_low[:, lanes], NN))

    def chunks(first, final):
        pl.loop(first * n_col // 8, final * n_col // 8)(chunk)

    def sketch_of(block, high, low):
        sk = sk_both[block]
        both = product(sk, high, NT)
        return both[:rank_dim] + both[rank_dim:] + product(sk[:rank_dim], low, NT)

    def own_sketch(slot):
        trail_load(slot, 0).wait()
        trail_load(slot, 1).wait()
        in_use = lax.broadcasted_iota(jnp.int32, (rank_dim, 1), 0) < ranks[slot]
        v_sketch = jnp.zeros((rank_dim, rank_dim), jnp.float32)
        u_sketch = jnp.zeros((rank_dim, rank_dim), jnp.float32)
        for block in range(n_col):
            lanes = slice(block * w, (block + 1) * w)
            high, low = halves(v_buf[slot, :, lanes])
            rv[slot, 0, :, lanes] = high
            rv[slot, 1, :, lanes] = low
            v_sketch += sketch_of(block, high, low)
            high, low = halves(jnp.where(in_use, u_buf[slot, :, lanes], 0.0))
            ru[slot, 0, :, lanes] = high
            ru[slot, 1, :, lanes] = low
            u_sketch += sketch_of(block, high, low)
        own_sketches[slot, 0] = v_sketch
        own_sketches[slot, 1] = u_sketch

    def own_all():
        for slot in range(slots):
            @pl.when(active(slot))
            def _(slot=slot):
                own_sketch(slot)

    corner = (n_row - row) // n_row
    pl.loop(0, corner)(chunk)

    @pl.when(corner == 1)
    def _():
        own_all()
    pl.semaphore_wait(barrier, n_row + 2 * z)

    for chip in range(n_z - 1):
        @pl.when(z > chip)
        def _(chip=chip):
            hello(far_sem, row, 2 * chip)
            hello(far_sem, row, 2 * chip + 1)

    def each_loc(act, higher):
        for chip in range(n_z):
            @pl.when(z < chip if higher else z > chip)
            def _(chip=chip):
                act(loc_copy(col, 2 * chip))
                act(loc_copy(col, 2 * chip + 1))

    def each_direct(act, higher, slot):
        for chip in (range(1, n_z) if higher else reversed(range(n_z - 1))):
            @when(z < chip if higher else z > chip, direct(slot, chip, z))
            def _(chip=chip):
                act(pu_direct(slot, chip))

    def each_pv(act, slot):
        for step in range(1, n_row):
            target = (row + step) % n_row

            @pl.when(last + target > slot * n_row + row)
            def _(target=target):
                act(pv_copy(slot, row, target))

    def straight(step):
        if step == n_z - 1:
            return True
        return False

    def each_column(act, block, step, slot=None):
        ours = is_owner if slot is None else jnp.logical_and(is_owner, owner_slot == slot)
        far = straight(step)

        @when(ours, wants_column(x_row))
        def _():
            act(pj_copy(block, 0))

        @when(ours, wants_column(y_row) if far is True else to_y)
        def _():
            act(pj_copy(block, 1))

        if far is not False:
            @when(ours, wants_column(diagonal), far)
            def _():
                act(pj_copy(block, 3))

    def start(copy):
        copy.start()

    def wait_send(copy):
        copy.wait_send()

    def send_lower(slot):
        each_direct(start, False, slot)

        @pl.when(needs(slot, z))
        def _():
            start(pu_partner(slot, col))

    start(loc_copy(col, partner))
    each_loc(start, False)
    each_pv(start, 0)

    @pl.when(z < n_z - 1)
    def _():
        send_lower(0)

    @when(z == 1, needs(0, z))
    def _():
        for slot in range(1, slots):
            send_lower(slot)
    def arrive(slot, step):
        chip = chip_at(step)
        block = 2 * chip + core

        @pl.when(needs(slot, z))
        def _():
            pu_partner(slot, block).wait_recv()

            @when(z == 1, chip >= 2)
            def _():
                pu_relay(slot, block).start()
            pu_partner(slot, block).start()
            each_column(start, block, step, slot)

    def spreads(slot):
        return jnp.logical_and(is_owner, owner_slot == slot)

    def from_partner(slot, step):
        block = 2 * chip_at(step) + other

        @when(needs(slot, z), spreads(slot))
        def _():
            pu_partner(slot, block).wait_recv()
            each_column(start, block, step, slot)

    def settle_rows(slot, first, final):
        @when(needs(slot, z), jnp.logical_not(spreads(slot)))
        def _():
            for step in range(first, final):
                pu_partner(slot, 2 * chip_at(step) + other).wait_recv()
        absorb_rows(slot, first, final)

    def pair(step):
        return [2 * chip_at(step) + (core + flip) % 2 for flip in range(2)]

    def column(step):
        @pl.when(is_relay)
        def _():
            for block in pair(step):
                pj_copy(block, 0).wait_recv()

                @pl.when(jnp.logical_not(straight(step)))
                def _(block=block):
                    pj_copy(block, 2).start()

    def settle_column(first, final):
        for step in range(first, final):
            late = step == n_z - 1

            @when(jnp.logical_not(is_owner), wants_column(row),
                  True if late else jnp.logical_not(is_relay))
            def _(step=step):
                for block in pair(step):
                    pj_copy(block, 0).wait_recv()
        absorb_column(first, final)

    def gram_part(slot):
        own_v = pv_all[row].reshape(slots * rank_dim, w)
        own_high, own_low = halves(own_v)
        for source in range(n_row):
            tile = slot * n_row + source

            @pl.when(last + row > tile)
            def _(source=source, tile=tile):
                @pl.when(row != source)
                def _():
                    pv_copy(slot, source, row).wait_recv()
                high, low = halves(pv_all[source, slot])
                both = product(jnp.concatenate([high, low], axis=0), own_high, NT)
                g_part[tile % 2, tile // 2] = (
                    both[:rank_dim] + both[rank_dim:] + product(high, own_low, NT))

    def has_batch(batch):
        return last + row > batch * n_row

    def gram_swap(batch):
        @pl.when(has_batch(batch))
        def _():
            gx_copy(batch).start()

    def gram_sum(batch):
        @pl.when(has_batch(batch))
        def _():
            gx_copy(batch).wait_recv()
            for chip in range(batch * half_z, (batch + 1) * half_z):
                g_sum[chip] = g_part[core, chip] + g_peer[chip]

    def each_gram(act, batch):
        for chip in range(batch * half_z, (batch + 1) * half_z):
            @when(last + row > 2 * chip + core, z != chip)
            def _(chip=chip):
                act(g_copy(z, chip))

    def blocks_of(first, final):
        return [2 * chip_at(step) + flip for step in range(first, final) for flip in range(2)]

    def absorb_rows(slot, first, final):
        @pl.when(active(slot))
        def _():
            total = row_sketch[slot]
            for block in blocks_of(first, final):
                lanes = pl.ds(pl.multiple_of(block * w, w), w)
                high, low = halves(pu_all[block, slot])
                rp[slot, 0, :, lanes] = high
                rp[slot, 1, :, lanes] = low
                total += sketch_of(block, high, low)
            row_sketch[slot] = total

    def absorb_column(first, final):
        @pl.when(any_active)
        def _():
            @pl.when(is_owner)
            def _():
                for block in blocks_of(first, final):
                    pj_all[block] = pu_all[block, owner_slot]
            total = col_sketch[...]
            for block in blocks_of(first, final):
                lanes = pl.ds(pl.multiple_of(block * w, w), w)
                high, low = halves(pj_all[block])
                rj[0, :, lanes] = high
                rj[1, :, lanes] = low
                total += sketch_of(block, high, low)
            col_sketch[...] = total

    def upward():
        @pl.when(z < n_z - 1)
        def _():
            pl.semaphore_wait(far_sem, 2 * (n_z - 1 - z))
        each_loc(start, True)
        for slot in range(slots):
            each_direct(start, True, slot)

    def early(slot, step):
        @pl.when(jnp.logical_or(z > 0, hosts(slot)))
        def _():
            arrive(slot, step)

    def late(slot, step):
        @when(z == 0, jnp.logical_not(hosts(slot)))
        def _():
            arrive(slot, step)

    top = n_z - 1
    pl.loop(corner, 1)(chunk)

    @pl.when(z == top)
    def _():
        send_lower(0)
    chunks(1, 2)

    @when(z != 1, z < top)
    def _():
        for slot in range(1, slots):
            send_lower(slot)
    for slot in range(1, slots):
        each_pv(start, slot)
    each_column(start, col, 0)

    @pl.when(corner == 0)
    def _():
        own_all()
    upward()

    @pl.when(jnp.logical_or(z == top, jnp.logical_and(z == 1, jnp.logical_not(needs(0, z)))))
    def _():
        for slot in range(1, slots):
            send_lower(slot)
    from_partner(0, 0)
    chunks(2, 3)
    for slot in range(1, slots):
        from_partner(slot, 0)
    @pl.when(z > 0)
    def _():
        arrive(0, 1)
    gram_part(0)

    @pl.when(z > 0)
    def _():
        arrive(0, 2)
    gram_swap(0)
    chunks(3, 4)

    @pl.when(z == 0)
    def _():
        arrive(0, 1)
    gram_sum(0)
    from_partner(0, 1)
    for slot in range(1, slots):
        early(slot, 1)

    @when(z == 0, hosts(0))
    def _():
        arrive(0, 2)
    each_gram(start, 0)
    chunks(4, 5)
    for slot in range(1, slots):
        early(slot, 2)
        from_partner(slot, 1)
        gram_part(slot)
    from_partner(0, 2)
    column(0)
    for slot in range(1, slots):
        gram_swap(slot)
    early(0, 3)
    chunks(5, 6)
    for slot in range(1, slots):
        gram_sum(slot)
        late(slot, 1)
        from_partner(slot, 2)
    late(0, 2)
    from_partner(0, 3)
    for slot in range(1, slots):
        each_gram(start, slot)
    chunks(6, 7)
    for slot in range(1, slots):
        early(slot, 3)
    column(1)
    chunks(7, 8)
    for slot in range(1, slots):
        settle_rows(slot, 0, n_z - 2)
    late(0, 3)
    column(2)
    for slot in range(1, slots):
        late(slot, 2)
    settle_rows(0, 0, n_z)
    pend_acc[...] = acc[...] * matern_scale

    wait_send(loc_copy(col, partner))
    for higher in (False, True):
        each_loc(wait_send, higher)
        for slot in range(slots):
            each_direct(wait_send, higher, slot)

    def forwards_done(slot, first, final):
        for step in range(first, final):
            block = 2 * chip_at(step) + core

            @pl.when(needs(slot, z))
            def _(block=block):
                pu_partner(slot, block).wait_send()

            @when(z == 1, chip_at(step) >= 2, needs(slot, z))
            def _(block=block):
                pu_relay(slot, block).wait_send()

    def columns_done(step):
        for block in pair(step):
            each_column(wait_send, block, step)
        if step < n_z - 1:
            @when(is_relay, jnp.logical_not(straight(step)))
            def _():
                for block in pair(step):
                    pj_copy(block, 2).wait_send()

    for slot in range(slots):
        each_pv(wait_send, slot)

        @pl.when(has_batch(slot))
        def _(slot=slot):
            gx_copy(slot).wait_send()
        each_gram(wait_send, slot)
        forwards_done(slot, 0, n_z - 1)
    forwards_done(0, n_z - 1, n_z)
    for step in range(n_z - 1):
        columns_done(step)
    for slot in range(1, slots):
        late(slot, 3)
        from_partner(slot, 3)
    settle_column(0, n_z - 1)
    for slot in range(1, slots):
        settle_rows(slot, n_z - 2, n_z)
    settle_column(n_z - 1, n_z)

    @pl.when(any_active)
    def _():
        gram = g_sum[z]
        for step in range(1, n_z):
            chip = chip_at(step)
            g_copy(chip, z).wait_recv()
            gram = gram + g_all[chip]
        left_core = dot3(col_sketch[...], gram, NN)
        nothing = jnp.zeros((rank_dim, 2 * rank_dim), jnp.bfloat16)

        def stacked(value):
            high, low = halves(value)
            return jnp.concatenate([
                jnp.concatenate([high, high], axis=1), jnp.concatenate([low, nothing], axis=1)
            ], axis=0)

        for slot in range(slots):
            lanes = slice(slot * rank_dim, (slot + 1) * rank_dim)

            @pl.when(active(slot))
            def _(slot=slot, lanes=lanes):
                right_core = dot3(row_sketch[slot], gram[:, lanes], NT)
                y_left[slot] = stacked(
                    jnp.concatenate([own_sketches[slot, 0], -left_core[:, lanes]], axis=1))
                z_left[slot] = stacked(
                    jnp.concatenate([own_sketches[slot, 1], -right_core], axis=1))

    for slot in range(1, slots):
        forwards_done(slot, n_z - 1, n_z)
    columns_done(n_z - 1)


def finish(
    n_row, ru, rv, rp, rj, y_left, z_left, pend_acc,
    trail_y, trail_z, pend_y, pend_z,
    y_buf, z_buf, out_sem, pend_sem,
):
    row, col = lax.axis_index("row"), lax.axis_index("col")
    slots, _, rank_dim, width = ru.shape
    w = pend_y.shape[3]
    pieces = out_sem.shape[2]
    span = width // pieces

    def pend_copy(slot, which):
        lanes = pl.ds((which * slots + slot) * w, w)
        return pltpu.make_async_copy(
            pend_acc.at[:, lanes], (pend_y, pend_z)[which].at[slot, 0], pend_sem.at[slot, which])

    def out_copy(slot, which, piece):
        lanes = pl.ds(piece * span, span)
        src, dst = ((y_buf, trail_y), (z_buf, trail_z))[which]
        return pltpu.make_async_copy(
            src.at[slot, :, lanes], dst.at[slot, 0, 0, :, lanes], out_sem.at[slot, which, piece])

    for slot in range(slots):
        pend_copy(slot, 0).start()
        pend_copy(slot, 1).start()

    for slot in range(slots):
        active = slot * n_row + row > col

        @pl.when(jnp.logical_not(active))
        def _(slot=slot):
            y_buf[slot] = jnp.zeros((rank_dim, width), jnp.float32)
            z_buf[slot] = jnp.zeros((rank_dim, width), jnp.float32)
            for which in range(2):
                for piece in range(pieces):
                    out_copy(slot, which, piece).start()

        @pl.when(active)
        def _(slot=slot):
            for which in range(2):
                left = (y_left, z_left)[which][slot]
                first = (ru, rv)[which]
                buf = (y_buf, z_buf)[which]
                for piece in range(pieces):
                    lanes = slice(piece * span, (piece + 1) * span)
                    second = [rj[part, :, lanes] if which else rp[slot, part, :, lanes]
                              for part in range(2)]
                    right = jnp.concatenate(
                        [first[slot, 0, :, lanes], second[0], first[slot, 1, :, lanes], second[1]],
                        axis=0)
                    both = product(left, right, NN)
                    buf[slot, :, lanes] = both[:rank_dim] + both[rank_dim:]
                    out_copy(slot, which, piece).start()

    for slot in range(slots):
        for which in range(2):
            pend_copy(slot, which).wait()
            for piece in range(pieces):
                out_copy(slot, which, piece).wait()


def broadcast(block, axis, owner):
    block = jnp.where(lax.axis_index(axis) == owner, block, jnp.zeros_like(block))
    return lax.psum(block, axis)


def matmul(left, right):
    return jnp.dot(left, right, precision=lax.Precision.HIGHEST, preferred_element_type=jnp.float32)


def batched(form, left, right):
    return jnp.einsum(
        form, left, right, precision=lax.Precision.HIGHEST, preferred_element_type=jnp.float32
    )


def matern(row_points, col_points):
    delta_x = row_points[0][:, None] - col_points[0][None, :]
    delta_y = row_points[1][:, None] - col_points[1][None, :]
    distance = jnp.sqrt(delta_x * delta_x + delta_y * delta_y)
    scaled = root_three * distance / length_scale
    return matern_scale * (1.0 + scaled) * jnp.exp(-scaled)


def plain_on_device(trail_u, trail_v, ranks, panel_u, panel_v, locations, pend_locs, sketch):
    row_count = lax.axis_size("row")
    row_index = lax.axis_index("row")
    col_index = lax.axis_index("col")
    row_slots = trail_u.shape[0]
    rank_dim = trail_u.shape[3]
    width = trail_u.shape[4]
    local_width = pend_locs.shape[1]
    gathered_u, gathered_v = (
        lax.all_gather(panel_u, "col", axis=3, tiled=True),
        lax.all_gather(panel_v, "col", axis=3, tiled=True),
    )
    slot_index = col_index // row_count
    own_u = lax.dynamic_index_in_dim(gathered_u[:, 0], slot_index, 0, keepdims=False)
    own_v = lax.dynamic_index_in_dim(gathered_v[:, 0], slot_index, 0, keepdims=False)
    col_pu, col_pv = (
        broadcast(own_u, "row", col_index % row_count),
        broadcast(own_v, "row", col_index % row_count),
    )
    rank_iota = lax.broadcasted_iota(jnp.int32, (row_slots, rank_dim), 1)
    in_use = (rank_iota < ranks[:, 0, 0][:, None]).astype(jnp.float32)
    u_tiles = trail_u[:, 0, 0] * in_use[:, :, None]
    v_tiles = trail_v[:, 0, 0]
    row_pu = gathered_u[:, 0]
    row_pv = gathered_v[:, 0]
    v_sketch = batched("tkn,ln->tkl", v_tiles, sketch)
    u_sketch = batched("tkn,ln->tkl", u_tiles, sketch)
    cross_gram = batched("tkn,ln->tkl", row_pv, col_pv)
    col_sketch = matmul(col_pu, sketch.T)
    row_sketch = batched("tkn,ln->tkl", row_pu, sketch)
    left_core = batched("tkm,ml->tkl", cross_gram, col_sketch)
    y_tiles = batched("tkl,tkn->tln", v_sketch, u_tiles) - batched(
        "tkl,tkn->tln", left_core, row_pu
    )
    right_core = batched("tkl,tkm->tlm", row_sketch, cross_gram)
    z_tiles = batched("tkl,tkn->tln", u_sketch, v_tiles) - batched(
        "tlm,mn->tln", right_core, col_pu
    )
    tile_rows = jnp.arange(row_slots, dtype=jnp.int32) * row_count + row_index
    keep_mask = (tile_rows > col_index)[:, None, None]
    trail_y = jnp.where(keep_mask, y_tiles, 0.0).reshape(row_slots, 1, 1, rank_dim, width)
    trail_z = jnp.where(keep_mask, z_tiles, 0.0).reshape(row_slots, 1, 1, rank_dim, width)
    y_list = []
    z_list = []
    rows_all, pend_all = (
        lax.all_gather(locations, "col", axis=3, tiled=True),
        lax.all_gather(pend_locs.reshape(1, 1, 2, local_width), "col", axis=3, tiled=True),
    )
    col_points = pend_all[0, 0]
    for slot_num in range(row_slots):
        own_kernel = matern(locations[slot_num, 0], col_points)
        y_list.append(matmul(sketch, own_kernel.T))
        col_kernel = matern(rows_all[slot_num, 0], pend_locs)
        z_list.append(matmul(sketch, col_kernel))
    pend_y = jnp.stack(y_list)
    pend_z = jnp.stack(z_list)
    pend_y = pend_y.reshape(row_slots, 1, rank_dim, local_width)
    pend_z = pend_z.reshape(row_slots, 1, rank_dim, local_width)
    return (trail_y, trail_z, pend_y, pend_z)


def on_device(n_row, n_col, trail_u, trail_v, ranks, panel_u, panel_v, locations, pend_locs, sketch):
    slots, _, _, rank_dim, width = trail_u.shape
    w = pend_locs.shape[1]
    n_z = n_col // 2
    fits = n_col == slots * n_row and n_row == 4 and slots == 2
    if w % 128 or rank_dim % 16 or not fits:
        return plain_on_device(
            trail_u, trail_v, ranks, panel_u, panel_v, locations, pend_locs, sketch
        )
    flat = slots * rank_dim
    f32, bf16 = jnp.float32, jnp.bfloat16
    dma = pltpu.SemaphoreType.DMA
    vmem = pl.BlockSpec(memory_space=pltpu.VMEM)
    hbm = pl.BlockSpec(memory_space=pltpu.HBM)
    point_rows = -(-(2 * slots + 2) // 8) * 8
    shape = jax.ShapeDtypeStruct
    kept = pl.pallas_call(
        functools.partial(kernel, n_row, n_col),
        out_shape=(
            pltpu.VMEM((slots, 2, rank_dim, width), bf16),
            pltpu.VMEM((slots, 2, rank_dim, width), bf16),
            pltpu.VMEM((slots, 2, rank_dim, width), bf16),
            pltpu.VMEM((2, rank_dim, width), bf16),
            pltpu.VMEM((slots, 2 * rank_dim, 4 * rank_dim), bf16),
            pltpu.VMEM((slots, 2 * rank_dim, 4 * rank_dim), bf16),
            pltpu.VMEM((rank_dim, 2 * slots * w), f32),
        ),
        in_specs=[hbm] * 8,
        out_specs=(vmem,) * 7,
        scratch_shapes=[
            pltpu.SMEM((slots,), jnp.int32),
            pltpu.VMEM((slots, rank_dim, width), f32),
            pltpu.VMEM((slots, rank_dim, width), f32),
            pltpu.VMEM((rank_dim, width), f32),
            pltpu.VMEM((n_col, slots + 1, 2, w), f32),
            pltpu.VMEM((n_col, slots, rank_dim, w), f32),
            pltpu.VMEM((n_col, rank_dim, w), f32),
            pltpu.VMEM((n_row, slots, rank_dim, w), f32),
            pltpu.VMEM((2, n_z, rank_dim, flat), f32),
            pltpu.VMEM((n_z, rank_dim, flat), f32),
            pltpu.VMEM((n_z, rank_dim, flat), f32),
            pltpu.VMEM((n_z, rank_dim, flat), f32),
            pltpu.VMEM((1, w, point_rows), f32),
            pltpu.VMEM((2, 2 * slots * w), f32),
            pltpu.VMEM((n_col, 2 * rank_dim, w), bf16),
            pltpu.VMEM((w, 2 * slots * w), bf16),
            pltpu.VMEM((w, 2 * slots * w), bf16),
            pltpu.VMEM((rank_dim, 2 * slots * w), f32),
            pltpu.VMEM((slots, 2, rank_dim, rank_dim), f32),
            pltpu.VMEM((slots, rank_dim, rank_dim), f32),
            pltpu.VMEM((rank_dim, rank_dim), f32),
            pltpu.SemaphoreType.REGULAR,
            dma((6,)), dma((slots, 2)), dma((n_col,)), dma((n_col,)),
            dma((slots, n_z)), dma((slots, n_col)), dma((slots, n_col)), dma((slots, n_col)),
            dma((slots, n_row)), dma((slots, n_row)),
            dma((4, n_col)), dma((n_col,)),
            dma((slots,)), dma((slots,)), dma((n_z,)), dma((n_z,)),
        ],
        compiler_params=pltpu.CompilerParams(
            collective_id=0, has_side_effects=True, vmem_limit_bytes=VMEM_LIMIT),
    )(*[
        pltpu.with_memory_space_constraint(value, pltpu.HBM) for value in (
            ranks.reshape(slots),
            trail_u.reshape(slots, rank_dim, width),
            trail_v.reshape(slots, rank_dim, width),
            panel_u.reshape(slots, rank_dim, w),
            panel_v.reshape(slots, rank_dim, w),
            locations.reshape(slots, 2, w),
            pend_locs,
            sketch,
        )
    ])
    kept = [pltpu.with_memory_space_constraint(value, pltpu.VMEM) for value in kept]
    pieces = 2
    return pl.pallas_call(
        functools.partial(finish, n_row),
        out_shape=(
            shape((slots, 1, 1, rank_dim, width), f32),
            shape((slots, 1, 1, rank_dim, width), f32),
            shape((slots, 1, rank_dim, w), f32),
            shape((slots, 1, rank_dim, w), f32),
        ),
        in_specs=[vmem] * 7,
        out_specs=(hbm,) * 4,
        scratch_shapes=[
            pltpu.VMEM((slots, rank_dim, width), f32),
            pltpu.VMEM((slots, rank_dim, width), f32),
            dma((slots, 2, pieces)), dma((slots, 2)),
        ],
        compiler_params=pltpu.CompilerParams(vmem_limit_bytes=VMEM_LIMIT),
    )(*kept)


def solution(mesh):
    in_specs = (
        P(None, "row", "col", None, None),
        P(None, "row", "col", None, None),
        P(None, "row", "col"),
        P(None, "row", None, "col"),
        P(None, "row", None, "col"),
        P(None, "row", None, "col"),
        P(None, "col"),
        P(),
    )
    out_specs = (
        P(None, "row", "col", None, None),
        P(None, "row", "col", None, None),
        P(None, "row", None, "col"),
        P(None, "row", None, "col"),
    )
    body = functools.partial(on_device, mesh.shape["row"], mesh.shape["col"])
    return jax.shard_map(
        body, mesh=mesh, in_specs=in_specs, out_specs=out_specs, check_vma=False
    )
```

```python
import functools
import math

import jax
import jax.numpy as jnp
from jax import lax
from jax.experimental import pallas as pl
from jax.experimental.pallas import tpu as pltpu
from jax.sharding import PartitionSpec as P

matern_scale = 4.0
length_scale = 0.15
root_three = math.sqrt(3.0)
point_scale = root_three / length_scale
log2_e = math.log2(math.e)
smallest = 1e-30

MESH = pl.DeviceIdType.MESH
NN = (((1,), (0,)), ((), ()))
NT = (((1,), (1,)), ((), ()))
SLAB = 16
VMEM_LIMIT = 32 << 20


def halves(value):
    high = value.astype(jnp.bfloat16)
    low = (value - high.astype(jnp.float32)).astype(jnp.bfloat16)
    return high, low


def product(left, right, dims):
    return lax.dot_general(left, right, dims, preferred_element_type=jnp.float32)


def dot3_split(left_both, right, dims):
    rows = left_both.shape[0] // 2
    right_high, right_low = halves(right)
    both = product(left_both, right_high, dims)
    return both[:rows] + both[rows:] + product(left_both[:rows], right_low, dims)


def dot3(left, right, dims):
    left_high, left_low = halves(left)
    return dot3_split(jnp.concatenate([left_high, left_low], axis=0), right, dims)


def kernel(
    n_row, n_col,
    ranks_hbm, trail_u, trail_v, panel_u, panel_v, locs, pend, sketch,
    ru, rv, rp, rj, y_left, z_left, pend_acc,
    ranks, u_buf, v_buf, sk_buf, loc_all, pu_all, pj_all, pv_all, g_part, g_peer, g_sum, g_all,
    points, own_points, sk_both, mat_high, mat_low, acc, own_sketches, row_sketch, col_sketch, gram_all,
    far_sem, load_sem, trail_sem, loc_send, lf_send, loc_recv, pu_send, pf_send, pr_send, pu_recv,
    pv_send, pv_recv, pj_send, pj_recv, gx_send, gx_recv, g_send, g_recv,
):
    row, col = lax.axis_index("row"), lax.axis_index("col")
    n_z = n_col // 2
    z, core = col // 2, col % 2
    other = 1 - core
    partner = 2 * z + other
    slots, rank_dim, width = u_buf.shape
    w = pu_all.shape[3]
    half_z = n_row // 2
    last = (slots - 1) * n_row
    owner_row, owner_slot = col % n_row, col // n_row
    is_owner = row == owner_row
    x_row = row + 1 - 2 * (row % 2)
    y_row = (row + half_z) % n_row
    diagonal = n_row - 1 - row
    any_active = last + row > col

    def active(slot):
        return slot * n_row + row > col

    def needs(slot, chip):
        return 2 * chip <= slot * n_row + row

    def direct(slot, chip, source):
        near = jnp.logical_or(chip > 0, source < 2)
        return jnp.logical_and(
            needs(slot, chip), jnp.logical_or(near, jnp.logical_not(needs(slot, 1))))

    def hosts(slot):
        return (slot * n_row + row) // 2 == z

    host_slot = 2 * z // n_row
    host_col = host_slot * n_row + row
    is_host = host_col // 2 == z

    def chip_at(step):
        over = (z + step) // n_z
        return z + step + over * (n_z - 1 - 2 * step - z)

    def wants_column(at_row):
        return last + at_row > col

    def remote(src, dst, send, recv, to_row, to_col):
        return pltpu.make_async_remote_copy(
            src_ref=src, dst_ref=dst, send_sem=send, recv_sem=recv,
            device_id=(to_row, to_col), device_id_type=MESH)

    def loc_copy(source, target):
        return remote(loc_all.at[source], loc_all.at[source], loc_send.at[target],
                      loc_recv.at[source], row, target)

    def loc_forward(block):
        return remote(loc_all.at[block], loc_all.at[block], lf_send.at[block],
                      loc_recv.at[block], row, partner)

    def pv_copy(slot, source, target):
        return remote(pv_all.at[source, slot], pv_all.at[source, slot],
                      pv_send.at[slot, target], pv_recv.at[slot, source], target, col)

    def pu_copy(slot, block, send, target):
        return remote(pu_all.at[block, slot], pu_all.at[block, slot], send,
                      pu_recv.at[slot, block], row, target)

    def pu_direct(slot, chip):
        return pu_copy(slot, col, pu_send.at[slot, chip], 2 * chip + core)

    def pu_partner(slot, block):
        return pu_copy(slot, block, pf_send.at[slot, block], partner)

    def pu_relay(slot, block):
        return pu_copy(slot, block, pr_send.at[slot, block], core)

    def pj_copy(block, way):
        src = pj_all.at[block] if way == 2 else pu_all.at[block, host_slot]
        return remote(src, pj_all.at[block], pj_send.at[way, block], pj_recv.at[block],
                      (x_row, y_row, x_row, diagonal)[way], col if way == 2 else host_col)

    def gx_copy(batch):
        chips = pl.ds(batch * half_z, half_z)
        return remote(g_part.at[other, chips], g_peer.at[chips], gx_send.at[batch],
                      gx_recv.at[batch], row, partner)

    def g_copy(source, chip):
        return remote(g_sum.at[chip], g_all.at[source], g_send.at[chip], g_recv.at[source],
                      row, 2 * chip + core)

    def when(*terms):
        return pl.when(functools.reduce(jnp.logical_and, terms))

    def host_wants(at_row):
        return last + at_row > host_col

    to_y = jnp.logical_or(host_wants(y_row), host_wants(diagonal))
    y_of_owner = row == (owner_row + half_z) % n_row
    is_relay = jnp.logical_and(y_of_owner, wants_column(x_row))

    barrier = pltpu.get_barrier_semaphore()

    def hello(semaphore, to_row, to_col):
        pl.semaphore_signal(semaphore, inc=1, device_id=(to_row, to_col), device_id_type=MESH)

    for step in range(1, n_row):
        hello(barrier, (row + step) % n_row, col)
        hello(barrier, (row + step) % n_row, partner)
    hello(barrier, row, partner)
    for chip in range(1, n_z):
        @pl.when(z < chip)
        def _(chip=chip):
            hello(barrier, row, 2 * chip + core)

    loads = [
        pltpu.make_async_copy(locs, loc_all.at[col, pl.ds(0, slots)], load_sem.at[0]),
        pltpu.make_async_copy(pend, loc_all.at[col, slots], load_sem.at[1]),
        pltpu.make_async_copy(panel_v, pv_all.at[row], load_sem.at[2]),
        pltpu.make_async_copy(panel_u, pu_all.at[col], load_sem.at[3]),
        pltpu.make_async_copy(sketch, sk_buf, load_sem.at[4]),
        pltpu.make_async_copy(ranks_hbm, ranks, load_sem.at[5]),
    ]
    for load in loads:
        load.start()

    def trail_load(slot, which):
        src, dst = ((trail_u, u_buf), (trail_v, v_buf))[which]
        return pltpu.make_async_copy(src.at[slot], dst.at[slot], trail_sem.at[slot, which])

    for slot in range(slots):
        @pl.when(active(slot))
        def _(slot=slot):
            trail_load(slot, 0).start()
            trail_load(slot, 1).start()

    for load in loads:
        load.wait()
    sk_high, sk_low = halves(sk_buf[...])
    for block in range(n_col):
        sk_both[block, 0:rank_dim] = sk_high[:, block * w:(block + 1) * w]
        sk_both[block, rank_dim:2 * rank_dim] = sk_low[:, block * w:(block + 1) * w]

    acc[...] = jnp.zeros_like(acc)
    row_sketch[...] = jnp.zeros_like(row_sketch)
    col_sketch[...] = jnp.zeros_like(col_sketch)
    own_points[0:1, :] = jnp.concatenate(
        [loc_all[col, slot, 0:1] for slot in range(slots)] + [loc_all[col, slots, 0:1]] * slots,
        axis=1) * point_scale
    own_points[1:2, :] = jnp.concatenate(
        [loc_all[col, slot, 1:2] for slot in range(slots)] + [loc_all[col, slots, 1:2]] * slots,
        axis=1) * point_scale
    pad_rows = points.shape[2] - 2 * slots - 2

    def chunk(step):
        block = 2 * chip_at(step // 2) + (core + step) % 2

        @pl.when(step % 2 == 1)
        def _():
            loc_copy(block, partner).wait_recv()

        stack = [loc_all[block, slot] for slot in range(slots + 1)]
        if pad_rows:
            stack.append(jnp.zeros((pad_rows, w), jnp.float32))
        points[0] = jnp.concatenate(stack, axis=0).T * point_scale

        sk = sk_both[block]
        for part in range(2 * slots):
            base = 2 * slots if part < slots else 2 * (part - slots)
            lanes = slice(part * w, (part + 1) * w)
            for slab in range(w // SLAB):
                rows = slice(slab * SLAB, (slab + 1) * SLAB)
                at = points[0, rows, :]
                delta_x = at[:, base:base + 1] - own_points[0:1, lanes]
                delta_y = at[:, base + 1:base + 2] - own_points[1:2, lanes]
                square = delta_x * delta_x + delta_y * delta_y
                scaled = square * lax.rsqrt(jnp.maximum(square, smallest))
                value = (1.0 + scaled) * jnp.exp2(scaled * -log2_e)
                high, low = halves(value)
                mat_high[rows, lanes] = high
                mat_low[rows, lanes] = low
            both = product(sk, mat_high[:, lanes], NN)
            acc[:, lanes] += (both[:rank_dim] + both[rank_dim:]
                              + product(sk[:rank_dim], mat_low[:, lanes], NN))

    def chunks(first, final):
        pl.loop(first * n_col // 8, final * n_col // 8)(chunk)

    def sketch_of(block, high, low):
        sk = sk_both[block]
        both = product(sk, high, NT)
        return both[:rank_dim] + both[rank_dim:] + product(sk[:rank_dim], low, NT)

    def own_sketch(slot):
        trail_load(slot, 0).wait()
        trail_load(slot, 1).wait()
        in_use = lax.broadcasted_iota(jnp.int32, (rank_dim, 1), 0) < ranks[slot]
        v_sketch = jnp.zeros((rank_dim, rank_dim), jnp.float32)
        u_sketch = jnp.zeros((rank_dim, rank_dim), jnp.float32)
        for block in range(n_col):
            lanes = slice(block * w, (block + 1) * w)
            high, low = halves(v_buf[slot, :, lanes])
            rv[slot, 0, :, lanes] = high
            rv[slot, 1, :, lanes] = low
            v_sketch += sketch_of(block, high, low)
            high, low = halves(jnp.where(in_use, u_buf[slot, :, lanes], 0.0))
            ru[slot, 0, :, lanes] = high
            ru[slot, 1, :, lanes] = low
            u_sketch += sketch_of(block, high, low)
        own_sketches[slot, 0] = v_sketch
        own_sketches[slot, 1] = u_sketch

    def own_all():
        for slot in range(slots):
            @pl.when(active(slot))
            def _(slot=slot):
                own_sketch(slot)

    corner = (n_row - row) // n_row
    pl.loop(0, corner)(chunk)

    @pl.when(corner == 1)
    def _():
        own_all()
    pl.semaphore_wait(barrier, 2 * n_row - 1 + z)

    for chip in range(n_z - 1):
        @pl.when(z > chip)
        def _(chip=chip):
            hello(far_sem, row, 2 * chip + core)

    def each_loc(act, higher):
        for chip in range(n_z):
            @pl.when(z < chip if higher else z > chip)
            def _(chip=chip):
                act(loc_copy(col, 2 * chip + core))

    def each_direct(act, higher, slot):
        for chip in (range(1, n_z) if higher else reversed(range(n_z - 1))):
            @when(z < chip if higher else z > chip, direct(slot, chip, z))
            def _(chip=chip):
                act(pu_direct(slot, chip))

    def each_pv(act, slot):
        for step in range(1, n_row):
            target = (row + step) % n_row

            @pl.when(last + target > slot * n_row + row)
            def _(target=target):
                act(pv_copy(slot, row, target))

    def straight(step):
        return step >= n_z - 2

    def each_column(act, block, step, slot=None):
        ours = is_host if slot is None else jnp.logical_and(is_host, host_slot == slot)
        far = straight(step)

        @when(ours, host_wants(x_row))
        def _():
            act(pj_copy(block, 0))

        @when(ours, host_wants(y_row) if far is True else to_y)
        def _():
            act(pj_copy(block, 1))

        if far is not False:
            @when(ours, host_wants(diagonal), far)
            def _():
                act(pj_copy(block, 3))

    def start(copy):
        copy.start()

    def wait_send(copy):
        copy.wait_send()

    def send_lower(slot):
        each_direct(start, False, slot)

        @pl.when(needs(slot, z))
        def _():
            start(pu_partner(slot, col))

    start(loc_copy(col, partner))
    each_loc(start, False)
    each_pv(start, 0)

    @pl.when(z < n_z - 1)
    def _():
        send_lower(0)

    @when(z == 1, needs(0, z))
    def _():
        for slot in range(1, slots):
            send_lower(slot)
    def arrive(slot, step):
        chip = chip_at(step)
        block = 2 * chip + core

        @pl.when(needs(slot, z))
        def _():
            pu_partner(slot, block).wait_recv()

            @when(z == 1, chip >= 2)
            def _():
                pu_relay(slot, block).start()
            pu_partner(slot, block).start()
            each_column(start, block, step, slot)

    def settle_rows(slot, first, final):
        @pl.when(needs(slot, z))
        def _():
            for step in range(first, final):
                pu_partner(slot, 2 * chip_at(step) + other).wait_recv()
        absorb_rows(slot, first, final)

    def pair(step):
        return [2 * chip_at(step) + (core + flip) % 2 for flip in range(2)]

    def column(step):
        @pl.when(is_relay)
        def _():
            for block in pair(step):
                pj_copy(block, 0).wait_recv()

                pj_copy(block, 2).start()

    def settle_column(first, final):
        for step in range(first, final):
            late = straight(step)

            @when(jnp.logical_not(is_owner), wants_column(row),
                  True if late else jnp.logical_not(is_relay))
            def _(step=step):
                for block in pair(step):
                    pj_copy(block, 0).wait_recv()
        absorb_column(first, final)

    def gram_part(slot):
        own_v = pv_all[row].reshape(slots * rank_dim, w)
        own_high, own_low = halves(own_v)
        for source in range(n_row):
            tile = slot * n_row + source

            @pl.when(last + row > tile)
            def _(source=source, tile=tile):
                @pl.when(row != source)
                def _():
                    pv_copy(slot, source, row).wait_recv()
                high, low = halves(pv_all[source, slot])
                both = product(jnp.concatenate([high, low], axis=0), own_high, NT)
                g_part[tile % 2, tile // 2] = (
                    both[:rank_dim] + both[rank_dim:] + product(high, own_low, NT))

    def has_batch(batch):
        return last + row > batch * n_row

    def gram_swap(batch):
        @pl.when(has_batch(batch))
        def _():
            gx_copy(batch).start()

    def gram_sum(batch):
        @pl.when(has_batch(batch))
        def _():
            gx_copy(batch).wait_recv()
            for chip in range(batch * half_z, (batch + 1) * half_z):
                g_sum[chip] = g_part[core, chip] + g_peer[chip]

    def each_gram(act, batch):
        for chip in range(batch * half_z, (batch + 1) * half_z):
            @when(last + row > 2 * chip + core, z != chip)
            def _(chip=chip):
                act(g_copy(z, chip))

    def blocks_of(first, final):
        return [2 * chip_at(step) + flip for step in range(first, final) for flip in range(2)]

    def absorb_rows(slot, first, final):
        @pl.when(active(slot))
        def _():
            total = row_sketch[slot]
            for block in blocks_of(first, final):
                lanes = pl.ds(pl.multiple_of(block * w, w), w)
                high, low = halves(pu_all[block, slot])
                rp[slot, 0, :, lanes] = high
                rp[slot, 1, :, lanes] = low
                total += sketch_of(block, high, low)
            row_sketch[slot] = total

    def absorb_column(first, final):
        @pl.when(any_active)
        def _():
            @pl.when(is_owner)
            def _():
                for block in blocks_of(first, final):
                    pj_all[block] = pu_all[block, owner_slot]
            total = col_sketch[...]
            for block in blocks_of(first, final):
                lanes = pl.ds(pl.multiple_of(block * w, w), w)
                high, low = halves(pj_all[block])
                rj[0, :, lanes] = high
                rj[1, :, lanes] = low
                total += sketch_of(block, high, low)
            col_sketch[...] = total

    def upward():
        @pl.when(z < n_z - 1)
        def _():
            pl.semaphore_wait(far_sem, n_z - 1 - z)
        each_loc(start, True)
        for slot in range(slots):
            each_direct(start, True, slot)

    def points_of(step):
        block = 2 * chip_at(step) + core
        loc_copy(block, partner).wait_recv()
        loc_forward(block).start()

    def early(slot, step):
        @pl.when(jnp.logical_or(z > 0, hosts(slot)))
        def _():
            arrive(slot, step)

    def late(slot, step):
        @when(z == 0, jnp.logical_not(hosts(slot)))
        def _():
            arrive(slot, step)

    top = n_z - 1
    pl.loop(corner, 1)(chunk)

    @pl.when(z == top)
    def _():
        send_lower(0)
    chunks(1, 2)

    @when(z != 1, z < top)
    def _():
        for slot in range(1, slots):
            send_lower(slot)
    for slot in range(1, slots):
        each_pv(start, slot)
    each_column(start, col, 0)

    @pl.when(corner == 0)
    def _():
        own_all()
    upward()

    @pl.when(jnp.logical_or(z == top, jnp.logical_and(z == 1, jnp.logical_not(needs(0, z)))))
    def _():
        for slot in range(1, slots):
            send_lower(slot)
    points_of(1)
    chunks(2, 3)
    @pl.when(z > 0)
    def _():
        arrive(0, 1)
    gram_part(0)

    @pl.when(z > 0)
    def _():
        arrive(0, 2)
    gram_swap(0)
    points_of(2)
    chunks(3, 4)

    @pl.when(z == 0)
    def _():
        arrive(0, 1)
    gram_sum(0)
    for slot in range(1, slots):
        early(slot, 1)

    @when(z == 0, hosts(0))
    def _():
        arrive(0, 2)
    chunks(4, 5)
    for slot in range(1, slots):
        early(slot, 2)
    each_gram(start, 0)
    for slot in range(1, slots):
        gram_part(slot)
    column(0)
    for slot in range(1, slots):
        gram_swap(slot)
    early(0, 3)
    points_of(3)
    chunks(5, 6)
    for slot in range(1, slots):
        gram_sum(slot)
        late(slot, 1)
    late(0, 2)
    for slot in range(1, slots):
        each_gram(start, slot)
    chunks(6, 7)
    for slot in range(1, slots):
        early(slot, 3)
    column(1)
    chunks(7, 8)
    for slot in range(1, slots):
        settle_rows(slot, 0, n_z - 2)
    late(0, 3)
    for slot in range(1, slots):
        late(slot, 2)
    settle_rows(0, 0, n_z)
    pend_acc[...] = acc[...] * matern_scale
    at_diagonal = row == n_row - 1 - owner_row

    @pl.when(jnp.logical_not(at_diagonal))
    def _():
        settle_column(0, n_z - 1)
    for slot in range(1, slots):
        late(slot, 3)
        settle_rows(slot, n_z - 2, n_z - 1)

    wait_send(loc_copy(col, partner))
    for higher in (False, True):
        each_loc(wait_send, higher)
        for slot in range(slots):
            each_direct(wait_send, higher, slot)
    for step in range(1, n_z):
        loc_forward(2 * chip_at(step) + core).wait_send()

    def forwards_done(slot, first, final):
        for step in range(first, final):
            block = 2 * chip_at(step) + core

            @pl.when(needs(slot, z))
            def _(block=block):
                pu_partner(slot, block).wait_send()

            @when(z == 1, chip_at(step) >= 2, needs(slot, z))
            def _(block=block):
                pu_relay(slot, block).wait_send()

    def columns_done(step):
        each_column(wait_send, 2 * chip_at(step) + core, step)
        if not straight(step):
            @pl.when(is_relay)
            def _():
                for block in pair(step):
                    pj_copy(block, 2).wait_send()

    for slot in range(slots):
        each_pv(wait_send, slot)

        @pl.when(has_batch(slot))
        def _(slot=slot):
            gx_copy(slot).wait_send()

    @pl.when(at_diagonal)
    def _():
        settle_column(0, n_z - 1)
    settle_column(n_z - 1, n_z)

    nothing = jnp.zeros((rank_dim, 2 * rank_dim), jnp.bfloat16)

    def stacked(value):
        high, low = halves(value)
        return jnp.concatenate([
            jnp.concatenate([high, high], axis=1), jnp.concatenate([low, nothing], axis=1)
        ], axis=0)

    def right_of(slot):
        @pl.when(active(slot))
        def _():
            lanes = slice(slot * rank_dim, (slot + 1) * rank_dim)
            right_core = dot3(row_sketch[slot], gram_all[:, lanes], NT)
            z_left[slot] = stacked(
                jnp.concatenate([own_sketches[slot, 1], -right_core], axis=1))

    @pl.when(any_active)
    def _():
        gram = g_sum[z]
        for step in range(1, n_z):
            chip = chip_at(step)
            g_copy(chip, z).wait_recv()
            gram = gram + g_all[chip]
        gram_all[...] = gram
        left_core = dot3(col_sketch[...], gram, NN)
        for slot in range(slots):
            lanes = slice(slot * rank_dim, (slot + 1) * rank_dim)

            @pl.when(active(slot))
            def _(slot=slot, lanes=lanes):
                y_left[slot] = stacked(
                    jnp.concatenate([own_sketches[slot, 0], -left_core[:, lanes]], axis=1))
    right_of(0)
    for slot in range(slots):
        each_gram(wait_send, slot)
        forwards_done(slot, 0, n_z - 1)
    forwards_done(0, n_z - 1, n_z)
    for step in range(n_z):
        columns_done(step)
    for slot in range(1, slots):
        settle_rows(slot, n_z - 1, n_z)
        right_of(slot)
    for slot in range(1, slots):
        forwards_done(slot, n_z - 1, n_z)


def finish(
    n_row, ru, rv, rp, rj, y_left, z_left, pend_acc,
    trail_y, trail_z, pend_y, pend_z,
    y_buf, z_buf, out_sem, pend_sem,
):
    row, col = lax.axis_index("row"), lax.axis_index("col")
    slots, _, rank_dim, width = ru.shape
    w = pend_y.shape[3]
    pieces = out_sem.shape[2]
    span = width // pieces

    def pend_copy(slot, which):
        lanes = pl.ds((which * slots + slot) * w, w)
        return pltpu.make_async_copy(
            pend_acc.at[:, lanes], (pend_y, pend_z)[which].at[slot, 0], pend_sem.at[slot, which])

    def out_copy(slot, which, piece):
        lanes = pl.ds(piece * span, span)
        src, dst = ((y_buf, trail_y), (z_buf, trail_z))[which]
        return pltpu.make_async_copy(
            src.at[slot, :, lanes], dst.at[slot, 0, 0, :, lanes], out_sem.at[slot, which, piece])

    for slot in range(slots):
        pend_copy(slot, 0).start()
        pend_copy(slot, 1).start()

    for slot in range(slots):
        active = slot * n_row + row > col

        @pl.when(jnp.logical_not(active))
        def _(slot=slot):
            y_buf[slot] = jnp.zeros((rank_dim, width), jnp.float32)
            z_buf[slot] = jnp.zeros((rank_dim, width), jnp.float32)
            for which in range(2):
                for piece in range(pieces):
                    out_copy(slot, which, piece).start()

        @pl.when(active)
        def _(slot=slot):
            for which in range(2):
                left = (y_left, z_left)[which][slot]
                first = (ru, rv)[which]
                buf = (y_buf, z_buf)[which]
                for piece in range(pieces):
                    lanes = slice(piece * span, (piece + 1) * span)
                    second = [rj[part, :, lanes] if which else rp[slot, part, :, lanes]
                              for part in range(2)]
                    right = jnp.concatenate(
                        [first[slot, 0, :, lanes], second[0], first[slot, 1, :, lanes], second[1]],
                        axis=0)
                    both = product(left, right, NN)
                    buf[slot, :, lanes] = both[:rank_dim] + both[rank_dim:]
                    out_copy(slot, which, piece).start()

    for slot in range(slots):
        for which in range(2):
            pend_copy(slot, which).wait()
            for piece in range(pieces):
                out_copy(slot, which, piece).wait()


def broadcast(block, axis, owner):
    block = jnp.where(lax.axis_index(axis) == owner, block, jnp.zeros_like(block))
    return lax.psum(block, axis)


def matmul(left, right):
    return jnp.dot(left, right, precision=lax.Precision.HIGHEST, preferred_element_type=jnp.float32)


def batched(form, left, right):
    return jnp.einsum(
        form, left, right, precision=lax.Precision.HIGHEST, preferred_element_type=jnp.float32
    )


def matern(row_points, col_points):
    delta_x = row_points[0][:, None] - col_points[0][None, :]
    delta_y = row_points[1][:, None] - col_points[1][None, :]
    distance = jnp.sqrt(delta_x * delta_x + delta_y * delta_y)
    scaled = root_three * distance / length_scale
    return matern_scale * (1.0 + scaled) * jnp.exp(-scaled)


def plain_on_device(trail_u, trail_v, ranks, panel_u, panel_v, locations, pend_locs, sketch):
    row_count = lax.axis_size("row")
    row_index = lax.axis_index("row")
    col_index = lax.axis_index("col")
    row_slots = trail_u.shape[0]
    rank_dim = trail_u.shape[3]
    width = trail_u.shape[4]
    local_width = pend_locs.shape[1]
    gathered_u, gathered_v = (
        lax.all_gather(panel_u, "col", axis=3, tiled=True),
        lax.all_gather(panel_v, "col", axis=3, tiled=True),
    )
    slot_index = col_index // row_count
    own_u = lax.dynamic_index_in_dim(gathered_u[:, 0], slot_index, 0, keepdims=False)
    own_v = lax.dynamic_index_in_dim(gathered_v[:, 0], slot_index, 0, keepdims=False)
    col_pu, col_pv = (
        broadcast(own_u, "row", col_index % row_count),
        broadcast(own_v, "row", col_index % row_count),
    )
    rank_iota = lax.broadcasted_iota(jnp.int32, (row_slots, rank_dim), 1)
    in_use = (rank_iota < ranks[:, 0, 0][:, None]).astype(jnp.float32)
    u_tiles = trail_u[:, 0, 0] * in_use[:, :, None]
    v_tiles = trail_v[:, 0, 0]
    row_pu = gathered_u[:, 0]
    row_pv = gathered_v[:, 0]
    v_sketch = batched("tkn,ln->tkl", v_tiles, sketch)
    u_sketch = batched("tkn,ln->tkl", u_tiles, sketch)
    cross_gram = batched("tkn,ln->tkl", row_pv, col_pv)
    col_sketch = matmul(col_pu, sketch.T)
    row_sketch = batched("tkn,ln->tkl", row_pu, sketch)
    left_core = batched("tkm,ml->tkl", cross_gram, col_sketch)
    y_tiles = batched("tkl,tkn->tln", v_sketch, u_tiles) - batched(
        "tkl,tkn->tln", left_core, row_pu
    )
    right_core = batched("tkl,tkm->tlm", row_sketch, cross_gram)
    z_tiles = batched("tkl,tkn->tln", u_sketch, v_tiles) - batched(
        "tlm,mn->tln", right_core, col_pu
    )
    tile_rows = jnp.arange(row_slots, dtype=jnp.int32) * row_count + row_index
    keep_mask = (tile_rows > col_index)[:, None, None]
    trail_y = jnp.where(keep_mask, y_tiles, 0.0).reshape(row_slots, 1, 1, rank_dim, width)
    trail_z = jnp.where(keep_mask, z_tiles, 0.0).reshape(row_slots, 1, 1, rank_dim, width)
    y_list = []
    z_list = []
    rows_all, pend_all = (
        lax.all_gather(locations, "col", axis=3, tiled=True),
        lax.all_gather(pend_locs.reshape(1, 1, 2, local_width), "col", axis=3, tiled=True),
    )
    col_points = pend_all[0, 0]
    for slot_num in range(row_slots):
        own_kernel = matern(locations[slot_num, 0], col_points)
        y_list.append(matmul(sketch, own_kernel.T))
        col_kernel = matern(rows_all[slot_num, 0], pend_locs)
        z_list.append(matmul(sketch, col_kernel))
    pend_y = jnp.stack(y_list)
    pend_z = jnp.stack(z_list)
    pend_y = pend_y.reshape(row_slots, 1, rank_dim, local_width)
    pend_z = pend_z.reshape(row_slots, 1, rank_dim, local_width)
    return (trail_y, trail_z, pend_y, pend_z)


def on_device(n_row, n_col, trail_u, trail_v, ranks, panel_u, panel_v, locations, pend_locs, sketch):
    slots, _, _, rank_dim, width = trail_u.shape
    w = pend_locs.shape[1]
    n_z = n_col // 2
    fits = n_col == slots * n_row and n_row == 4 and slots == 2
    if w % 128 or rank_dim % 16 or not fits:
        return plain_on_device(
            trail_u, trail_v, ranks, panel_u, panel_v, locations, pend_locs, sketch
        )
    flat = slots * rank_dim
    f32, bf16 = jnp.float32, jnp.bfloat16
    dma = pltpu.SemaphoreType.DMA
    vmem = pl.BlockSpec(memory_space=pltpu.VMEM)
    hbm = pl.BlockSpec(memory_space=pltpu.HBM)
    point_rows = -(-(2 * slots + 2) // 8) * 8
    shape = jax.ShapeDtypeStruct
    kept = pl.pallas_call(
        functools.partial(kernel, n_row, n_col),
        out_shape=(
            pltpu.VMEM((slots, 2, rank_dim, width), bf16),
            pltpu.VMEM((slots, 2, rank_dim, width), bf16),
            pltpu.VMEM((slots, 2, rank_dim, width), bf16),
            pltpu.VMEM((2, rank_dim, width), bf16),
            pltpu.VMEM((slots, 2 * rank_dim, 4 * rank_dim), bf16),
            pltpu.VMEM((slots, 2 * rank_dim, 4 * rank_dim), bf16),
            pltpu.VMEM((rank_dim, 2 * slots * w), f32),
        ),
        in_specs=[hbm] * 8,
        out_specs=(vmem,) * 7,
        scratch_shapes=[
            pltpu.SMEM((slots,), jnp.int32),
            pltpu.VMEM((slots, rank_dim, width), f32),
            pltpu.VMEM((slots, rank_dim, width), f32),
            pltpu.VMEM((rank_dim, width), f32),
            pltpu.VMEM((n_col, slots + 1, 2, w), f32),
            pltpu.VMEM((n_col, slots, rank_dim, w), f32),
            pltpu.VMEM((n_col, rank_dim, w), f32),
            pltpu.VMEM((n_row, slots, rank_dim, w), f32),
            pltpu.VMEM((2, n_z, rank_dim, flat), f32),
            pltpu.VMEM((n_z, rank_dim, flat), f32),
            pltpu.VMEM((n_z, rank_dim, flat), f32),
            pltpu.VMEM((n_z, rank_dim, flat), f32),
            pltpu.VMEM((1, w, point_rows), f32),
            pltpu.VMEM((2, 2 * slots * w), f32),
            pltpu.VMEM((n_col, 2 * rank_dim, w), bf16),
            pltpu.VMEM((w, 2 * slots * w), bf16),
            pltpu.VMEM((w, 2 * slots * w), bf16),
            pltpu.VMEM((rank_dim, 2 * slots * w), f32),
            pltpu.VMEM((slots, 2, rank_dim, rank_dim), f32),
            pltpu.VMEM((slots, rank_dim, rank_dim), f32),
            pltpu.VMEM((rank_dim, rank_dim), f32),
            pltpu.VMEM((rank_dim, flat), f32),
            pltpu.SemaphoreType.REGULAR,
            dma((6,)), dma((slots, 2)), dma((n_col,)), dma((n_col,)), dma((n_col,)),
            dma((slots, n_z)), dma((slots, n_col)), dma((slots, n_col)), dma((slots, n_col)),
            dma((slots, n_row)), dma((slots, n_row)),
            dma((4, n_col)), dma((n_col,)),
            dma((slots,)), dma((slots,)), dma((n_z,)), dma((n_z,)),
        ],
        compiler_params=pltpu.CompilerParams(
            collective_id=0, has_side_effects=True, vmem_limit_bytes=VMEM_LIMIT),
    )(*[
        pltpu.with_memory_space_constraint(value, pltpu.HBM) for value in (
            ranks.reshape(slots),
            trail_u.reshape(slots, rank_dim, width),
            trail_v.reshape(slots, rank_dim, width),
            panel_u.reshape(slots, rank_dim, w),
            panel_v.reshape(slots, rank_dim, w),
            locations.reshape(slots, 2, w),
            pend_locs,
            sketch,
        )
    ])
    kept = [pltpu.with_memory_space_constraint(value, pltpu.VMEM) for value in kept]
    pieces = 2
    return pl.pallas_call(
        functools.partial(finish, n_row),
        out_shape=(
            shape((slots, 1, 1, rank_dim, width), f32),
            shape((slots, 1, 1, rank_dim, width), f32),
            shape((slots, 1, rank_dim, w), f32),
            shape((slots, 1, rank_dim, w), f32),
        ),
        in_specs=[vmem] * 7,
        out_specs=(hbm,) * 4,
        scratch_shapes=[
            pltpu.VMEM((slots, rank_dim, width), f32),
            pltpu.VMEM((slots, rank_dim, width), f32),
            dma((slots, 2, pieces)), dma((slots, 2)),
        ],
        compiler_params=pltpu.CompilerParams(vmem_limit_bytes=VMEM_LIMIT),
    )(*kept)


def solution(mesh):
    in_specs = (
        P(None, "row", "col", None, None),
        P(None, "row", "col", None, None),
        P(None, "row", "col"),
        P(None, "row", None, "col"),
        P(None, "row", None, "col"),
        P(None, "row", None, "col"),
        P(None, "col"),
        P(),
    )
    out_specs = (
        P(None, "row", "col", None, None),
        P(None, "row", "col", None, None),
        P(None, "row", None, "col"),
        P(None, "row", None, "col"),
    )
    body = functools.partial(on_device, mesh.shape["row"], mesh.shape["col"])
    return jax.shard_map(
        body, mesh=mesh, in_specs=in_specs, out_specs=out_specs, check_vma=False
    )
```

```python
import functools
import math

import jax
import jax.numpy as jnp
from jax import lax
from jax.experimental import pallas as pl
from jax.experimental.pallas import tpu as pltpu
from jax.sharding import PartitionSpec as P

matern_scale = 4.0
length_scale = 0.15
root_three = math.sqrt(3.0)
point_scale = root_three / length_scale
log2_e = math.log2(math.e)
smallest = 1e-30

MESH = pl.DeviceIdType.MESH
NN = (((1,), (0,)), ((), ()))
NT = (((1,), (1,)), ((), ()))
SLAB = 16
VMEM_LIMIT = 32 << 20


def halves(value):
    high = value.astype(jnp.bfloat16)
    low = (value - high.astype(jnp.float32)).astype(jnp.bfloat16)
    return high, low


def product(left, right, dims):
    return lax.dot_general(left, right, dims, preferred_element_type=jnp.float32)


def dot3_split(left_both, right, dims):
    rows = left_both.shape[0] // 2
    right_high, right_low = halves(right)
    both = product(left_both, right_high, dims)
    return both[:rows] + both[rows:] + product(left_both[:rows], right_low, dims)


def dot3(left, right, dims):
    left_high, left_low = halves(left)
    return dot3_split(jnp.concatenate([left_high, left_low], axis=0), right, dims)


def kernel(
    n_row, n_col,
    ranks_hbm, trail_u, trail_v, panel_u, panel_v, locs, pend, sketch,
    ru, rv, rp, rj, y_left, z_left, pend_acc,
    ranks, u_buf, v_buf, sk_buf, loc_all, pu_all, pj_all, pv_all, g_part, g_peer, g_sum, g_all,
    points, own_points, sk_both, mat_high, mat_low, acc, own_sketches, row_sketch, col_sketch, gram_all,
    far_sem, load_sem, loc_send, lf_send, loc_recv, pu_send, pf_send, pu_recv,
    pv_send, pv_recv, pj_send, pj_recv, gx_send, gx_recv, g_send, g_recv,
):
    row, col = lax.axis_index("row"), lax.axis_index("col")
    n_z = n_col // 2
    z, core = col // 2, col % 2
    other = 1 - core
    partner = 2 * z + other
    slots, rank_dim, width = u_buf.shape
    w = pu_all.shape[3]
    half_z = n_row // 2
    last = (slots - 1) * n_row
    owner_row, owner_slot = col % n_row, col // n_row
    is_owner = row == owner_row
    x_row = row + 1 - 2 * (row % 2)
    y_row = (row + half_z) % n_row
    diagonal = n_row - 1 - row
    any_active = last + row > col

    def active(slot):
        return slot * n_row + row > col

    def needs(slot, chip):
        return 2 * chip <= slot * n_row + row

    def direct(slot, chip, source):
        near = jnp.logical_or(chip > 0, source < 2)
        return jnp.logical_and(
            needs(slot, chip), jnp.logical_or(near, jnp.logical_not(needs(slot, 1))))

    def hosts(slot):
        return (slot * n_row + row) // 2 == z

    host_slot = 2 * z // n_row
    host_col = host_slot * n_row + row
    is_host = host_col // 2 == z

    def chip_at(step):
        over = (z + step) // n_z
        return z + step + over * (n_z - 1 - 2 * step - z)

    def wants_column(at_row):
        return last + at_row > col

    def remote(src, dst, send, recv, to_row, to_col):
        return pltpu.make_async_remote_copy(
            src_ref=src, dst_ref=dst, send_sem=send, recv_sem=recv,
            device_id=(to_row, to_col), device_id_type=MESH)

    def loc_copy(source, target):
        return remote(loc_all.at[source], loc_all.at[source], loc_send.at[target // 2],
                      loc_recv.at[source], row, target)

    def loc_forward(block):
        return remote(loc_all.at[block], loc_all.at[block], lf_send,
                      loc_recv.at[block], row, partner)

    def pv_copy(slot, source, target):
        return remote(pv_all.at[source, slot], pv_all.at[source, slot],
                      pv_send.at[slot, target], pv_recv.at[slot, source], target, col)

    def pu_copy(slot, block, send, target):
        return remote(pu_all.at[block, slot], pu_all.at[block, slot], send,
                      pu_recv.at[slot, block], row, target)

    def pu_direct(slot, chip):
        return pu_copy(slot, col, pu_send.at[slot, chip], 2 * chip + core)

    def pu_partner(slot, block):
        return pu_copy(slot, block, pf_send.at[slot], partner)

    def pu_relay(slot, block):
        return pu_copy(slot, block, pu_send.at[slot, n_z + block // 2 - 2], core)

    def pj_copy(block, way):
        src = pj_all.at[block] if way == 2 else pu_all.at[block, host_slot]
        return remote(src, pj_all.at[block], pj_send.at[block % 2, block // 2] if way == 2 else pj_send.at[way % 3 + way // 3 * 2, block // 2],
                      pj_recv.at[block],
                      (x_row, y_row, x_row, diagonal)[way], col if way == 2 else host_col)

    def gx_copy(batch):
        chips = pl.ds(batch * half_z, half_z)
        return remote(g_part.at[other, chips], g_peer.at[chips], gx_send.at[batch],
                      gx_recv.at[batch], row, partner)

    def g_copy(source, chip):
        return remote(g_sum.at[chip], g_all.at[source], g_send.at[chip], g_recv.at[source],
                      row, 2 * chip + core)

    def when(*terms):
        return pl.when(functools.reduce(jnp.logical_and, terms))

    def host_wants(at_row):
        return last + at_row > host_col

    to_y = jnp.logical_or(host_wants(y_row), host_wants(diagonal))
    y_of_owner = row == (owner_row + half_z) % n_row
    is_relay = jnp.logical_and(y_of_owner, wants_column(x_row))

    barrier = pltpu.get_barrier_semaphore()

    def hello(semaphore, to_row, to_col):
        pl.semaphore_signal(semaphore, inc=1, device_id=(to_row, to_col), device_id_type=MESH)

    for step in range(1, n_row):
        hello(barrier, (row + step) % n_row, col)
        hello(barrier, (row + step) % n_row, partner)
    hello(barrier, row, partner)
    for chip in range(1, n_z):
        @pl.when(z < chip)
        def _(chip=chip):
            hello(barrier, row, 2 * chip + core)

    loads = [
        pltpu.make_async_copy(locs, loc_all.at[col, pl.ds(0, slots)], load_sem.at[0]),
        pltpu.make_async_copy(pend, loc_all.at[col, slots], load_sem.at[1]),
        pltpu.make_async_copy(panel_v, pv_all.at[row], load_sem.at[2]),
        pltpu.make_async_copy(panel_u, pu_all.at[col], load_sem.at[3]),
        pltpu.make_async_copy(sketch, sk_buf, load_sem.at[4]),
        pltpu.make_async_copy(ranks_hbm, ranks, load_sem.at[5]),
    ]
    for load in loads:
        load.start()

    def trail_load(slot, which):
        src, dst = ((trail_u, u_buf), (trail_v, v_buf))[which]
        return pltpu.make_async_copy(src.at[slot], dst.at[slot], load_sem.at[2 * slot + which])

    for load in loads[:4]:
        load.wait()
    for slot in range(slots):
        @pl.when(active(slot))
        def _(slot=slot):
            trail_load(slot, 0).start()
            trail_load(slot, 1).start()

    def prepare():
        for load in loads[4:]:
            load.wait()
        sk_high, sk_low = halves(sk_buf[...])
        for block in range(n_col):
            sk_both[block, 0:rank_dim] = sk_high[:, block * w:(block + 1) * w]
            sk_both[block, rank_dim:2 * rank_dim] = sk_low[:, block * w:(block + 1) * w]

        acc[...] = jnp.zeros_like(acc)
        row_sketch[...] = jnp.zeros_like(row_sketch)
        col_sketch[...] = jnp.zeros_like(col_sketch)
        own_points[0:1, :] = jnp.concatenate(
            [loc_all[col, slot, 0:1] for slot in range(slots)] + [loc_all[col, slots, 0:1]] * slots,
            axis=1) * point_scale
        own_points[1:2, :] = jnp.concatenate(
            [loc_all[col, slot, 1:2] for slot in range(slots)] + [loc_all[col, slots, 1:2]] * slots,
            axis=1) * point_scale

    pad_rows = points.shape[2] - 2 * slots - 2

    def chunk(step):
        block = 2 * chip_at(step // 2) + (core + step) % 2

        @pl.when(step % 2 == 1)
        def _():
            loc_copy(block, partner).wait_recv()

        stack = [loc_all[block, slot] for slot in range(slots + 1)]
        if pad_rows:
            stack.append(jnp.zeros((pad_rows, w), jnp.float32))
        points[0] = jnp.concatenate(stack, axis=0).T * point_scale

        sk = sk_both[block]
        for part in range(2 * slots):
            base = 2 * slots if part < slots else 2 * (part - slots)
            lanes = slice(part * w, (part + 1) * w)
            for slab in range(w // SLAB):
                rows = slice(slab * SLAB, (slab + 1) * SLAB)
                at = points[0, rows, :]
                delta_x = at[:, base:base + 1] - own_points[0:1, lanes]
                delta_y = at[:, base + 1:base + 2] - own_points[1:2, lanes]
                square = delta_x * delta_x + delta_y * delta_y
                scaled = square * lax.rsqrt(jnp.maximum(square, smallest))
                value = (1.0 + scaled) * jnp.exp2(scaled * -log2_e)
                high, low = halves(value)
                mat_high[rows, lanes] = high
                mat_low[rows, lanes] = low
            both = product(sk, mat_high[:, lanes], NN)
            acc[:, lanes] += (both[:rank_dim] + both[rank_dim:]
                              + product(sk[:rank_dim], mat_low[:, lanes], NN))

    def chunks(first, final):
        pl.loop(first * n_col // 8, final * n_col // 8)(chunk)

    def sketch_of(block, high, low):
        sk = sk_both[block]
        both = product(sk, high, NT)
        return both[:rank_dim] + both[rank_dim:] + product(sk[:rank_dim], low, NT)

    def own_sketch(slot):
        trail_load(slot, 0).wait()
        trail_load(slot, 1).wait()
        in_use = lax.broadcasted_iota(jnp.int32, (rank_dim, 1), 0) < ranks[slot]
        v_sketch = jnp.zeros((rank_dim, rank_dim), jnp.float32)
        u_sketch = jnp.zeros((rank_dim, rank_dim), jnp.float32)
        for block in range(n_col):
            lanes = slice(block * w, (block + 1) * w)
            high, low = halves(v_buf[slot, :, lanes])
            rv[slot, 0, :, lanes] = high
            rv[slot, 1, :, lanes] = low
            v_sketch += sketch_of(block, high, low)
            high, low = halves(jnp.where(in_use, u_buf[slot, :, lanes], 0.0))
            ru[slot, 0, :, lanes] = high
            ru[slot, 1, :, lanes] = low
            u_sketch += sketch_of(block, high, low)
        own_sketches[slot, 0] = v_sketch
        own_sketches[slot, 1] = u_sketch

    def own_all():
        for slot in range(slots):
            @pl.when(active(slot))
            def _(slot=slot):
                own_sketch(slot)

    corner = (n_row - row) // n_row

    @pl.when(corner == 1)
    def _():
        prepare()
        chunk(0)
        own_all()
    pl.semaphore_wait(barrier, 2 * n_row - 1 + z)

    for chip in range(n_z - 1):
        @pl.when(z > chip)
        def _(chip=chip):
            hello(far_sem, row, 2 * chip + core)

    def each_loc(act, higher):
        for chip in range(n_z):
            @pl.when(z < chip if higher else z > chip)
            def _(chip=chip):
                act(loc_copy(col, 2 * chip + core))

    def each_direct(act, higher, slot):
        for chip in (range(1, n_z) if higher else reversed(range(n_z - 1))):
            @when(z < chip if higher else z > chip, direct(slot, chip, z))
            def _(chip=chip):
                act(pu_direct(slot, chip))

    def each_pv(act, slot):
        for step in range(1, n_row):
            target = (row + step) % n_row

            @pl.when(last + target > slot * n_row + row)
            def _(target=target):
                act(pv_copy(slot, row, target))

    def straight(step):
        return step >= n_z - 2

    def each_column(act, block, step, slot=None):
        ours = is_host if slot is None else jnp.logical_and(is_host, host_slot == slot)
        far = straight(step)

        @when(ours, host_wants(x_row))
        def _():
            act(pj_copy(block, 0))

        @when(ours, host_wants(y_row) if far is True else to_y)
        def _():
            act(pj_copy(block, 1))

        if far is not False:
            @when(ours, host_wants(diagonal), far)
            def _():
                act(pj_copy(block, 3))

    def start(copy):
        copy.start()

    def wait_send(copy):
        copy.wait_send()

    def send_lower(slot):
        each_direct(start, False, slot)

        @pl.when(needs(slot, z))
        def _():
            start(pu_partner(slot, col))

    start(loc_copy(col, partner))
    each_loc(start, False)
    each_pv(start, 0)

    @pl.when(z < n_z - 1)
    def _():
        send_lower(0)

    @when(z == 1, needs(0, z))
    def _():
        for slot in range(1, slots):
            send_lower(slot)
    def arrive(slot, step):
        chip = chip_at(step)
        block = 2 * chip + core

        @pl.when(needs(slot, z))
        def _():
            pu_partner(slot, block).wait_recv()

            @when(z == 1, chip >= 2)
            def _():
                pu_relay(slot, block).start()
            pu_partner(slot, col).wait_send()
            pu_partner(slot, block).start()
            each_column(start, block, step, slot)

    def settle_rows(slot, first, final):
        @pl.when(needs(slot, z))
        def _():
            for step in range(first, final):
                pu_partner(slot, 2 * chip_at(step) + other).wait_recv()
        absorb_rows(slot, first, final)

    def pair(step):
        return [2 * chip_at(step) + (core + flip) % 2 for flip in range(2)]

    def column(step):
        @pl.when(is_relay)
        def _():
            for block in pair(step):
                pj_copy(block, 0).wait_recv()

                pj_copy(block, 2).start()

    def settle_column(first, final):
        for step in range(first, final):
            late = straight(step)

            @when(jnp.logical_not(is_owner), wants_column(row),
                  True if late else jnp.logical_not(is_relay))
            def _(step=step):
                for block in pair(step):
                    pj_copy(block, 0).wait_recv()
        absorb_column(first, final)

    def gram_part(slot):
        own_v = pv_all[row].reshape(slots * rank_dim, w)
        own_high, own_low = halves(own_v)
        for source in range(n_row):
            tile = slot * n_row + source

            @pl.when(last + row > tile)
            def _(source=source, tile=tile):
                @pl.when(row != source)
                def _():
                    pv_copy(slot, source, row).wait_recv()
                high, low = halves(pv_all[source, slot])
                both = product(jnp.concatenate([high, low], axis=0), own_high, NT)
                g_part[tile % 2, tile // 2] = (
                    both[:rank_dim] + both[rank_dim:] + product(high, own_low, NT))

    def has_batch(batch):
        return last + row > batch * n_row

    def gram_swap(batch):
        @pl.when(has_batch(batch))
        def _():
            gx_copy(batch).start()

    def gram_sum(batch):
        @pl.when(has_batch(batch))
        def _():
            gx_copy(batch).wait_recv()
            for chip in range(batch * half_z, (batch + 1) * half_z):
                g_sum[chip] = g_part[core, chip] + g_peer[chip]

    def each_gram(act, batch):
        for chip in range(batch * half_z, (batch + 1) * half_z):
            @when(last + row > 2 * chip + core, z != chip)
            def _(chip=chip):
                act(g_copy(z, chip))

    def blocks_of(first, final):
        return [2 * chip_at(step) + flip for step in range(first, final) for flip in range(2)]

    def absorb_rows(slot, first, final):
        @pl.when(active(slot))
        def _():
            total = row_sketch[slot]
            for block in blocks_of(first, final):
                lanes = pl.ds(pl.multiple_of(block * w, w), w)
                high, low = halves(pu_all[block, slot])
                rp[slot, 0, :, lanes] = high
                rp[slot, 1, :, lanes] = low
                total += sketch_of(block, high, low)
            row_sketch[slot] = total

    def absorb_column(first, final):
        @pl.when(any_active)
        def _():
            @pl.when(is_owner)
            def _():
                for block in blocks_of(first, final):
                    pj_all[block] = pu_all[block, owner_slot]
            total = col_sketch[...]
            for block in blocks_of(first, final):
                lanes = pl.ds(pl.multiple_of(block * w, w), w)
                high, low = halves(pj_all[block])
                rj[0, :, lanes] = high
                rj[1, :, lanes] = low
                total += sketch_of(block, high, low)
            col_sketch[...] = total

    def upward():
        @pl.when(z < n_z - 1)
        def _():
            pl.semaphore_wait(far_sem, n_z - 1 - z)
        each_loc(start, True)
        for slot in range(slots):
            each_direct(start, True, slot)

    def points_of(step):
        block = 2 * chip_at(step) + core
        loc_copy(block, partner).wait_recv()
        if step > 1:
            loc_forward(block).wait_send()
        loc_forward(block).start()

    def early(slot, step):
        @pl.when(jnp.logical_or(z > 0, hosts(slot)))
        def _():
            arrive(slot, step)

    def late(slot, step):
        @when(z == 0, jnp.logical_not(hosts(slot)))
        def _():
            arrive(slot, step)

    top = n_z - 1

    @pl.when(corner == 0)
    def _():
        prepare()
        chunk(0)

    @pl.when(z == top)
    def _():
        send_lower(0)
    chunks(1, 2)

    @when(z != 1, z < top)
    def _():
        for slot in range(1, slots):
            send_lower(slot)
    for slot in range(1, slots):
        each_pv(start, slot)
    each_column(start, col, 0)

    @pl.when(corner == 0)
    def _():
        own_all()
    upward()

    @pl.when(jnp.logical_or(z == top, jnp.logical_and(z == 1, jnp.logical_not(needs(0, z)))))
    def _():
        for slot in range(1, slots):
            send_lower(slot)
    points_of(1)
    chunks(2, 3)
    @pl.when(z > 0)
    def _():
        arrive(0, 1)
    gram_part(0)

    @pl.when(z > 0)
    def _():
        arrive(0, 2)
    gram_swap(0)
    points_of(2)
    chunks(3, 4)

    @pl.when(z == 0)
    def _():
        arrive(0, 1)
    gram_sum(0)
    for slot in range(1, slots):
        early(slot, 1)

    @when(z == 0, hosts(0))
    def _():
        arrive(0, 2)
    chunks(4, 5)
    for slot in range(1, slots):
        early(slot, 2)
    each_gram(start, 0)
    for slot in range(1, slots):
        gram_part(slot)
    column(0)
    for slot in range(1, slots):
        gram_swap(slot)
    early(0, 3)
    points_of(3)
    chunks(5, 6)
    for slot in range(1, slots):
        gram_sum(slot)
        late(slot, 1)
    late(0, 2)
    for slot in range(1, slots):
        each_gram(start, slot)
    chunks(6, 7)
    for slot in range(1, slots):
        early(slot, 3)
    late(0, 3)
    chunks(7, 8)
    for slot in range(1, slots):
        settle_rows(slot, 0, n_z - 2)
    column(1)
    for slot in range(1, slots):
        late(slot, 2)
    settle_rows(0, 0, n_z)
    pend_acc[...] = acc[...] * matern_scale
    at_diagonal = row == n_row - 1 - owner_row

    @pl.when(jnp.logical_not(at_diagonal))
    def _():
        settle_column(0, n_z - 2)
    for slot in range(1, slots):
        late(slot, 3)
        settle_rows(slot, n_z - 2, n_z - 1)

    wait_send(loc_copy(col, partner))
    for higher in (False, True):
        each_loc(wait_send, higher)
        for slot in range(slots):
            each_direct(wait_send, higher, slot)
    loc_forward(col).wait_send()

    def relays_done(slot):
        for step in range(1, n_z):
            block = 2 * chip_at(step) + core

            @when(z == 1, chip_at(step) >= 2, needs(slot, z))
            def _(block=block):
                pu_relay(slot, block).wait_send()

    def forwards_done(slot):
        @pl.when(needs(slot, z))
        def _():
            pu_partner(slot, col).wait_send()

    def columns_done(step):
        each_column(wait_send, 2 * chip_at(step) + core, step)
        if not straight(step):
            @pl.when(is_relay)
            def _():
                for block in pair(step):
                    pj_copy(block, 2).wait_send()

    for slot in range(slots):
        each_pv(wait_send, slot)

        @pl.when(has_batch(slot))
        def _(slot=slot):
            gx_copy(slot).wait_send()

    @pl.when(at_diagonal)
    def _():
        settle_column(0, n_z - 2)
    settle_column(n_z - 2, n_z)

    nothing = jnp.zeros((rank_dim, 2 * rank_dim), jnp.bfloat16)

    def stacked(value):
        high, low = halves(value)
        return jnp.concatenate([
            jnp.concatenate([high, high], axis=1), jnp.concatenate([low, nothing], axis=1)
        ], axis=0)

    def right_of(slot):
        @pl.when(active(slot))
        def _():
            lanes = slice(slot * rank_dim, (slot + 1) * rank_dim)
            right_core = dot3(row_sketch[slot], gram_all[:, lanes], NT)
            z_left[slot] = stacked(
                jnp.concatenate([own_sketches[slot, 1], -right_core], axis=1))

    @pl.when(any_active)
    def _():
        gram = g_sum[z]
        for step in range(1, n_z):
            chip = chip_at(step)
            g_copy(chip, z).wait_recv()
            gram = gram + g_all[chip]
        gram_all[...] = gram
        left_core = dot3(col_sketch[...], gram, NN)
        for slot in range(slots):
            lanes = slice(slot * rank_dim, (slot + 1) * rank_dim)

            @pl.when(active(slot))
            def _(slot=slot, lanes=lanes):
                y_left[slot] = stacked(
                    jnp.concatenate([own_sketches[slot, 0], -left_core[:, lanes]], axis=1))
    right_of(0)
    for slot in range(slots):
        each_gram(wait_send, slot)
        relays_done(slot)
    forwards_done(0)
    for step in range(n_z):
        columns_done(step)
    for slot in range(1, slots):
        forwards_done(slot)
        settle_rows(slot, n_z - 1, n_z)
        right_of(slot)


def finish(
    n_row, ru, rv, rp, rj, y_left, z_left, pend_acc,
    trail_y, trail_z, pend_y, pend_z,
    y_buf, z_buf, out_sem, pend_sem,
):
    row, col = lax.axis_index("row"), lax.axis_index("col")
    slots, _, rank_dim, width = ru.shape
    w = pend_y.shape[3]
    pieces = out_sem.shape[2]
    span = width // pieces

    def pend_copy(slot, which):
        lanes = pl.ds((which * slots + slot) * w, w)
        return pltpu.make_async_copy(
            pend_acc.at[:, lanes], (pend_y, pend_z)[which].at[slot, 0], pend_sem.at[slot, which])

    def out_copy(slot, which, piece):
        lanes = pl.ds(piece * span, span)
        src, dst = ((y_buf, trail_y), (z_buf, trail_z))[which]
        return pltpu.make_async_copy(
            src.at[slot, :, lanes], dst.at[slot, 0, 0, :, lanes], out_sem.at[slot, which, piece])

    for slot in range(slots):
        pend_copy(slot, 0).start()
        pend_copy(slot, 1).start()

    for slot in range(slots):
        active = slot * n_row + row > col

        @pl.when(jnp.logical_not(active))
        def _(slot=slot):
            y_buf[slot] = jnp.zeros((rank_dim, width), jnp.float32)
            z_buf[slot] = jnp.zeros((rank_dim, width), jnp.float32)
            for which in range(2):
                for piece in range(pieces):
                    out_copy(slot, which, piece).start()

        @pl.when(active)
        def _(slot=slot):
            for which in range(2):
                left = (y_left, z_left)[which][slot]
                first = (ru, rv)[which]
                buf = (y_buf, z_buf)[which]
                for piece in range(pieces):
                    lanes = slice(piece * span, (piece + 1) * span)
                    second = [rj[part, :, lanes] if which else rp[slot, part, :, lanes]
                              for part in range(2)]
                    right = jnp.concatenate(
                        [first[slot, 0, :, lanes], second[0], first[slot, 1, :, lanes], second[1]],
                        axis=0)
                    both = product(left, right, NN)
                    buf[slot, :, lanes] = both[:rank_dim] + both[rank_dim:]
                    out_copy(slot, which, piece).start()

    for slot in range(slots):
        for which in range(2):
            pend_copy(slot, which).wait()
            for piece in range(pieces):
                out_copy(slot, which, piece).wait()


def broadcast(block, axis, owner):
    block = jnp.where(lax.axis_index(axis) == owner, block, jnp.zeros_like(block))
    return lax.psum(block, axis)


def matmul(left, right):
    return jnp.dot(left, right, precision=lax.Precision.HIGHEST, preferred_element_type=jnp.float32)


def batched(form, left, right):
    return jnp.einsum(
        form, left, right, precision=lax.Precision.HIGHEST, preferred_element_type=jnp.float32
    )


def matern(row_points, col_points):
    delta_x = row_points[0][:, None] - col_points[0][None, :]
    delta_y = row_points[1][:, None] - col_points[1][None, :]
    distance = jnp.sqrt(delta_x * delta_x + delta_y * delta_y)
    scaled = root_three * distance / length_scale
    return matern_scale * (1.0 + scaled) * jnp.exp(-scaled)


def plain_on_device(trail_u, trail_v, ranks, panel_u, panel_v, locations, pend_locs, sketch):
    row_count = lax.axis_size("row")
    row_index = lax.axis_index("row")
    col_index = lax.axis_index("col")
    row_slots = trail_u.shape[0]
    rank_dim = trail_u.shape[3]
    width = trail_u.shape[4]
    local_width = pend_locs.shape[1]
    gathered_u, gathered_v = (
        lax.all_gather(panel_u, "col", axis=3, tiled=True),
        lax.all_gather(panel_v, "col", axis=3, tiled=True),
    )
    slot_index = col_index // row_count
    own_u = lax.dynamic_index_in_dim(gathered_u[:, 0], slot_index, 0, keepdims=False)
    own_v = lax.dynamic_index_in_dim(gathered_v[:, 0], slot_index, 0, keepdims=False)
    col_pu, col_pv = (
        broadcast(own_u, "row", col_index % row_count),
        broadcast(own_v, "row", col_index % row_count),
    )
    rank_iota = lax.broadcasted_iota(jnp.int32, (row_slots, rank_dim), 1)
    in_use = (rank_iota < ranks[:, 0, 0][:, None]).astype(jnp.float32)
    u_tiles = trail_u[:, 0, 0] * in_use[:, :, None]
    v_tiles = trail_v[:, 0, 0]
    row_pu = gathered_u[:, 0]
    row_pv = gathered_v[:, 0]
    v_sketch = batched("tkn,ln->tkl", v_tiles, sketch)
    u_sketch = batched("tkn,ln->tkl", u_tiles, sketch)
    cross_gram = batched("tkn,ln->tkl", row_pv, col_pv)
    col_sketch = matmul(col_pu, sketch.T)
    row_sketch = batched("tkn,ln->tkl", row_pu, sketch)
    left_core = batched("tkm,ml->tkl", cross_gram, col_sketch)
    y_tiles = batched("tkl,tkn->tln", v_sketch, u_tiles) - batched(
        "tkl,tkn->tln", left_core, row_pu
    )
    right_core = batched("tkl,tkm->tlm", row_sketch, cross_gram)
    z_tiles = batched("tkl,tkn->tln", u_sketch, v_tiles) - batched(
        "tlm,mn->tln", right_core, col_pu
    )
    tile_rows = jnp.arange(row_slots, dtype=jnp.int32) * row_count + row_index
    keep_mask = (tile_rows > col_index)[:, None, None]
    trail_y = jnp.where(keep_mask, y_tiles, 0.0).reshape(row_slots, 1, 1, rank_dim, width)
    trail_z = jnp.where(keep_mask, z_tiles, 0.0).reshape(row_slots, 1, 1, rank_dim, width)
    y_list = []
    z_list = []
    rows_all, pend_all = (
        lax.all_gather(locations, "col", axis=3, tiled=True),
        lax.all_gather(pend_locs.reshape(1, 1, 2, local_width), "col", axis=3, tiled=True),
    )
    col_points = pend_all[0, 0]
    for slot_num in range(row_slots):
        own_kernel = matern(locations[slot_num, 0], col_points)
        y_list.append(matmul(sketch, own_kernel.T))
        col_kernel = matern(rows_all[slot_num, 0], pend_locs)
        z_list.append(matmul(sketch, col_kernel))
    pend_y = jnp.stack(y_list)
    pend_z = jnp.stack(z_list)
    pend_y = pend_y.reshape(row_slots, 1, rank_dim, local_width)
    pend_z = pend_z.reshape(row_slots, 1, rank_dim, local_width)
    return (trail_y, trail_z, pend_y, pend_z)


def on_device(n_row, n_col, trail_u, trail_v, ranks, panel_u, panel_v, locations, pend_locs, sketch):
    slots, _, _, rank_dim, width = trail_u.shape
    w = pend_locs.shape[1]
    n_z = n_col // 2
    fits = n_col == slots * n_row and n_row == 4 and slots == 2
    if w % 128 or rank_dim % 16 or not fits:
        return plain_on_device(
            trail_u, trail_v, ranks, panel_u, panel_v, locations, pend_locs, sketch
        )
    flat = slots * rank_dim
    f32, bf16 = jnp.float32, jnp.bfloat16
    dma = pltpu.SemaphoreType.DMA
    vmem = pl.BlockSpec(memory_space=pltpu.VMEM)
    hbm = pl.BlockSpec(memory_space=pltpu.HBM)
    point_rows = -(-(2 * slots + 2) // 8) * 8
    shape = jax.ShapeDtypeStruct
    kept = pl.pallas_call(
        functools.partial(kernel, n_row, n_col),
        out_shape=(
            pltpu.VMEM((slots, 2, rank_dim, width), bf16),
            pltpu.VMEM((slots, 2, rank_dim, width), bf16),
            pltpu.VMEM((slots, 2, rank_dim, width), bf16),
            pltpu.VMEM((2, rank_dim, width), bf16),
            pltpu.VMEM((slots, 2 * rank_dim, 4 * rank_dim), bf16),
            pltpu.VMEM((slots, 2 * rank_dim, 4 * rank_dim), bf16),
            pltpu.VMEM((rank_dim, 2 * slots * w), f32),
        ),
        in_specs=[hbm] * 8,
        out_specs=(vmem,) * 7,
        scratch_shapes=[
            pltpu.SMEM((slots,), jnp.int32),
            pltpu.VMEM((slots, rank_dim, width), f32),
            pltpu.VMEM((slots, rank_dim, width), f32),
            pltpu.VMEM((rank_dim, width), f32),
            pltpu.VMEM((n_col, slots + 1, 2, w), f32),
            pltpu.VMEM((n_col, slots, rank_dim, w), f32),
            pltpu.VMEM((n_col, rank_dim, w), f32),
            pltpu.VMEM((n_row, slots, rank_dim, w), f32),
            pltpu.VMEM((2, n_z, rank_dim, flat), f32),
            pltpu.VMEM((n_z, rank_dim, flat), f32),
            pltpu.VMEM((n_z, rank_dim, flat), f32),
            pltpu.VMEM((n_z, rank_dim, flat), f32),
            pltpu.VMEM((1, w, point_rows), f32),
            pltpu.VMEM((2, 2 * slots * w), f32),
            pltpu.VMEM((n_col, 2 * rank_dim, w), bf16),
            pltpu.VMEM((w, 2 * slots * w), bf16),
            pltpu.VMEM((w, 2 * slots * w), bf16),
            pltpu.VMEM((rank_dim, 2 * slots * w), f32),
            pltpu.VMEM((slots, 2, rank_dim, rank_dim), f32),
            pltpu.VMEM((slots, rank_dim, rank_dim), f32),
            pltpu.VMEM((rank_dim, rank_dim), f32),
            pltpu.VMEM((rank_dim, flat), f32),
            pltpu.SemaphoreType.REGULAR,
            dma((6,)), dma((n_z,)), dma, dma((n_col,)),
            dma((slots, 2 * n_z - 2)), dma((slots,)), dma((slots, n_col)),
            dma((slots, n_row)), dma((slots, n_row)),
            dma((3, n_z)), dma((n_col,)),
            dma((slots,)), dma((slots,)), dma((n_z,)), dma((n_z,)),
        ],
        compiler_params=pltpu.CompilerParams(
            collective_id=0, has_side_effects=True, vmem_limit_bytes=VMEM_LIMIT),
    )(*[
        pltpu.with_memory_space_constraint(value, pltpu.HBM) for value in (
            ranks.reshape(slots),
            trail_u.reshape(slots, rank_dim, width),
            trail_v.reshape(slots, rank_dim, width),
            panel_u.reshape(slots, rank_dim, w),
            panel_v.reshape(slots, rank_dim, w),
            locations.reshape(slots, 2, w),
            pend_locs,
            sketch,
        )
    ])
    kept = [pltpu.with_memory_space_constraint(value, pltpu.VMEM) for value in kept]
    pieces = 4
    return pl.pallas_call(
        functools.partial(finish, n_row),
        out_shape=(
            shape((slots, 1, 1, rank_dim, width), f32),
            shape((slots, 1, 1, rank_dim, width), f32),
            shape((slots, 1, rank_dim, w), f32),
            shape((slots, 1, rank_dim, w), f32),
        ),
        in_specs=[vmem] * 7,
        out_specs=(hbm,) * 4,
        scratch_shapes=[
            pltpu.VMEM((slots, rank_dim, width), f32),
            pltpu.VMEM((slots, rank_dim, width), f32),
            dma((slots, 2, pieces)), dma((slots, 2)),
        ],
        compiler_params=pltpu.CompilerParams(vmem_limit_bytes=VMEM_LIMIT),
    )(*kept)


def solution(mesh):
    in_specs = (
        P(None, "row", "col", None, None),
        P(None, "row", "col", None, None),
        P(None, "row", "col"),
        P(None, "row", None, "col"),
        P(None, "row", None, "col"),
        P(None, "row", None, "col"),
        P(None, "col"),
        P(),
    )
    out_specs = (
        P(None, "row", "col", None, None),
        P(None, "row", "col", None, None),
        P(None, "row", None, "col"),
        P(None, "row", None, "col"),
    )
    body = functools.partial(on_device, mesh.shape["row"], mesh.shape["col"])
    return jax.shard_map(
        body, mesh=mesh, in_specs=in_specs, out_specs=out_specs, check_vma=False
    )
```

```python
import functools
import math

import jax
import jax.numpy as jnp
from jax import lax
from jax.experimental import pallas as pl
from jax.experimental.pallas import tpu as pltpu
from jax.sharding import PartitionSpec as P

matern_scale = 4.0
length_scale = 0.15
root_three = math.sqrt(3.0)
point_scale = root_three / length_scale
log2_e = math.log2(math.e)
smallest = 1e-30

MESH = pl.DeviceIdType.MESH
NN = (((1,), (0,)), ((), ()))
NT = (((1,), (1,)), ((), ()))
SLAB = 16
VMEM_LIMIT = 32 << 20


def halves(value):
    high = value.astype(jnp.bfloat16)
    low = (value - high.astype(jnp.float32)).astype(jnp.bfloat16)
    return high, low


def product(left, right, dims):
    return lax.dot_general(left, right, dims, preferred_element_type=jnp.float32)


def dot3_split(left_both, right, dims):
    rows = left_both.shape[0] // 2
    right_high, right_low = halves(right)
    both = product(left_both, right_high, dims)
    return both[:rows] + both[rows:] + product(left_both[:rows], right_low, dims)


def dot3(left, right, dims):
    left_high, left_low = halves(left)
    return dot3_split(jnp.concatenate([left_high, left_low], axis=0), right, dims)


def kernel(
    n_row, n_col,
    ranks_hbm, trail_u, trail_v, panel_u, panel_v, locs, pend, sketch,
    ru, rv, rp, rj, y_left, z_left, pend_acc,
    ranks, u_buf, v_buf, sk_buf, loc_all, pu_all, pj_all, pv_all, g_part, g_peer, g_sum, g_all,
    points, own_points, sk_both, mat_high, mat_low, acc, own_sketches, row_sketch, col_sketch, gram_all,
    far_sem, load_sem, loc_send, lf_send, loc_recv, pu_send, pf_send, pu_recv,
    pv_send, pv_recv, pj_send, pj_recv, gx_send, gx_recv, g_send, g_recv,
):
    row, col = lax.axis_index("row"), lax.axis_index("col")
    n_z = n_col // 2
    z, core = col // 2, col % 2
    other = 1 - core
    partner = 2 * z + other
    slots, rank_dim, width = u_buf.shape
    w = pu_all.shape[3]
    half_z = n_row // 2
    last = (slots - 1) * n_row
    owner_row, owner_slot = col % n_row, col // n_row
    is_owner = row == owner_row
    x_row = row + 1 - 2 * (row % 2)
    y_row = (row + half_z) % n_row
    diagonal = n_row - 1 - row
    any_active = last + row > col

    def active(slot):
        return slot * n_row + row > col

    def needs(slot, chip):
        return 2 * chip <= slot * n_row + row

    def direct(slot, chip, source):
        near = jnp.logical_or(chip > 0, source < 2)
        return jnp.logical_and(
            needs(slot, chip), jnp.logical_or(near, jnp.logical_not(needs(slot, 1))))

    def hosts(slot):
        return (slot * n_row + row) // 2 == z

    host_slot = 2 * z // n_row
    host_col = host_slot * n_row + row
    is_host = host_col // 2 == z

    def chip_at(step):
        over = (z + step) // n_z
        return z + step + over * (n_z - 1 - 2 * step - z)

    def wants_column(at_row):
        return last + at_row > col

    def remote(src, dst, send, recv, to_row, to_col):
        return pltpu.make_async_remote_copy(
            src_ref=src, dst_ref=dst, send_sem=send, recv_sem=recv,
            device_id=(to_row, to_col), device_id_type=MESH)

    def loc_copy(source, target):
        return remote(loc_all.at[source], loc_all.at[source], loc_send.at[target // 2],
                      loc_recv.at[source], row, target)

    def loc_forward(block):
        return remote(loc_all.at[block], loc_all.at[block], lf_send,
                      loc_recv.at[block], row, partner)

    def pv_copy(slot, source, target):
        return remote(pv_all.at[source, slot], pv_all.at[source, slot],
                      pv_send.at[slot, target], pv_recv.at[slot, source], target, col)

    def pu_copy(slot, block, send, target):
        return remote(pu_all.at[block, slot], pu_all.at[block, slot], send,
                      pu_recv.at[slot, block], row, target)

    def pu_direct(slot, chip):
        return pu_copy(slot, col, pu_send.at[slot, chip], 2 * chip + core)

    def pu_partner(slot, block):
        return pu_copy(slot, block, pf_send.at[slot], partner)

    def pu_relay(slot, block):
        return pu_copy(slot, block, pu_send.at[slot, n_z + block // 2 - 2], core)

    def pj_copy(block, way):
        src = pj_all.at[block] if way == 2 else pu_all.at[block, host_slot]
        return remote(src, pj_all.at[block], pj_send.at[block % 2, block // 2] if way == 2 else pj_send.at[way % 3 + way // 3 * 2, block // 2],
                      pj_recv.at[block],
                      (x_row, y_row, x_row, diagonal)[way], col if way == 2 else host_col)

    def gx_copy(batch):
        chips = pl.ds(batch * half_z, half_z)
        return remote(g_part.at[other, chips], g_peer.at[chips], gx_send.at[batch],
                      gx_recv.at[batch], row, partner)

    def g_copy(source, chip):
        return remote(g_sum.at[chip], g_all.at[source], g_send.at[chip], g_recv.at[source],
                      row, 2 * chip + core)

    def when(*terms):
        return pl.when(functools.reduce(jnp.logical_and, terms))

    def host_wants(at_row):
        return last + at_row > host_col

    to_y = jnp.logical_or(host_wants(y_row), host_wants(diagonal))
    y_of_owner = row == (owner_row + half_z) % n_row
    is_relay = jnp.logical_and(y_of_owner, wants_column(x_row))

    barrier = pltpu.get_barrier_semaphore()

    def hello(semaphore, to_row, to_col):
        pl.semaphore_signal(semaphore, inc=1, device_id=(to_row, to_col), device_id_type=MESH)

    for step in range(1, n_row):
        hello(barrier, (row + step) % n_row, col)
        hello(barrier, (row + step) % n_row, partner)
    hello(barrier, row, partner)
    for chip in range(1, n_z):
        @pl.when(z < chip)
        def _(chip=chip):
            hello(barrier, row, 2 * chip + core)

    loads = [
        pltpu.make_async_copy(locs, loc_all.at[col, pl.ds(0, slots)], load_sem.at[0]),
        pltpu.make_async_copy(pend, loc_all.at[col, slots], load_sem.at[1]),
        pltpu.make_async_copy(panel_v, pv_all.at[row], load_sem.at[2]),
        pltpu.make_async_copy(panel_u, pu_all.at[col], load_sem.at[3]),
        pltpu.make_async_copy(sketch, sk_buf, load_sem.at[4]),
        pltpu.make_async_copy(ranks_hbm, ranks, load_sem.at[5]),
    ]
    for load in loads:
        load.start()

    def trail_load(slot, which):
        src, dst = ((trail_u, u_buf), (trail_v, v_buf))[which]
        return pltpu.make_async_copy(src.at[slot], dst.at[slot], load_sem.at[2 * slot + which])

    for load in loads[:4]:
        load.wait()
    for slot in range(slots):
        @pl.when(active(slot))
        def _(slot=slot):
            trail_load(slot, 0).start()
            trail_load(slot, 1).start()

    def prepare():
        for load in loads[4:]:
            load.wait()
        sk_high, sk_low = halves(sk_buf[...])
        for block in range(n_col):
            sk_both[block, 0:rank_dim] = sk_high[:, block * w:(block + 1) * w]
            sk_both[block, rank_dim:2 * rank_dim] = sk_low[:, block * w:(block + 1) * w]

        acc[...] = jnp.zeros_like(acc)
        row_sketch[...] = jnp.zeros_like(row_sketch)
        col_sketch[...] = jnp.zeros_like(col_sketch)
        own_points[0:1, :] = jnp.concatenate(
            [loc_all[col, slot, 0:1] for slot in range(slots)] + [loc_all[col, slots, 0:1]] * slots,
            axis=1) * point_scale
        own_points[1:2, :] = jnp.concatenate(
            [loc_all[col, slot, 1:2] for slot in range(slots)] + [loc_all[col, slots, 1:2]] * slots,
            axis=1) * point_scale

    pad_rows = points.shape[2] - 2 * slots - 2

    def chunk(step):
        block = 2 * chip_at(step // 2) + (core + step) % 2

        @pl.when(step % 2 == 1)
        def _():
            loc_copy(block, partner).wait_recv()

        stack = [loc_all[block, slot] for slot in range(slots + 1)]
        if pad_rows:
            stack.append(jnp.zeros((pad_rows, w), jnp.float32))
        points[0] = jnp.concatenate(stack, axis=0).T * point_scale

        sk = sk_both[block]
        for part in range(2 * slots):
            base = 2 * slots if part < slots else 2 * (part - slots)
            lanes = slice(part * w, (part + 1) * w)
            for slab in range(w // SLAB):
                rows = slice(slab * SLAB, (slab + 1) * SLAB)
                at = points[0, rows, :]
                delta_x = at[:, base:base + 1] - own_points[0:1, lanes]
                delta_y = at[:, base + 1:base + 2] - own_points[1:2, lanes]
                square = delta_x * delta_x + delta_y * delta_y
                scaled = square * lax.rsqrt(jnp.maximum(square, smallest))
                value = (1.0 + scaled) * jnp.exp2(scaled * -log2_e)
                high, low = halves(value)
                mat_high[rows, lanes] = high
                mat_low[rows, lanes] = low
            both = product(sk, mat_high[:, lanes], NN)
            acc[:, lanes] += (both[:rank_dim] + both[rank_dim:]
                              + product(sk[:rank_dim], mat_low[:, lanes], NN))

    def chunks(first, final):
        pl.loop(first * n_col // 8, final * n_col // 8)(chunk)

    def sketch_of(block, high, low):
        sk = sk_both[block]
        both = product(sk, high, NT)
        return both[:rank_dim] + both[rank_dim:] + product(sk[:rank_dim], low, NT)

    def own_sketch(slot):
        trail_load(slot, 0).wait()
        trail_load(slot, 1).wait()
        in_use = lax.broadcasted_iota(jnp.int32, (rank_dim, 1), 0) < ranks[slot]
        v_sketch = jnp.zeros((rank_dim, rank_dim), jnp.float32)
        u_sketch = jnp.zeros((rank_dim, rank_dim), jnp.float32)
        for block in range(n_col):
            lanes = slice(block * w, (block + 1) * w)
            high, low = halves(v_buf[slot, :, lanes])
            rv[slot, 0, :, lanes] = high
            rv[slot, 1, :, lanes] = low
            v_sketch += sketch_of(block, high, low)
            high, low = halves(jnp.where(in_use, u_buf[slot, :, lanes], 0.0))
            ru[slot, 0, :, lanes] = high
            ru[slot, 1, :, lanes] = low
            u_sketch += sketch_of(block, high, low)
        own_sketches[slot, 0] = v_sketch
        own_sketches[slot, 1] = u_sketch

    def own_all():
        for slot in range(slots):
            @pl.when(active(slot))
            def _(slot=slot):
                own_sketch(slot)

    corner = (n_row - row) // n_row

    @pl.when(corner == 1)
    def _():
        prepare()
        chunk(0)
        own_all()
    pl.semaphore_wait(barrier, 2 * n_row - 1 + z)

    for chip in range(n_z - 1):
        @pl.when(z > chip)
        def _(chip=chip):
            hello(far_sem, row, 2 * chip + core)

    def each_loc(act, higher):
        for chip in range(n_z):
            @pl.when(z < chip if higher else z > chip)
            def _(chip=chip):
                act(loc_copy(col, 2 * chip + core))

    def each_direct(act, higher, slot):
        for chip in (range(1, n_z) if higher else reversed(range(n_z - 1))):
            @when(z < chip if higher else z > chip, direct(slot, chip, z))
            def _(chip=chip):
                act(pu_direct(slot, chip))

    def each_pv(act, slot):
        for step in range(1, n_row):
            target = (row + step) % n_row

            @pl.when(last + target > slot * n_row + row)
            def _(target=target):
                act(pv_copy(slot, row, target))

    def straight(step):
        return step >= n_z - 2

    def each_column(act, block, step, slot=None):
        ours = is_host if slot is None else jnp.logical_and(is_host, host_slot == slot)
        far = straight(step)

        @when(ours, host_wants(x_row))
        def _():
            act(pj_copy(block, 0))

        @when(ours, host_wants(y_row) if far is True else to_y)
        def _():
            act(pj_copy(block, 1))

        if far is not False:
            @when(ours, host_wants(diagonal), far)
            def _():
                act(pj_copy(block, 3))

    def start(copy):
        copy.start()

    def wait_send(copy):
        copy.wait_send()

    def send_lower(slot):
        each_direct(start, False, slot)

        @pl.when(needs(slot, z))
        def _():
            start(pu_partner(slot, col))

    start(loc_copy(col, partner))
    each_loc(start, False)
    each_pv(start, 0)

    @pl.when(z < n_z - 1)
    def _():
        send_lower(0)

    @when(z == 1, needs(0, z))
    def _():
        for slot in range(1, slots):
            send_lower(slot)
    def arrive(slot, step):
        chip = chip_at(step)
        block = 2 * chip + core

        @pl.when(needs(slot, z))
        def _():
            pu_partner(slot, block).wait_recv()

            @when(z == 1, chip >= 2)
            def _():
                pu_relay(slot, block).start()
            pu_partner(slot, col).wait_send()
            pu_partner(slot, block).start()
            each_column(start, block, step, slot)

    def settle_rows(slot, first, final):
        @pl.when(needs(slot, z))
        def _():
            for step in range(first, final):
                pu_partner(slot, 2 * chip_at(step) + other).wait_recv()
        absorb_rows(slot, first, final)

    def pair(step):
        return [2 * chip_at(step) + (core + flip) % 2 for flip in range(2)]

    def column(step):
        @pl.when(is_relay)
        def _():
            for block in pair(step):
                pj_copy(block, 0).wait_recv()

                pj_copy(block, 2).start()

    def settle_column(first, final):
        for step in range(first, final):
            late = straight(step)

            @when(jnp.logical_not(is_owner), wants_column(row),
                  True if late else jnp.logical_not(is_relay))
            def _(step=step):
                for block in pair(step):
                    pj_copy(block, 0).wait_recv()
        absorb_column(first, final)

    def gram_part(slot):
        own_v = pv_all[row].reshape(slots * rank_dim, w)
        own_high, own_low = halves(own_v)
        for source in range(n_row):
            tile = slot * n_row + source

            @pl.when(last + row > tile)
            def _(source=source, tile=tile):
                @pl.when(row != source)
                def _():
                    pv_copy(slot, source, row).wait_recv()
                high, low = halves(pv_all[source, slot])
                both = product(jnp.concatenate([high, low], axis=0), own_high, NT)
                g_part[tile % 2, tile // 2] = (
                    both[:rank_dim] + both[rank_dim:] + product(high, own_low, NT))

    def has_batch(batch):
        return last + row > batch * n_row

    def gram_swap(batch):
        @pl.when(has_batch(batch))
        def _():
            gx_copy(batch).start()

    def gram_sum(batch):
        @pl.when(has_batch(batch))
        def _():
            gx_copy(batch).wait_recv()
            for chip in range(batch * half_z, (batch + 1) * half_z):
                g_sum[chip] = g_part[core, chip] + g_peer[chip]

    def each_gram(act, batch):
        for chip in range(batch * half_z, (batch + 1) * half_z):
            @when(last + row > 2 * chip + core, z != chip)
            def _(chip=chip):
                act(g_copy(z, chip))

    def blocks_of(first, final):
        return [2 * chip_at(step) + flip for step in range(first, final) for flip in range(2)]

    def absorb_rows(slot, first, final):
        @pl.when(active(slot))
        def _():
            total = row_sketch[slot]
            for block in blocks_of(first, final):
                lanes = pl.ds(pl.multiple_of(block * w, w), w)
                high, low = halves(pu_all[block, slot])
                rp[slot, 0, :, lanes] = high
                rp[slot, 1, :, lanes] = low
                total += sketch_of(block, high, low)
            row_sketch[slot] = total

    def absorb_column(first, final):
        @pl.when(any_active)
        def _():
            @pl.when(is_owner)
            def _():
                for block in blocks_of(first, final):
                    pj_all[block] = pu_all[block, owner_slot]
            total = col_sketch[...]
            for block in blocks_of(first, final):
                lanes = pl.ds(pl.multiple_of(block * w, w), w)
                high, low = halves(pj_all[block])
                rj[0, :, lanes] = high
                rj[1, :, lanes] = low
                total += sketch_of(block, high, low)
            col_sketch[...] = total

    def upward():
        @pl.when(z < n_z - 1)
        def _():
            pl.semaphore_wait(far_sem, n_z - 1 - z)
        each_loc(start, True)
        for slot in range(slots):
            each_direct(start, True, slot)

    def points_of(step):
        block = 2 * chip_at(step) + core
        loc_copy(block, partner).wait_recv()
        if step > 1:
            loc_forward(block).wait_send()
        loc_forward(block).start()

    def early(slot, step):
        @pl.when(jnp.logical_or(z > 0, hosts(slot)))
        def _():
            arrive(slot, step)

    def late(slot, step):
        @when(z == 0, jnp.logical_not(hosts(slot)))
        def _():
            arrive(slot, step)

    top = n_z - 1

    @pl.when(corner == 0)
    def _():
        prepare()
        chunk(0)

    @pl.when(z == top)
    def _():
        send_lower(0)
    chunks(1, 2)

    @when(z != 1, z < top)
    def _():
        for slot in range(1, slots):
            send_lower(slot)
    for slot in range(1, slots):
        each_pv(start, slot)
    each_column(start, col, 0)

    @pl.when(corner == 0)
    def _():
        own_all()
    upward()

    @pl.when(jnp.logical_or(z == top, jnp.logical_and(z == 1, jnp.logical_not(needs(0, z)))))
    def _():
        for slot in range(1, slots):
            send_lower(slot)
    points_of(1)
    chunks(2, 3)
    @pl.when(z > 0)
    def _():
        arrive(0, 1)
    gram_part(0)

    @pl.when(z > 0)
    def _():
        arrive(0, 2)
    gram_swap(0)
    points_of(2)
    chunks(3, 4)

    @pl.when(z == 0)
    def _():
        arrive(0, 1)
    gram_sum(0)
    for slot in range(1, slots):
        early(slot, 1)

    @when(z == 0, hosts(0))
    def _():
        arrive(0, 2)
    chunks(4, 5)
    for slot in range(1, slots):
        early(slot, 2)
    each_gram(start, 0)
    for slot in range(1, slots):
        gram_part(slot)
    column(0)
    for slot in range(1, slots):
        gram_swap(slot)
    early(0, 3)
    points_of(3)
    chunks(5, 6)
    for slot in range(1, slots):
        gram_sum(slot)
        late(slot, 1)
    late(0, 2)
    for slot in range(1, slots):
        each_gram(start, slot)
    chunks(6, 7)
    for slot in range(1, slots):
        early(slot, 3)
    late(0, 3)
    chunks(7, 8)
    for slot in range(1, slots):
        settle_rows(slot, 0, n_z - 2)
    column(1)
    for slot in range(1, slots):
        late(slot, 2)
    settle_rows(0, 0, n_z)
    pend_acc[...] = acc[...] * matern_scale
    at_diagonal = row == n_row - 1 - owner_row

    @pl.when(jnp.logical_not(at_diagonal))
    def _():
        settle_column(0, n_z - 2)
    for slot in range(1, slots):
        late(slot, 3)
        settle_rows(slot, n_z - 2, n_z - 1)

    wait_send(loc_copy(col, partner))
    for higher in (False, True):
        each_loc(wait_send, higher)
        for slot in range(slots):
            each_direct(wait_send, higher, slot)
    loc_forward(col).wait_send()

    def relays_done(slot):
        for step in range(1, n_z):
            block = 2 * chip_at(step) + core

            @when(z == 1, chip_at(step) >= 2, needs(slot, z))
            def _(block=block):
                pu_relay(slot, block).wait_send()

    def forwards_done(slot):
        @pl.when(needs(slot, z))
        def _():
            pu_partner(slot, col).wait_send()

    def columns_done(step):
        each_column(wait_send, 2 * chip_at(step) + core, step)
        if not straight(step):
            @pl.when(is_relay)
            def _():
                for block in pair(step):
                    pj_copy(block, 2).wait_send()

    for slot in range(slots):
        each_pv(wait_send, slot)

        @pl.when(has_batch(slot))
        def _(slot=slot):
            gx_copy(slot).wait_send()

    @pl.when(at_diagonal)
    def _():
        settle_column(0, n_z - 2)
    settle_column(n_z - 2, n_z)

    nothing = jnp.zeros((rank_dim, 2 * rank_dim), jnp.bfloat16)

    def stacked(value):
        high, low = halves(value)
        return jnp.concatenate([
            jnp.concatenate([high, high], axis=1), jnp.concatenate([low, nothing], axis=1)
        ], axis=0)

    def right_of(slot):
        @pl.when(active(slot))
        def _():
            lanes = slice(slot * rank_dim, (slot + 1) * rank_dim)
            right_core = dot3(row_sketch[slot], gram_all[:, lanes], NT)
            z_left[slot] = stacked(
                jnp.concatenate([own_sketches[slot, 1], -right_core], axis=1))

    @pl.when(any_active)
    def _():
        gram = g_sum[z]
        for step in range(1, n_z):
            chip = chip_at(step)
            g_copy(chip, z).wait_recv()
            gram = gram + g_all[chip]
        gram_all[...] = gram
        left_core = dot3(col_sketch[...], gram, NN)
        for slot in range(slots):
            lanes = slice(slot * rank_dim, (slot + 1) * rank_dim)

            @pl.when(active(slot))
            def _(slot=slot, lanes=lanes):
                y_left[slot] = stacked(
                    jnp.concatenate([own_sketches[slot, 0], -left_core[:, lanes]], axis=1))
    right_of(0)
    for slot in range(slots):
        each_gram(wait_send, slot)
        relays_done(slot)
    forwards_done(0)
    for step in range(n_z):
        columns_done(step)
    for slot in range(1, slots):
        forwards_done(slot)
        settle_rows(slot, n_z - 1, n_z)
        right_of(slot)


def finish(
    n_row, ru, rv, rp, rj, y_left, z_left, pend_acc,
    trail_y, trail_z, pend_y, pend_z,
    y_buf, z_buf, out_sem, pend_sem,
):
    row, col = lax.axis_index("row"), lax.axis_index("col")
    slots, _, rank_dim, width = ru.shape
    w = pend_y.shape[3]
    pieces = out_sem.shape[2]
    span = width // pieces

    def pend_copy(slot, which):
        lanes = pl.ds((which * slots + slot) * w, w)
        return pltpu.make_async_copy(
            pend_acc.at[:, lanes], (pend_y, pend_z)[which].at[slot, 0], pend_sem.at[slot, which])

    def out_copy(slot, which, piece):
        lanes = pl.ds(piece * span, span)
        src, dst = ((y_buf, trail_y), (z_buf, trail_z))[which]
        return pltpu.make_async_copy(
            src.at[slot, :, lanes], dst.at[slot, 0, 0, :, lanes], out_sem.at[slot, which, piece])

    for slot in range(slots):
        pend_copy(slot, 0).start()
        pend_copy(slot, 1).start()

    for slot in range(slots):
        active = slot * n_row + row > col

        @pl.when(jnp.logical_not(active))
        def _(slot=slot):
            y_buf[slot] = jnp.zeros((rank_dim, width), jnp.float32)
            z_buf[slot] = jnp.zeros((rank_dim, width), jnp.float32)
            for which in range(2):
                for piece in range(pieces):
                    out_copy(slot, which, piece).start()

        @pl.when(active)
        def _(slot=slot):
            for which in range(2):
                left = (y_left, z_left)[which][slot]
                first = (ru, rv)[which]
                buf = (y_buf, z_buf)[which]
                for piece in range(pieces):
                    lanes = slice(piece * span, (piece + 1) * span)
                    second = [rj[part, :, lanes] if which else rp[slot, part, :, lanes]
                              for part in range(2)]
                    right = jnp.concatenate(
                        [first[slot, 0, :, lanes], second[0], first[slot, 1, :, lanes], second[1]],
                        axis=0)
                    both = product(left, right, NN)
                    buf[slot, :, lanes] = both[:rank_dim] + both[rank_dim:]
                    out_copy(slot, which, piece).start()

    for slot in range(slots):
        for which in range(2):
            pend_copy(slot, which).wait()
            for piece in range(pieces):
                out_copy(slot, which, piece).wait()


def broadcast(block, axis, owner):
    block = jnp.where(lax.axis_index(axis) == owner, block, jnp.zeros_like(block))
    return lax.psum(block, axis)


def matmul(left, right):
    return jnp.dot(left, right, precision=lax.Precision.HIGHEST, preferred_element_type=jnp.float32)


def batched(form, left, right):
    return jnp.einsum(
        form, left, right, precision=lax.Precision.HIGHEST, preferred_element_type=jnp.float32
    )


def matern(row_points, col_points):
    delta_x = row_points[0][:, None] - col_points[0][None, :]
    delta_y = row_points[1][:, None] - col_points[1][None, :]
    distance = jnp.sqrt(delta_x * delta_x + delta_y * delta_y)
    scaled = root_three * distance / length_scale
    return matern_scale * (1.0 + scaled) * jnp.exp(-scaled)


def plain_on_device(trail_u, trail_v, ranks, panel_u, panel_v, locations, pend_locs, sketch):
    row_count = lax.axis_size("row")
    row_index = lax.axis_index("row")
    col_index = lax.axis_index("col")
    row_slots = trail_u.shape[0]
    rank_dim = trail_u.shape[3]
    width = trail_u.shape[4]
    local_width = pend_locs.shape[1]
    gathered_u, gathered_v = (
        lax.all_gather(panel_u, "col", axis=3, tiled=True),
        lax.all_gather(panel_v, "col", axis=3, tiled=True),
    )
    slot_index = col_index // row_count
    own_u = lax.dynamic_index_in_dim(gathered_u[:, 0], slot_index, 0, keepdims=False)
    own_v = lax.dynamic_index_in_dim(gathered_v[:, 0], slot_index, 0, keepdims=False)
    col_pu, col_pv = (
        broadcast(own_u, "row", col_index % row_count),
        broadcast(own_v, "row", col_index % row_count),
    )
    rank_iota = lax.broadcasted_iota(jnp.int32, (row_slots, rank_dim), 1)
    in_use = (rank_iota < ranks[:, 0, 0][:, None]).astype(jnp.float32)
    u_tiles = trail_u[:, 0, 0] * in_use[:, :, None]
    v_tiles = trail_v[:, 0, 0]
    row_pu = gathered_u[:, 0]
    row_pv = gathered_v[:, 0]
    v_sketch = batched("tkn,ln->tkl", v_tiles, sketch)
    u_sketch = batched("tkn,ln->tkl", u_tiles, sketch)
    cross_gram = batched("tkn,ln->tkl", row_pv, col_pv)
    col_sketch = matmul(col_pu, sketch.T)
    row_sketch = batched("tkn,ln->tkl", row_pu, sketch)
    left_core = batched("tkm,ml->tkl", cross_gram, col_sketch)
    y_tiles = batched("tkl,tkn->tln", v_sketch, u_tiles) - batched(
        "tkl,tkn->tln", left_core, row_pu
    )
    right_core = batched("tkl,tkm->tlm", row_sketch, cross_gram)
    z_tiles = batched("tkl,tkn->tln", u_sketch, v_tiles) - batched(
        "tlm,mn->tln", right_core, col_pu
    )
    tile_rows = jnp.arange(row_slots, dtype=jnp.int32) * row_count + row_index
    keep_mask = (tile_rows > col_index)[:, None, None]
    trail_y = jnp.where(keep_mask, y_tiles, 0.0).reshape(row_slots, 1, 1, rank_dim, width)
    trail_z = jnp.where(keep_mask, z_tiles, 0.0).reshape(row_slots, 1, 1, rank_dim, width)
    y_list = []
    z_list = []
    rows_all, pend_all = (
        lax.all_gather(locations, "col", axis=3, tiled=True),
        lax.all_gather(pend_locs.reshape(1, 1, 2, local_width), "col", axis=3, tiled=True),
    )
    col_points = pend_all[0, 0]
    for slot_num in range(row_slots):
        own_kernel = matern(locations[slot_num, 0], col_points)
        y_list.append(matmul(sketch, own_kernel.T))
        col_kernel = matern(rows_all[slot_num, 0], pend_locs)
        z_list.append(matmul(sketch, col_kernel))
    pend_y = jnp.stack(y_list)
    pend_z = jnp.stack(z_list)
    pend_y = pend_y.reshape(row_slots, 1, rank_dim, local_width)
    pend_z = pend_z.reshape(row_slots, 1, rank_dim, local_width)
    return (trail_y, trail_z, pend_y, pend_z)


def on_device(n_row, n_col, trail_u, trail_v, ranks, panel_u, panel_v, locations, pend_locs, sketch):
    slots, _, _, rank_dim, width = trail_u.shape
    w = pend_locs.shape[1]
    n_z = n_col // 2
    fits = n_col == slots * n_row and n_row == 4 and slots == 2
    if w % 128 or rank_dim % 16 or not fits:
        return plain_on_device(
            trail_u, trail_v, ranks, panel_u, panel_v, locations, pend_locs, sketch
        )
    flat = slots * rank_dim
    f32, bf16 = jnp.float32, jnp.bfloat16
    dma = pltpu.SemaphoreType.DMA
    vmem = pl.BlockSpec(memory_space=pltpu.VMEM)
    hbm = pl.BlockSpec(memory_space=pltpu.HBM)
    point_rows = -(-(2 * slots + 2) // 8) * 8
    shape = jax.ShapeDtypeStruct
    kept = pl.pallas_call(
        functools.partial(kernel, n_row, n_col),
        out_shape=(
            pltpu.VMEM((slots, 2, rank_dim, width), bf16),
            pltpu.VMEM((slots, 2, rank_dim, width), bf16),
            pltpu.VMEM((slots, 2, rank_dim, width), bf16),
            pltpu.VMEM((2, rank_dim, width), bf16),
            pltpu.VMEM((slots, 2 * rank_dim, 4 * rank_dim), bf16),
            pltpu.VMEM((slots, 2 * rank_dim, 4 * rank_dim), bf16),
            pltpu.VMEM((rank_dim, 2 * slots * w), f32),
        ),
        in_specs=[hbm] * 8,
        out_specs=(vmem,) * 7,
        scratch_shapes=[
            pltpu.SMEM((slots,), jnp.int32),
            pltpu.VMEM((slots, rank_dim, width), f32),
            pltpu.VMEM((slots, rank_dim, width), f32),
            pltpu.VMEM((rank_dim, width), f32),
            pltpu.VMEM((n_col, slots + 1, 2, w), f32),
            pltpu.VMEM((n_col, slots, rank_dim, w), f32),
            pltpu.VMEM((n_col, rank_dim, w), f32),
            pltpu.VMEM((n_row, slots, rank_dim, w), f32),
            pltpu.VMEM((2, n_z, rank_dim, flat), f32),
            pltpu.VMEM((n_z, rank_dim, flat), f32),
            pltpu.VMEM((n_z, rank_dim, flat), f32),
            pltpu.VMEM((n_z, rank_dim, flat), f32),
            pltpu.VMEM((1, w, point_rows), f32),
            pltpu.VMEM((2, 2 * slots * w), f32),
            pltpu.VMEM((n_col, 2 * rank_dim, w), bf16),
            pltpu.VMEM((w, 2 * slots * w), bf16),
            pltpu.VMEM((w, 2 * slots * w), bf16),
            pltpu.VMEM((rank_dim, 2 * slots * w), f32),
            pltpu.VMEM((slots, 2, rank_dim, rank_dim), f32),
            pltpu.VMEM((slots, rank_dim, rank_dim), f32),
            pltpu.VMEM((rank_dim, rank_dim), f32),
            pltpu.VMEM((rank_dim, flat), f32),
            pltpu.SemaphoreType.REGULAR,
            dma((6,)), dma((n_z,)), dma, dma((n_col,)),
            dma((slots, 2 * n_z - 2)), dma((slots,)), dma((slots, n_col)),
            dma((slots, n_row)), dma((slots, n_row)),
            dma((3, n_z)), dma((n_col,)),
            dma((slots,)), dma((slots,)), dma((n_z,)), dma((n_z,)),
        ],
        compiler_params=pltpu.CompilerParams(
            collective_id=0, has_side_effects=True, vmem_limit_bytes=VMEM_LIMIT),
    )(*[
        pltpu.with_memory_space_constraint(value, pltpu.HBM) for value in (
            ranks.reshape(slots),
            trail_u.reshape(slots, rank_dim, width),
            trail_v.reshape(slots, rank_dim, width),
            panel_u.reshape(slots, rank_dim, w),
            panel_v.reshape(slots, rank_dim, w),
            locations.reshape(slots, 2, w),
            pend_locs,
            sketch,
        )
    ])
    kept = [pltpu.with_memory_space_constraint(value, pltpu.VMEM) for value in kept]
    pieces = 2
    return pl.pallas_call(
        functools.partial(finish, n_row),
        out_shape=(
            shape((slots, 1, 1, rank_dim, width), f32),
            shape((slots, 1, 1, rank_dim, width), f32),
            shape((slots, 1, rank_dim, w), f32),
            shape((slots, 1, rank_dim, w), f32),
        ),
        in_specs=[vmem] * 7,
        out_specs=(hbm,) * 4,
        scratch_shapes=[
            pltpu.VMEM((slots, rank_dim, width), f32),
            pltpu.VMEM((slots, rank_dim, width), f32),
            dma((slots, 2, pieces)), dma((slots, 2)),
        ],
        compiler_params=pltpu.CompilerParams(vmem_limit_bytes=VMEM_LIMIT),
    )(*kept)


def solution(mesh):
    in_specs = (
        P(None, "row", "col", None, None),
        P(None, "row", "col", None, None),
        P(None, "row", "col"),
        P(None, "row", None, "col"),
        P(None, "row", None, "col"),
        P(None, "row", None, "col"),
        P(None, "col"),
        P(),
    )
    out_specs = (
        P(None, "row", "col", None, None),
        P(None, "row", "col", None, None),
        P(None, "row", None, "col"),
        P(None, "row", None, "col"),
    )
    body = functools.partial(on_device, mesh.shape["row"], mesh.shape["col"])
    return jax.shard_map(
        body, mesh=mesh, in_specs=in_specs, out_specs=out_specs, check_vma=False
    )
```
